512 devices in a mesh: gx: 8 (over z), gy: 8 (over y), gz: 8 (over x, core).
Axes of the slice: x: 4, y: 8, z: 8, core: 2. Of those that a mesh axis runs over, the one named last changes fastest.
Arguments:
- right_side: float32 [512, 512, 512], P('gx', 'gy', 'gz'), may hold values from -6 to 6
- guess: float32 [512, 512, 512], P('gx', 'gy', 'gz'), may hold values from -6 to 6
Outputs:
- solution: float32 [512, 512, 512], P('gx', 'gy', 'gz')
- residual: float32 [512, 512, 512], P('gx', 'gy', 'gz')
The draws below stay inside these ranges and needn't reach their ends.
All inputs are finite; a program needn't handle non-finite values.
Results may differ from the reference program's by a relative error of at most 0.0003.
Values sent between devices are 32-bit elements.
No kernel may reach another device: no remote copies, remote signals or barrier semaphores. Data moves between devices by JAX's collectives and lax.ppermute only.
A program may use at most 256 MiB of HBM per device.

```python
import jax
import jax.numpy as jnp
from jax import lax

LEVELS = 7
COARSE_SWEEPS = 4
NX = 512
NY = 512
NZ = 512


def level_of(stream_key, dims, split, low, largest):
    def one(axis_at, blocks):
        heights = jax.random.uniform(jax.random.fold_in(jax.random.fold_in(stream_key, 6), axis_at), (blocks,), jnp.float32, low / len(split), largest / len(split))
        return jnp.repeat(jnp.exp(heights), dims[axis_at] // blocks).reshape((-1,) + (1,) * (len(dims) - axis_at - 1))

    loudness = one(*split[0])
    for cut in split[1:]:
        loudness = loudness * one(*cut)
    return loudness


def bell_draw(key, shape, deviation, most, cuts=(), held_as=jnp.bfloat16):
    array = deviation * jax.random.normal(key, shape, jnp.float32)
    if cuts:
        array = array * level_of(key, shape, cuts, -0.22, 0.18)
    return jnp.clip(array, -most, most).astype(held_as)


def setup_inputs(seed: int = 0) -> dict:
    streams_of = jax.random.split(jax.random.key(seed), 3)
    right_side = bell_draw(streams_of[0], (NX, NY, NZ), 1.0, 6.0, ((0, 8), (1, 8), (2, 8)), jnp.float32)
    guess = bell_draw(streams_of[1], (NX, NY, NZ), 1.0, 6.0, ((0, 8), (1, 8), (2, 8)), jnp.float32)
    return dict(right_side=right_side, guess=guess)


def face_total(padded):
    total = padded[2:, 1:-1, 1:-1] + padded[:-2, 1:-1, 1:-1]
    total = total + padded[1:-1, 2:, 1:-1] + padded[1:-1, :-2, 1:-1]
    total = total + padded[1:-1, 1:-1, 2:] + padded[1:-1, 1:-1, :-2]
    return total


def neighbours(field):
    return face_total(jnp.pad(field, 1))


def walls(index, total):
    return (index == 0).astype(jnp.float32) + (index == total - 1).astype(jnp.float32)


def geometry(shape):
    first = lax.iota(jnp.int32, shape[0])[:, None, None]
    second = lax.iota(jnp.int32, shape[1])[None, :, None]
    third = lax.iota(jnp.int32, shape[2])[None, None, :]
    parity = (first + second + third) % 2
    diagonal = 6.0 + walls(first, shape[0]) + walls(second, shape[1]) + walls(third, shape[2])
    return parity == 0, parity == 1, diagonal


def half_sweep(field, source, colour, diagonal, scale):
    updated = (scale * source + neighbours(field)) / diagonal
    return jnp.where(colour, updated, field)


def residual_of(field, source, diagonal, inverse):
    return source - (diagonal * field - neighbours(field)) * inverse


def restrict(remainder):
    shape = remainder.shape
    grouped = remainder.reshape(shape[0] // 2, 2, shape[1] // 2, 2, shape[2] // 2, 2)
    return jnp.sum(grouped, axis=(1, 3, 5)) * 0.125


def odd_pad(field):
    for axis in range(3):
        count = field.shape[axis]
        lowest = -lax.slice_in_dim(field, 0, 1, axis=axis)
        highest = -lax.slice_in_dim(field, count - 1, count, axis=axis)
        field = jnp.concatenate([lowest, field, highest], axis=axis)
    return field


def prolong(padded):
    centre = padded[1:-1, 1:-1, 1:-1]
    below_first = 0.25 * (padded[:-2, 1:-1, 1:-1] - centre)
    above_first = 0.25 * (padded[2:, 1:-1, 1:-1] - centre)
    below_second = 0.25 * (padded[1:-1, :-2, 1:-1] - centre)
    above_second = 0.25 * (padded[1:-1, 2:, 1:-1] - centre)
    below_third = 0.25 * (padded[1:-1, 1:-1, :-2] - centre)
    above_third = 0.25 * (padded[1:-1, 1:-1, 2:] - centre)
    along_first = jnp.stack([below_first, above_first], axis=1)[:, :, :, None, :, None]
    along_second = jnp.stack([below_second, above_second], axis=2)[:, None, :, :, :, None]
    along_third = jnp.stack([below_third, above_third], axis=3)[:, None, :, None, :, :]
    fine = centre[:, None, :, None, :, None] + along_first + along_second + along_third
    shape = centre.shape
    return fine.reshape(2 * shape[0], 2 * shape[1], 2 * shape[2])


def cycle(field, source, level):
    red, black, diagonal = geometry(source.shape)
    scale = 4.0 ** level
    if level == LEVELS - 1:
        for sweep_index in range(COARSE_SWEEPS):
            field = half_sweep(field, source, red, diagonal, scale)
            field = half_sweep(field, source, black, diagonal, scale)
        return field
    field = half_sweep(field, source, red, diagonal, scale)
    field = half_sweep(field, source, black, diagonal, scale)
    coarse = restrict(residual_of(field, source, diagonal, 0.25 ** level))
    correction = cycle(jnp.zeros_like(coarse), coarse, level + 1)
    field = field + prolong(odd_pad(correction))
    field = half_sweep(field, source, red, diagonal, scale)
    return half_sweep(field, source, black, diagonal, scale)


def reference(right_side, guess):
    solution = cycle(guess, right_side, 0)
    red, black, diagonal = geometry(right_side.shape)
    return solution, residual_of(solution, right_side, diagonal, 1.0)
```

```python
import functools
import typing

import jax
import jax.numpy as jnp
from jax import lax
from jax.experimental import pallas as pl
from jax.experimental.pallas import tpu as pltpu
from jax.sharding import PartitionSpec as P

F32 = jnp.float32
BF16 = jnp.bfloat16
COARSE_SWEEPS = 4
COUNT = 8


class Level(typing.NamedTuple):
    level: int
    pairs: int
    rows: int
    first: int
    offset: int
    size: int

    @property
    def scale(self):
        return 4.0**self.level

    @property
    def inverse(self):
        return 0.25**self.level

    @property
    def own(self):
        return self.size // 2

    def shape(self):
        return (self.pairs + 2, self.rows, 128)


L0 = Level(0, 40, 80, 3, 8, 64)
L1 = Level(1, 30, 64, 7, 16, 32)
L2 = Level(2, 14, 32, 3, 8, 16)
L3_OWN = Level(3, 6, 16, 1, 4, 8)
L3 = Level(3, 12, 24, 4, 8, 8)
L4 = Level(4, 16, 64, 0, 0, 32)
L5 = Level(5, 8, 32, 0, 0, 16)
L6 = Level(6, 4, 16, 0, 0, 8)


class Edges(typing.NamedTuple):
    ilo: typing.Any
    ihi: typing.Any
    jlo: typing.Any
    jhi: typing.Any
    klo: typing.Any
    khi: typing.Any


def block_edges():
    ends = []
    for axis in ("gx", "gy", "gz"):
        place = lax.axis_index(axis)
        ends += [place == 0, place == COUNT - 1]
    return Edges(*ends)


def whole_edges():
    yes = lax.axis_index("gx") >= 0
    return Edges(*([yes] * 6))


def lanes_of(shape):
    return lax.broadcasted_iota(jnp.int32, shape, len(shape) - 1)


def rows_of(shape):
    return lax.broadcasted_iota(jnp.int32, shape, len(shape) - 2)


def signed(lane):
    return jnp.where(lane < 96, lane, lane - 128)


def even_mask(rows):
    shape = (rows, 128)
    return ((rows_of(shape) + lanes_of(shape)) & 1) == 0


def turn(value, shift, axis):
    size = value.shape[axis]
    if isinstance(shift, int):
        shift %= size
        if shift == 0:
            return value
    return pltpu.roll(value, shift, axis)


def bounds(low, high, size):
    return jnp.where(low, 0, -4096), jnp.where(high, size, 4096)


def set_coefficients(lv, edges, c_ref, d_ref):
    shape = (lv.rows, 128)
    row = rows_of(shape) - lv.offset
    lane = signed(lanes_of(shape))
    row_low, row_high = bounds(edges.jlo, edges.jhi, lv.size)
    lane_low, lane_high = bounds(edges.klo, edges.khi, lv.size)
    inside = (row >= row_low) & (row < row_high) & (lane >= lane_low) & (lane < lane_high)
    diagonal = 6.0 + jnp.where(row == row_low, 1.0, 0.0) + jnp.where(row == row_high - 1, 1.0, 0.0)
    diagonal = diagonal + jnp.where(lane == lane_low, 1.0, 0.0) + jnp.where(lane == lane_high - 1, 1.0, 0.0)
    even = jnp.where(even_mask(lv.rows), 1.0, 0.0)
    for index, extra in enumerate((0.0, even, 1.0 - even)):
        d_ref[index] = diagonal + extra
        c_ref[index] = jnp.where(inside, 1.0 / (diagonal + extra), 0.0)
    c_ref[3] = jnp.zeros(shape, F32)


def kind(lv, edges, p, red):
    last = lv.first + lv.own - 1
    low, high = (1, 2) if red else (2, 1)
    inner = jnp.where((p == lv.first) & edges.ilo, low, jnp.where((p == last) & edges.ihi, high, 0))
    return jnp.where(((p < lv.first) & edges.ilo) | ((p > last) & edges.ihi), 3, inner)


def loop(low, high, body, unroll=1):
    def step(p, carry):
        body(p)
        return carry

    lax.fori_loop(low, high, step, 0, unroll=unroll)


def around(ref, p, even, red):
    value = ref[p + 1]
    before, after = ref[p], ref[p + 2]
    rows = value.shape[0]
    total = value + (jnp.where(even, before, after) if red else jnp.where(even, after, before))
    total = total + (turn(value, 1, 0) + turn(value, rows - 1, 0))
    return total + (turn(value, 1, 1) + turn(value, 127, 1))


def relax(lv, edges, c_ref, other, source, dest, low, high, red):
    even = even_mask(lv.rows)

    def body(p):
        total = around(other, p, even, red)
        if source is not None:
            total = total + (source[p + 1] if lv.level == 0 else lv.scale * source[p + 1])
        dest[p + 1] = total * c_ref[kind(lv, edges, p, red)]

    loop(low, high, body)


def relax_zero(lv, edges, c_ref, source, dest, low, high):
    loop(low, high, lambda p: dest.__setitem__(p + 1, lv.scale * source[p + 1] * c_ref[kind(lv, edges, p, True)]))


def remainder_at(lv, edges, d_ref, g_red, g_black, red, black, p, even):
    def one(mine, theirs, source, is_red):
        d = d_ref[jnp.minimum(kind(lv, edges, p, is_red), 2)]
        gap = d * mine[p + 1] - around(theirs, p, even, is_red)
        return source[p + 1] - (gap if lv.level == 0 else lv.inverse * gap)

    return one(red, black, g_red, True), one(black, red, g_black, False)


def clear_guards(lv, *refs):
    for ref in refs:
        ref[0] = jnp.zeros(ref.shape[1:], F32)
        ref[ref.shape[0] - 1] = jnp.zeros(ref.shape[1:], F32)


def split_dot(value, weights):
    high = value.astype(BF16)
    low = (value - high.astype(F32)).astype(BF16)
    return jnp.dot(jnp.concatenate([high, low], axis=1), weights, preferred_element_type=F32)


def halving_weights(own_lanes):
    shape = (256, 128)
    fine = signed(rows_of(shape) & 127)
    coarse = signed(lanes_of(shape))
    hit = (fine >> 1) == coarse
    if own_lanes:
        hit = hit & (fine >= 0) & (fine < own_lanes)
    return jnp.where(hit, 0.125, 0.0).astype(BF16)


def doubling_weights(size, low, high):
    shape = (256, 256)
    coarse = signed(rows_of(shape) & 127)
    lane = lanes_of(shape)
    fine = signed(lane & 127)
    parent = fine >> 1
    beside = parent + jnp.where((fine & 1) == 1, 1, -1)
    beyond = ((beside == -1) & low) | ((beside == size) & high)
    centre = jnp.where(coarse == parent, 0.25, 0.0)
    neighbour = jnp.where(coarse == beside, 0.25, 0.0)
    mixed = jnp.where(beyond, 0.0, centre + neighbour)
    return jnp.where(lane < 128, mixed, centre).astype(BF16)


def restrict(lv, edges, d_ref, g_red, g_black, red, black, low, count, row_low, rows, y_ref, z_ref, out_ref, own_lanes):
    even = even_mask(lv.rows)
    half = rows // 2

    def body(t):
        r_red, r_black = remainder_at(lv, edges, d_ref, g_red, g_black, red, black, low + t, even)
        y_ref[t] = r_red + r_black

    loop(0, count, body)

    def fold(t):
        z_ref[t] = y_ref[t, pl.ds(row_low, half, stride=2), :] + y_ref[t, pl.ds(row_low + 1, half, stride=2), :]

    loop(0, count, fold)
    weights = halving_weights(own_lanes)
    chunk = max(c for c in range(1, count + 1) if count % c == 0 and (c * half <= 256 or c == 1))

    def product(n):
        value = z_ref[pl.ds(n * chunk, chunk)].reshape(chunk * half, 128)
        out_ref[pl.ds(n * chunk, chunk)] = split_dot(value, weights).reshape(chunk, half, 128)

    loop(0, count // chunk, product)


def colour_planes(planes, pairs, red, black):
    even = even_mask(planes.shape[1])

    def body(p):
        low, high = planes[2 * p], planes[2 * p + 1]
        red[p + 1] = jnp.where(even, low, high)
        black[p + 1] = jnp.where(even, high, low)

    loop(0, pairs, body)


def whole_planes(red, black, pair_low, pairs, row_low, rows, e_ref, start=0):
    even = even_mask(rows)

    def body(t):
        r = red[pair_low + t + 1, pl.ds(row_low, rows), :]
        b = black[pair_low + t + 1, pl.ds(row_low, rows), :]
        e_ref[start + 2 * t] = jnp.where(even, r, b)
        e_ref[start + 2 * t + 1] = jnp.where(even, b, r)

    loop(0, pairs, body)


def prolong(e_ref, count, rows, row_zero, plane_zero, size, edges, near, plain):
    weights = doubling_weights(size, edges.klo, edges.khi)
    chunk = max(c for c in range(1, count + 1) if count % c == 0 and (c * rows <= 320 or c == 1))
    shape = (rows, 128)
    row = rows_of(shape) - row_zero
    at_low = (row == 0) & edges.jlo
    at_high = (row == size - 1) & edges.jhi

    def body(n):
        both = split_dot(e_ref[pl.ds(n * chunk, chunk)].reshape(chunk * rows, 128), weights).reshape(chunk, rows, 256)
        for c in range(chunk):
            t = n * chunk + c
            mixed, value = both[c, :, :128], both[c, :, 128:]
            before = jnp.where(at_low, -value, turn(value, 1, 0))
            after = jnp.where(at_high, -value, turn(value, rows - 1, 0))
            near[t, pl.ds(0, rows, stride=2), :] = mixed + before
            near[t, pl.ds(1, rows, stride=2), :] = mixed + after
            plain[t, pl.ds(0, rows, stride=2), :] = value
            plain[t, pl.ds(1, rows, stride=2), :] = value

    loop(0, count // chunk, body)
    if plane_zero > 0:
        pl.when(edges.ilo)(lambda: plain.__setitem__(plane_zero - 1, -plain[plane_zero]))
    last = plane_zero + size - 1
    if last + 1 < count:
        pl.when(edges.ihi)(lambda: plain.__setitem__(last + 1, -plain[last]))


def correct(lv, edges, c_ref, kept, near, plain, plane_zero, dest, low, high):
    even = even_mask(lv.rows)

    def body(p):
        t = p - lv.first + plane_zero
        step = near[t, : lv.rows] + jnp.where(even, plain[t + 1, : lv.rows], plain[t - 1, : lv.rows])
        c = c_ref[kind(lv, edges, p, False)]
        dest[p + 1] = jnp.where(c > 0.0, kept[p + 1] + step, 0.0)

    loop(low, high, body)


def compact_kernel(guess, source, x_ref, y_ref):
    even = ((rows_of((64, 64)) + lanes_of((64, 64))) & 1) == 0

    def body(u):
        blacks = []
        for s in range(2):
            p = 2 * u + s
            low, high = guess[2 * p], guess[2 * p + 1]
            f_low, f_high = source[2 * p], source[2 * p + 1]
            x_ref[p] = jnp.concatenate([jnp.where(even, high, low), jnp.where(even, f_low, f_high)], axis=1)
            blacks.append(jnp.where(even, f_high, f_low))
        y_ref[u] = jnp.concatenate(blacks, axis=1)

    loop(0, 16, body)


def pack_kernel(ib, ia, x, y, jb, ja, xf, yf, ku, kd):
    zero = jnp.zeros((80, 128), F32)
    for p in range(3):
        xf[p, 8:72] = ib[p]
        xf[35 + p, 8:72] = ia[p]
    loop(0, 32, lambda p: xf.__setitem__((p + 3, slice(8, 72)), x[p]))
    yf[0, 8:72] = ib[3]
    yf[17, 8:72] = ia[3]
    loop(0, 16, lambda p: yf.__setitem__((p + 1, slice(8, 72)), y[p]))

    def ends(p):
        xf[p, 0:8] = jb[p]
        xf[p, 72:80] = ja[p]

    loop(0, 38, ends)

    def more(p):
        yf[p, 0:8] = jb[p + 38]
        yf[p, 72:80] = ja[p + 38]

    loop(0, 18, more)
    for p in (38, 39):
        xf[p] = zero
    for p in range(18, 24):
        yf[p] = zero
    half = lanes_of((80, 128)) & 63
    lane = lanes_of((80, 128))
    x_down = (lane < 5) | ((lane >= 64) & (lane < 68))
    x_up = ((lane >= 59) & (lane < 64)) | (lane >= 124)
    y_down = half < 3
    y_up = half >= 61
    for u in range(5):
        down, up = zero, zero
        for s in range(8):
            value = xf[8 * u + s]
            down = down + turn(jnp.where(x_down, value, 0.0), 8 * s, 1)
            up = up + turn(jnp.where(x_up, value, 0.0), 8 * s, 1)
            if u < 3:
                value = yf[8 * u + s]
                down = down + turn(jnp.where(y_down, value, 0.0), 8 * s + 5, 1)
                up = up + turn(jnp.where(y_up, value, 0.0), 8 * s + 3, 1)
        kd[u] = down
        ku[u] = up


def fine_kernel(xf, yf, kb, ka, v_black, g_red, g_black, low_quads, high_quads, black, red, y_ref, z_ref, planes, c_ref, d_ref):
    edges = block_edges()
    set_coefficients(L0, edges, c_ref, d_ref)
    zero = jnp.zeros((80, 128), F32)
    lane = lanes_of((80, 128))
    own = lane < 64
    for u in range(5):
        below, above = kb[u], ka[u]
        for s in range(8):
            p = 8 * u + s
            value = xf[p]
            place = (lane - 8 * s) & 127
            edge = jnp.where(place < 5, above, jnp.where((place >= 59) & (place < 64), below, 0.0))
            black[p + 1] = jnp.where(own, value, turn(edge, 64 - 8 * s, 1))
            edge = jnp.where((place >= 64) & (place < 68), above, jnp.where(place >= 124, below, 0.0))
            g_red[p + 1] = jnp.where(own, turn(value, 64, 1), turn(edge, -8 * s, 1))
            if 8 * u + s < 18:
                value = yf[p]
                high = turn(above, 59 - 8 * s, 1)
                low = turn(below, 61 - 8 * s, 1)
                edge = jnp.where((lane >= 64) & (lane < 67), high, jnp.where(lane >= 125, low, 0.0))
                g_black[2 * p + 2] = jnp.where(own, value, edge)
                high, low, value = turn(high, 64, 1), turn(low, 64, 1), turn(value, 64, 1)
                edge = jnp.where((lane >= 64) & (lane < 67), high, jnp.where(lane >= 125, low, 0.0))
                g_black[2 * p + 3] = jnp.where(own, value, edge)
    for q in (0, 1, 38, 39, 40, 41):
        g_black[q] = zero
    clear_guards(L0, black, g_red, red, v_black)
    for q in (1, 38, 39, 40):
        red[q] = zero
        v_black[q] = zero
    relax(L0, edges, c_ref, black, g_red, red, 1, 37, True)
    relax(L0, edges, c_ref, red, g_black, v_black, 1, 37, False)
    restrict(L0, edges, d_ref, g_red, g_black, red, v_black, 3, 32, 8, 64, y_ref, z_ref, planes, 64)

    def quad(q, out):
        total = planes[4 * q]
        for m in range(1, 4):
            total = total + turn(planes[4 * q + m], 32 * m, 1)
        return total

    for q in range(4):
        low_quads[q] = quad(q, None)
        high_quads[q] = quad(q + 4, None)


def pack_quads_kernel(ib, ia, low_quads, high_quads, jb, ja, qf, ku, kd):
    for index, part in enumerate((ib, low_quads, high_quads, ia)):
        for q in range(4):
            qf[4 * index + q, 16:48] = part[q]
    for q in range(16):
        qf[q, 0:16] = jb[q]
        qf[q, 48:64] = ja[q]
    low_half = (lanes_of((64, 128)) & 31) < 16
    for u in range(8):
        first, second = qf[2 * u], qf[2 * u + 1]
        kd[u] = jnp.where(low_half, first, turn(second, 16, 1))
        ku[u] = jnp.where(low_half, turn(first, -16, 1), second)


def middle_kernel(
    qf, kb, ka, v1, gr1, gb1, v2, gr2, gb2, message,
    red1, y1, z1, p1, red2, y2, z2, p2, gr3, gb3, red3, black3, y3, z3, p3,
    c1, d1, c2, d2, c3, d3,
):
    edges = block_edges()
    for lv, c, d in ((L1, c1, d1), (L2, c2, d2), (L3_OWN, c3, d3)):
        set_coefficients(lv, edges, c, d)
    lane = lanes_of((64, 128))
    even = even_mask(64)

    def unpack(u):
        below, above = kb[u], ka[u]
        for h in range(2):
            value = qf[2 * u + h]
            for t in range(2):
                pair = []
                for m in (2 * t, 2 * t + 1):
                    at = 32 * m + 16 * h
                    right = turn(above, 32 - at, 1)
                    left = turn(below, 112 - at, 1)
                    edge = jnp.where(lane < 48, right, jnp.where(lane >= 112, left, 0.0))
                    pair.append(jnp.where(lane < 32, turn(value, -32 * m, 1), edge))
                index = 4 * u + 2 * h + t
                gr1[index] = jnp.where(even, pair[0], pair[1])
                gb1[index] = jnp.where(even, pair[1], pair[0])

    loop(0, 8, unpack)
    clear_guards(L1, red1, v1)
    relax_zero(L1, edges, c1, gr1, red1, 0, 30)
    relax(L1, edges, c1, red1, gb1, v1, 0, 30, False)
    restrict(L1, edges, d1, gr1, gb1, red1, v1, 1, 28, 0, 64, y1, z1, p1, 0)
    colour_planes(p1, 14, gr2, gb2)
    clear_guards(L2, red2, v2, gr2, gb2)
    relax_zero(L2, edges, c2, gr2, red2, 0, 14)
    relax(L2, edges, c2, red2, gb2, v2, 0, 14, False)
    restrict(L2, edges, d2, gr2, gb2, red2, v2, 1, 12, 0, 32, y2, z2, p2, 0)
    colour_planes(p2, 6, gr3, gb3)
    clear_guards(L3_OWN, red3, black3)
    relax_zero(L3_OWN, edges, c3, gr3, red3, 0, 6)
    relax(L3_OWN, edges, c3, red3, gb3, black3, 0, 6, False)
    restrict(L3_OWN, edges, d3, gr3, gb3, red3, black3, 1, 4, 0, 16, y3, z3, p3, 8)
    lane = lanes_of((8, 128))
    row = rows_of((8, 128))
    third = jnp.zeros((8, 128), F32)
    for i in range(8):
        third = third + turn(jnp.where(lane < 8, p2[i + 2, 4:12], 0.0), 8 * i, 1)
    fourth = jnp.zeros((8, 128), F32)
    for i in range(4):
        fourth = fourth + turn(jnp.where((lane < 4) & (row >= 2) & (row < 6), p3[i], 0.0), 32 * i, 1)
    fourth = pltpu.roll(fourth, 4 * lax.axis_index("gz"), 1)
    fourth = jnp.where((lax.axis_index("gy") & 1) == 0, turn(fourth, 6, 0), turn(fourth, 2, 0))

    def store(n):
        message[n, 0] = third
        message[n, 1] = fourth

    loop(0, 64, store)


def plane_kernel(tiles, message):
    y, z = lax.axis_index("gy"), lax.axis_index("gz")
    parts = []
    for t in range(4):
        total = tiles[16 * t, 1]
        for n in range(1, 16):
            total = total + tiles[16 * t + n, 1]
        parts.append(total)
    window = []
    for dy in range(3):
        for dz in range(3):
            yy, zz = y + (dy - 1), z + (dz - 1)
            inside = (yy >= 0) & (yy < COUNT) & (zz >= 0) & (zz < COUNT)
            index = jnp.clip(yy, 0, COUNT - 1) * COUNT + jnp.clip(zz, 0, COUNT - 1)
            window.append(jnp.where(inside, tiles[index, 0], 0.0))
    window.append(jnp.zeros((8, 128), F32))
    for n in range(5):
        parts.append(window[2 * n] + turn(window[2 * n + 1], 64, 1))

    def store(n):
        for index, part in enumerate(parts):
            message[n, index] = part

    loop(0, 8, store)


def coarse_kernel(
    tiles, v2, gr2, gb2, v1, gr1, gb1, v0, gr0, gb0, out, rest,
    gr4, gb4, red4, v4, y4, z4, p4, gr5, gb5, red5, v5, y5, z5, p5, gr6, gb6, red6, v6, full, window,
    gr3, gb3, red3, v3, b3, b2, red2, b1, red1, b0, red0, e_ref, near, plain,
    c0, d0, c1, d1, c2, d2, c3, d3, c4, d4, c5, d5, c6, d6,
):
    edges = block_edges()
    whole = whole_edges()
    for lv, c, d in ((L0, c0, d0), (L1, c1, d1), (L2, c2, d2), (L3, c3, d3)):
        set_coefficients(lv, edges, c, d)
    for lv, c, d in ((L4, c4, d4), (L5, c5, d5), (L6, c6, d6)):
        set_coefficients(lv, whole, c, d)
    x, y, z = (lax.axis_index(axis) for axis in ("gx", "gy", "gz"))

    lane = signed(lanes_of((8, 128)))
    even8 = even_mask(8)
    for dx in range(3):
        at = x + (dx - 1)
        inside = (at >= 0) & (at < COUNT)
        at = jnp.clip(at, 0, COUNT - 1)
        for dy in range(3):
            parts = [jnp.where(inside, tiles[at, 4 + (3 * dy + dz) // 2], 0.0) for dz in range(3)]
            for pair in range(4):
                both = []
                for i in (2 * pair, 2 * pair + 1):
                    total = jnp.zeros((8, 128), F32)
                    for dz in range(3):
                        shift = 8 * (dz - 1) - 8 * i - 64 * ((3 * dy + dz) % 2)
                        hit = (lane >= 8 * (dz - 1)) & (lane < 8 * dz)
                        total = jnp.where(hit, turn(parts[dz], shift, 1), total)
                    both.append(total)
                index = 4 * dx + pair + 1
                gr3[index, 8 * dy : 8 * dy + 8] = jnp.where(even8, both[0], both[1])
                gb3[index, 8 * dy : 8 * dy + 8] = jnp.where(even8, both[1], both[0])
    clear_guards(L3, red3, v3)
    relax_zero(L3, edges, c3, gr3, red3, 0, 12)
    relax(L3, edges, c3, red3, gb3, v3, 0, 12, False)

    lane = lanes_of((32, 128))
    even32 = even_mask(32)
    zero = jnp.zeros((32, 128), F32)

    def place(n):
        value = tiles[n, 0:4].reshape(32, 128)
        for t in range(2):
            low = jnp.where(lane < 32, turn(value, -64 * t, 1), 0.0)
            high = jnp.where(lane < 32, turn(value, -64 * t - 32, 1), 0.0)
            index = 2 * n + t + 1
            gr4[index, 0:32] = jnp.where(even32, low, high)
            gb4[index, 0:32] = jnp.where(even32, high, low)
            gr4[index, 32:64] = zero
            gb4[index, 32:64] = zero

    loop(0, 8, place)
    clear_guards(L4, red4, v4, gr4, gb4)
    relax_zero(L4, whole, c4, gr4, red4, 0, 16)
    relax(L4, whole, c4, red4, gb4, v4, 0, 16, False)
    restrict(L4, whole, d4, gr4, gb4, red4, v4, 0, 16, 0, 64, y4, z4, p4, 32)
    colour_planes(p4, 8, gr5, gb5)
    clear_guards(L5, red5, v5, gr5, gb5)
    relax_zero(L5, whole, c5, gr5, red5, 0, 8)
    relax(L5, whole, c5, red5, gb5, v5, 0, 8, False)
    restrict(L5, whole, d5, gr5, gb5, red5, v5, 0, 8, 0, 32, y5, z5, p5, 16)
    colour_planes(p5, 4, gr6, gb6)
    clear_guards(L6, red6, v6)
    relax_zero(L6, whole, c6, gr6, red6, 0, 4)
    relax(L6, whole, c6, red6, gb6, v6, 0, 4, False)
    for sweep_index in range(COARSE_SWEEPS - 1):
        relax(L6, whole, c6, v6, gr6, red6, 0, 4, True)
        relax(L6, whole, c6, red6, gb6, v6, 0, 4, False)

    def lift(coarse_red, coarse_black, pair_low, pairs, row_low, rows, plane_zero, row_zero, size, at, fine, c, kept, dest, low, high):
        e = e_ref.at[0 : 2 * pairs + 2, 0:rows]
        n = near.at[0 : 2 * pairs + 2, 0 : 2 * rows]
        p = plain.at[0 : 2 * pairs + 2, 0 : 2 * rows]
        whole_planes(coarse_red, coarse_black, pair_low, pairs, row_low, rows, e)
        prolong(e, 2 * pairs, rows, row_zero, plane_zero, size, at, n, p)
        correct(fine, at, c, kept, n, p, plane_zero, dest, low, high)

    def smooth(lv, at, c, black, g_red, g_black, red, dest, low, high, low2, high2):
        relax(lv, at, c, black, g_red, red, low, high, True)
        relax(lv, at, c, red, g_black, dest, low2, high2, False)

    ascend_whole(L6, L5, whole, c5, red6, v6, v5, gr5, gb5, red5, y5, e_ref, near, plain)
    ascend_whole(L5, L4, whole, c4, red5, v5, v4, gr4, gb4, red4, y4, e_ref, near, plain)

    full[...] = jnp.zeros(full.shape, F32)
    even = even_mask(32)

    def spread(t):
        r, b = red4[t + 1, 0:32], v4[t + 1, 0:32]
        full[2 * t + 4, 8:40] = jnp.where(even, r, b)
        full[2 * t + 5, 8:40] = jnp.where(even, b, r)

    loop(0, 16, spread)

    def cut(t):
        rows = full[4 * x + t, pl.ds(4 * y + 4, 16), :]
        e_ref[t, 0:16] = pltpu.roll(rows, (128 - 4 * z) & 127, 1)

    loop(0, 12, cut)
    n, p = near.at[0:12, 0:32], plain.at[0:12, 0:32]
    prolong(e_ref.at[0:12, 0:16], 12, 16, 4, 4, 4, edges, n, p)
    correct(L3, edges, c3, v3, n, p, 4, b3, 1, 11)
    clear_guards(L3, b3, red3)
    smooth(L3, edges, c3, b3, gr3, gb3, red3, b3, 2, 10, 2, 10)

    lift(red3, b3, 2, 8, 4, 16, 4, 4, 8, edges, L2, c2, v2, b2, 0, 14)
    clear_guards(L2, b2, red2)
    smooth(L2, edges, c2, b2, gr2, gb2, red2, b2, 1, 13, 1, 13)

    lift(red2, b2, 1, 12, 0, 32, 4, 8, 16, edges, L1, c1, v1, b1, 5, 25)
    b1[5] = jnp.zeros(b1.shape[1:], F32)
    b1[26] = jnp.zeros(b1.shape[1:], F32)
    red1[6] = jnp.zeros(b1.shape[1:], F32)
    red1[25] = jnp.zeros(b1.shape[1:], F32)
    smooth(L1, edges, c1, b1, gr1, gb1, red1, b1, 5, 25, 6, 24)

    lift(red1, b1, 5, 20, 12, 40, 4, 4, 32, edges, L0, c0, v0, b0, 1, 37)
    b0[1] = jnp.zeros(b0.shape[1:], F32)
    b0[38] = jnp.zeros(b0.shape[1:], F32)
    smooth(L0, edges, c0, b0, gr0, gb0, red0, b0, 1, 37, 2, 36)

    even0 = even_mask(80)
    own = even_mask(64)[:, 0:64]

    def finish(t):
        p = t + 3
        r, b = red0[p + 1, 8:72, 0:64], b0[p + 1, 8:72, 0:64]
        out[2 * t] = jnp.where(own, r, b)
        out[2 * t + 1] = jnp.where(own, b, r)
        r, b = remainder_at(L0, edges, d0, gr0, gb0, red0, b0, p, even0)
        r, b = r[8:72, 0:64], b[8:72, 0:64]
        rest[2 * t] = jnp.where(own, r, b)
        rest[2 * t + 1] = jnp.where(own, b, r)

    loop(0, 32, finish)


def ascend_whole(coarse, fine, at, c, coarse_red, coarse_black, kept, g_red, g_black, red, scratch, e_ref, near, plain):
    rows = coarse.rows
    count = coarse.size
    e = e_ref.at[0:count, 0:rows]
    n = near.at[0 : count + 2, 0 : 2 * rows]
    p = plain.at[0 : count + 2, 0 : 2 * rows]
    whole_planes(coarse_red, coarse_black, 0, coarse.pairs, 0, rows, e)
    prolong(e, count, rows, 0, 0, count, at, near.at[1 : count + 1, 0 : 2 * rows], plain.at[1 : count + 1, 0 : 2 * rows])
    p[0] = -p[1]
    p[count + 1] = -p[count]
    correct(fine, at, c, kept, n, p, 1, kept, 0, fine.pairs)
    relax(fine, at, c, kept, g_red, red, 0, fine.pairs, True)
    relax(fine, at, c, red, g_black, kept, 0, fine.pairs, False)


def struct(*shape):
    return jax.ShapeDtypeStruct(shape, F32)


def call(kernel, outs, scratch, name, flops=2_000_000):
    space = pl.BlockSpec(memory_space=pltpu.VMEM)

    def run(*args):
        return pl.pallas_call(
            kernel,
            out_shape=outs,
            in_specs=[space] * len(args),
            out_specs=[space] * len(outs),
            scratch_shapes=[pltpu.VMEM(shape, F32) for shape in scratch],
            compiler_params=pltpu.CompilerParams(vmem_limit_bytes=40 * 2**20),
            cost_estimate=pl.CostEstimate(flops=flops, bytes_accessed=1_000_000, transcendentals=0),
            name=name,
        )(*args)

    return run


def pair(to_next, to_before, axis):
    up = [(i, i + 1) for i in range(COUNT - 1)]
    down = [(i + 1, i) for i in range(COUNT - 1)]
    return lax.ppermute(to_next, axis, up), lax.ppermute(to_before, axis, down)


def face(guess, source, start, first):
    even = ((lax.broadcasted_iota(jnp.int32, (64, 64), 0) + lax.broadcasted_iota(jnp.int32, (64, 64), 1)) & 1) == 0
    low, high = guess[start : start + 6 : 2], guess[start + 1 : start + 6 : 2]
    f_low, f_high = source[start : start + 6 : 2], source[start + 1 : start + 6 : 2]
    red = jnp.where(even, f_low, f_high)
    black = jnp.where(even, f_high, f_low)
    mixed = jnp.concatenate([jnp.where(even, high, low), red], axis=2)
    return jnp.concatenate([mixed, jnp.concatenate([black[first : first + 1], black[first + 1 : first + 2]], axis=2)], axis=0)


def coefficient_scratch(*levels):
    shapes = []
    for lv in levels:
        shapes += [(4, lv.rows, 128), (3, lv.rows, 128)]
    return shapes


def per_device(right_side, guess):
    ib, ia = pair(face(guess, right_side, 58, 1), face(guess, right_side, 0, 0), "gx")
    x, y = call(compact_kernel, (struct(32, 64, 128), struct(16, 64, 128)), [], "compact")(guess, right_side)

    def ends(low):
        parts = [ib[:3], x, ia[:3], ib[3:], y, ia[3:]]
        return jnp.concatenate([part[:, low : low + 8] for part in parts], axis=0)

    jb, ja = pair(ends(56), ends(0), "gy")
    xf, yf, ku, kd = call(
        pack_kernel, (struct(40, 80, 128), struct(24, 80, 128), struct(5, 80, 128), struct(5, 80, 128)), [], "pack"
    )(ib, ia, x, y, jb, ja)
    kb, ka = pair(ku, kd, "gz")
    fine = L0.shape()
    v0, gr0, gb0, low_quads, high_quads = call(
        fine_kernel,
        (struct(*fine), struct(*fine), struct(*fine), struct(4, 32, 128), struct(4, 32, 128)),
        [fine, fine, (32, 80, 128), (32, 32, 128), (32, 32, 128)] + coefficient_scratch(L0),
        "fine",
    )(xf, yf, kb, ka)

    ib, ia = pair(high_quads, low_quads, "gx")

    def quad_ends(low):
        return jnp.concatenate([part[:, low : low + 16] for part in (ib, low_quads, high_quads, ia)], axis=0)

    jb, ja = pair(quad_ends(16), quad_ends(0), "gy")
    qf, ku, kd = call(pack_quads_kernel, (struct(16, 64, 128), struct(8, 64, 128), struct(8, 64, 128)), [], "pack_quads")(
        ib, ia, low_quads, high_quads, jb, ja
    )
    kb, ka = pair(ku, kd, "gz")
    s1, s2, s3 = L1.shape(), L2.shape(), L3_OWN.shape()
    v1, gr1, gb1, v2, gr2, gb2, message = call(
        middle_kernel,
        tuple(struct(*s) for s in (s1, s1, s1, s2, s2, s2, (64, 2, 8, 128))),
        [s1, (28, 64, 128), (28, 32, 128), (28, 32, 128), s2, (12, 32, 128), (12, 16, 128), (12, 16, 128)]
        + [s3, s3, s3, s3, (4, 16, 128), (4, 8, 128), (4, 8, 128)]
        + coefficient_scratch(L1, L2, L3_OWN),
        "middle",
    )(qf, kb, ka)

    tiles = lax.all_to_all(message, ("gy", "gz"), 0, 0)
    (message,) = call(plane_kernel, (struct(8, 9, 8, 128),), [], "plane")(tiles)
    tiles = lax.all_to_all(message, "gx", 0, 0)
    s3, s4, s5, s6 = L3.shape(), L4.shape(), L5.shape(), L6.shape()
    return tuple(
        call(
            coarse_kernel,
            (struct(64, 64, 64), struct(64, 64, 64)),
            [s4, s4, s4, s4, (16, 64, 128), (16, 32, 128), (16, 32, 128)]
            + [s5, s5, s5, s5, (8, 32, 128), (8, 16, 128), (8, 16, 128)]
            + [s6, s6, s6, s6, (40, 48, 128), (12, 16, 128)]
            + [s3, s3, s3, s3, s3, s2, s2, s1, s1, fine, fine]
            + [(42, 40, 128), (42, 80, 128), (42, 80, 128)]
            + coefficient_scratch(L0, L1, L2, L3, L4, L5, L6),
            "coarse",
        )(tiles, v2, gr2, gb2, v1, gr1, gb1, v0, gr0, gb0)
    )


def solution(mesh):
    return jax.shard_map(
        per_device,
        mesh=mesh,
        in_specs=(P("gx", "gy", "gz"), P("gx", "gy", "gz")),
        out_specs=(P("gx", "gy", "gz"), P("gx", "gy", "gz")),
        check_vma=False,
    )
```

```python
import typing

import jax
import jax.numpy as jnp
from jax import lax
from jax.experimental import pallas as pl
from jax.experimental.pallas import tpu as pltpu
from jax.sharding import PartitionSpec as P


F32 = jnp.float32
BF16 = jnp.bfloat16
COARSE_SWEEPS = 4
COUNT = 8


class Level(typing.NamedTuple):
    level: int
    pairs: int
    rows: int
    first: int
    offset: int
    size: int

    @property
    def scale(self):
        return 4.0**self.level

    @property
    def inverse(self):
        return 0.25**self.level

    @property
    def own(self):
        return self.size // 2

    def shape(self):
        return (self.pairs + 2, self.rows, 128)


L0 = Level(0, 40, 80, 3, 8, 64)
L1 = Level(1, 30, 64, 7, 16, 32)
L2 = Level(2, 14, 32, 3, 8, 16)
L3_OWN = Level(3, 6, 16, 1, 4, 8)
L3 = Level(3, 12, 32, 4, 8, 8)
L4 = Level(4, 16, 32, 0, 0, 32)
L5 = Level(5, 8, 16, 0, 0, 16)
L6 = Level(6, 4, 8, 0, 0, 8)


class Edges(typing.NamedTuple):
    ilo: typing.Any
    ihi: typing.Any
    jlo: typing.Any
    jhi: typing.Any
    klo: typing.Any
    khi: typing.Any


def block_edges():
    ends = []
    for axis in ("gx", "gy", "gz"):
        place = lax.axis_index(axis)
        ends += [place == 0, place == COUNT - 1]
    return Edges(*ends)


def whole_edges():
    yes = lax.axis_index("gx") >= 0
    return Edges(*([yes] * 6))


def lanes_of(shape):
    return lax.broadcasted_iota(jnp.int32, shape, len(shape) - 1)


def rows_of(shape):
    return lax.broadcasted_iota(jnp.int32, shape, len(shape) - 2)


def signed(lane):
    return jnp.where(lane < 96, lane, lane - 128)


def cells_of(shape):
    row = rows_of(shape)
    return (row & 7) * (shape[-2] // 8) + (row >> 3)


def even_mask(rows):
    shape = (rows, 128)
    return ((cells_of(shape) + lanes_of(shape)) & 1) == 0


def even_natural(shape):
    return ((rows_of(shape) + lanes_of(shape)) & 1) == 0


def gather_rows(ref, index, rows, start=0):
    stride = rows // 8
    if stride == 1:
        return ref[index, pl.ds(start, 8), :]
    return jnp.concatenate([ref[index, pl.ds(start + t, 8, stride=stride), :] for t in range(stride)], axis=0)


def scatter_rows(ref, index, value, start=0):
    stride = value.shape[0] // 8
    for t in range(stride):
        ref[index, pl.ds(start + t, 8, stride=stride), :] = value[8 * t : 8 * t + 8]


def row_before(value):
    last = value[value.shape[0] - 8 :]
    first = jnp.where(rows_of((8, 128)) == 0, 0.0, pltpu.roll(last, 1, 0))
    return first if value.shape[0] == 8 else jnp.concatenate([first, value[: value.shape[0] - 8]], axis=0)


def row_after(value):
    last = jnp.where(rows_of((8, 128)) == 7, 0.0, pltpu.roll(value[:8], 7, 0))
    return last if value.shape[0] == 8 else jnp.concatenate([value[8:], last], axis=0)


def fold_rows(value):
    tiles = value.shape[0] // 16
    if tiles == 0:
        raise ValueError("rows")
    return jnp.concatenate([value[16 * t : 16 * t + 8] + value[16 * t + 8 : 16 * t + 16] for t in range(tiles)], axis=0)


def double_rows(even, odd):
    parts = []
    for t in range(even.shape[0] // 8):
        parts += [even[8 * t : 8 * t + 8], odd[8 * t : 8 * t + 8]]
    return jnp.concatenate(parts, axis=0)


def turn(value, shift, axis):
    size = value.shape[axis]
    if isinstance(shift, int):
        shift %= size
        if shift == 0:
            return value
    return pltpu.roll(value, shift, axis)


def bounds(low, high, size):
    return jnp.where(low, 0, -4096), jnp.where(high, size, 4096)


def set_coefficients(lv, edges, c_ref, d_ref):
    shape = (lv.rows, 128)
    row = cells_of(shape) - lv.offset
    lane = signed(lanes_of(shape))
    row_low, row_high = bounds(edges.jlo, edges.jhi, lv.size)
    lane_low, lane_high = bounds(edges.klo, edges.khi, lv.size)
    inside = (row >= row_low) & (row < row_high) & (lane >= lane_low) & (lane < lane_high)
    diagonal = 6.0 + jnp.where(row == row_low, 1.0, 0.0) + jnp.where(row == row_high - 1, 1.0, 0.0)
    diagonal = diagonal + jnp.where(lane == lane_low, 1.0, 0.0) + jnp.where(lane == lane_high - 1, 1.0, 0.0)
    even = jnp.where(even_mask(lv.rows), 1.0, 0.0)
    for index, extra in enumerate((0.0, even, 1.0 - even)):
        d_ref[index] = diagonal + extra
        c_ref[index] = jnp.where(inside, 1.0 / (diagonal + extra), 0.0)
    c_ref[3] = jnp.zeros(shape, F32)


def kind(lv, edges, p, red):
    last = lv.first + lv.own - 1
    low, high = (1, 2) if red else (2, 1)
    if isinstance(p, int):
        if p in (lv.first, last):
            return jnp.where(edges.ilo, low, 0) if p == lv.first else jnp.where(edges.ihi, high, 0)
        return 0 if lv.first < p < last else jnp.where(edges.ilo if p < lv.first else edges.ihi, 3, 0)
    inner = jnp.where((p == lv.first) & edges.ilo, low, jnp.where((p == last) & edges.ihi, high, 0))
    return jnp.where(((p < lv.first) & edges.ilo) | ((p > last) & edges.ihi), 3, inner)


def loop(low, high, body, width=0):
    count = high - low
    width = count if width == 0 else min(width, count)

    def step(n, carry):
        for k in range(width):
            body(low + n * width + k)
        return carry

    if count // width > 1:
        lax.fori_loop(0, count // width, step, 0)
        done = count // width * width
    else:
        done = 0
    for p in range(low + done, high):
        body(p)


def group(rows):
    return max(1, 180 // (rows // 8))


def around(ref, p, even, red):
    value = ref[p + 1]
    before, after = ref[p], ref[p + 2]
    total = value + (jnp.where(even, before, after) if red else jnp.where(even, after, before))
    total = total + (row_before(value) + row_after(value))
    return total + (turn(value, 1, 1) + turn(value, 127, 1))


def relax_at(lv, edges, c_ref, other, source, dest, p, red, even):
    total = around(other, p, even, red) + (source[p + 1] if lv.level == 0 else lv.scale * source[p + 1])
    dest[p + 1] = total * c_ref[kind(lv, edges, p, red)]


def relax(lv, edges, c_ref, other, source, dest, low, high, red):
    even = even_mask(lv.rows)
    loop(low, high, lambda p: relax_at(lv, edges, c_ref, other, source, dest, p, red, even), group(lv.rows))


def relax_zero(lv, edges, c_ref, source, dest, low, high):
    def body(p):
        dest[p + 1] = lv.scale * source[p + 1] * c_ref[kind(lv, edges, p, True)]

    loop(low, high, body, group(lv.rows))


def gap(lv, d, value, total):
    return d * value - total if lv.level == 0 else lv.inverse * (d * value - total)


def black_rest_at(lv, edges, c_ref, d_ref, red, source, dest, rest, p, even):
    total = around(red, p, even, False)
    g = source[p + 1]
    at = kind(lv, edges, p, False)
    value = (total + (g if lv.level == 0 else lv.scale * g)) * c_ref[at]
    dest[p + 1] = value
    rest[p + 1] = g - gap(lv, d_ref[jnp.minimum(at, 2)], value, total)


def relax_black_rest(lv, edges, c_ref, d_ref, red, source, dest, rest, low, high):
    even = even_mask(lv.rows)
    loop(low, high, lambda p: black_rest_at(lv, edges, c_ref, d_ref, red, source, dest, rest, p, even), group(lv.rows))


def red_rest(lv, edges, d_ref, source, red, black, p, even):
    d = d_ref[jnp.minimum(kind(lv, edges, p, True), 2)]
    return source[p + 1] - gap(lv, d, red[p + 1], around(black, p, even, True))


def clear_guards(*refs):
    for ref in refs:
        ref[0] = jnp.zeros(ref.shape[1:], F32)
        ref[ref.shape[0] - 1] = jnp.zeros(ref.shape[1:], F32)


def split_dot(value, weights):
    high = value.astype(BF16)
    low = (value - high.astype(F32)).astype(BF16)
    return jnp.dot(jnp.concatenate([high, low], axis=1), weights, preferred_element_type=F32)


def halving_weights(own_lanes):
    shape = (256, 128)
    fine = signed(rows_of(shape) & 127)
    coarse = signed(lanes_of(shape))
    hit = (fine >> 1) == coarse
    if own_lanes:
        hit = hit & (fine >= 0) & (fine < own_lanes)
    return jnp.where(hit, 0.125, 0.0).astype(BF16)


def doubling_weights(size, low, high):
    shape = (256, 256)
    coarse = signed(rows_of(shape) & 127)
    lane = lanes_of(shape)
    fine = signed(lane & 127)
    parent = fine >> 1
    beside = parent + jnp.where((fine & 1) == 1, 1, -1)
    beyond = ((beside == -1) & low) | ((beside == size) & high)
    centre = jnp.where(coarse == parent, 0.25, 0.0)
    neighbour = jnp.where(coarse == beside, 0.25, 0.0)
    mixed = jnp.where(beyond, 0.0, centre + neighbour)
    return jnp.where(lane < 128, mixed, centre).astype(BF16)


def rest_fold_at(lv, edges, d_ref, g_red, red, black, rest, low, z_ref, p, even):
    z_ref[p - low] = fold_rows(rest[p + 1] + red_rest(lv, edges, d_ref, g_red, red, black, p, even))


def restrict(lv, edges, d_ref, g_red, red, black, rest, low, count, z_ref, out_ref, weights):
    even = even_mask(lv.rows)
    loop(
        low, low + count,
        lambda p: rest_fold_at(lv, edges, d_ref, g_red, red, black, rest, low, z_ref, p, even), group(lv.rows),
    )
    halve(lv, count, z_ref, out_ref, weights)


def halve(lv, count, z_ref, out_ref, weights):
    half = lv.rows // 2
    chunk = max(c for c in range(1, count + 1) if count % c == 0 and (c * half <= 320 or c == 1))

    def product(n):
        value = z_ref[pl.ds(n * chunk, chunk)].reshape(chunk * half, 128)
        out_ref[pl.ds(n * chunk, chunk)] = split_dot(value, weights[...]).reshape(chunk, half, 128)

    loop(0, count // chunk, product)


def colour_planes(planes, pairs, red, black):
    even = even_mask(planes.shape[1])

    def body(p):
        low, high = planes[2 * p], planes[2 * p + 1]
        red[p + 1] = jnp.where(even, low, high)
        black[p + 1] = jnp.where(even, high, low)

    loop(0, pairs, body, 8)


def whole_planes(lv, red, black, pair_low, pairs, e_ref):
    even = even_mask(lv.rows)

    def body(t):
        r, b = red[pair_low + t + 1], black[pair_low + t + 1]
        e_ref[2 * t] = jnp.where(even, r, b)
        e_ref[2 * t + 1] = jnp.where(even, b, r)

    loop(0, pairs, body, 8)


def window_planes(lv, red, black, pair_low, pairs, row_low, natural, e_ref):
    even = even_mask(lv.rows)
    rows = e_ref.shape[1]

    def body(t):
        r, b = red[pair_low + t + 1], black[pair_low + t + 1]
        scatter_rows(natural, 2 * t, jnp.where(even, r, b))
        scatter_rows(natural, 2 * t + 1, jnp.where(even, b, r))

    def again(t):
        e_ref[t] = gather_rows(natural, t, rows, row_low)

    loop(0, pairs, body, 4)
    loop(0, 2 * pairs, again, 8)


def prolong(e_ref, count, plane_zero, size, edges, weights, mixed, plain):
    rows = e_ref.shape[1]
    chunk = max(c for c in range(1, count + 1) if count % c == 0 and (c * rows <= 320 or c == 1))

    def body(n):
        at = pl.ds(n * chunk, chunk)
        both = split_dot(e_ref[at].reshape(chunk * rows, 128), weights[...])
        mixed[at] = both[:, :128].reshape(chunk, rows, 128)
        plain[at] = both[:, 128:].reshape(chunk, rows, 128)

    loop(0, count // chunk, body)
    if plane_zero > 0:
        pl.when(edges.ilo)(lambda: plain.__setitem__(plane_zero - 1, -plain[plane_zero]))
    last = plane_zero + size - 1
    if last + 1 < count:
        pl.when(edges.ihi)(lambda: plain.__setitem__(last + 1, -plain[last]))


def correct(lv, edges, c_ref, kept, mixed, plain, row_zero, plane_zero, dest, low, high):
    body = correct_at(lv, edges, c_ref, kept, mixed, plain, row_zero, plane_zero, dest)
    loop(low, high, body, group(lv.rows))


def correct_at(lv, edges, c_ref, kept, mixed, plain, row_zero, plane_zero, dest):
    even = even_mask(lv.rows)
    half = lv.rows // 2
    row = cells_of((half, 128)) - row_zero
    at_low = (row == 0) & edges.jlo
    at_high = (row == lv.size // 2 - 1) & edges.jhi

    def body(p):
        t = p - lv.first + plane_zero
        value, near = plain[t], mixed[t]
        before = near + jnp.where(at_low, -value, row_before(value))
        after = near + jnp.where(at_high, -value, row_after(value))
        up, down = plain[t + 1], plain[t - 1]
        step = double_rows(before, after) + jnp.where(even, double_rows(up, up), double_rows(down, down))
        c = c_ref[kind(lv, edges, p, False)]
        dest[p + 1] = jnp.where(c > 0.0, kept[p + 1] + step, 0.0)

    return body


def compact_kernel(guess, source, x_ref, y_ref):
    even = ((rows_of((64, 64)) + lanes_of((64, 64))) & 1) == 0

    def body(u):
        blacks = []
        for s in range(2):
            p = 2 * u + s
            low, high = guess[2 * p], guess[2 * p + 1]
            f_low, f_high = source[2 * p], source[2 * p + 1]
            x_ref[p] = jnp.concatenate([jnp.where(even, high, low), jnp.where(even, f_low, f_high)], axis=1)
            blacks.append(jnp.where(even, f_high, f_low))
        y_ref[u] = jnp.concatenate(blacks, axis=1)

    loop(0, 16, body, 2)


def pack_kernel(ib, ia, x, y, jb, ja, xf, yf, ku, kd):
    zero = jnp.zeros((80, 128), F32)
    for p in range(3):
        xf[p, 8:72] = ib[p]
        xf[35 + p, 8:72] = ia[p]
    loop(0, 32, lambda p: xf.__setitem__((p + 3, slice(8, 72)), x[p]), 4)
    yf[0, 8:72] = ib[3]
    yf[17, 8:72] = ia[3]
    loop(0, 16, lambda p: yf.__setitem__((p + 1, slice(8, 72)), y[p]), 4)

    tile = jnp.zeros((8, 128), F32)
    for p in range(38):
        xf[p, 0:8] = tile
        xf[p, 3:8] = jb[5 * p : 5 * p + 5]
        xf[p, 72:80] = tile
        xf[p, 72:77] = ja[5 * p : 5 * p + 5]
    for p in range(18):
        yf[p, 0:8] = tile
        yf[p, 5:8] = jb[190 + 3 * p : 193 + 3 * p]
        yf[p, 72:80] = tile
        yf[p, 72:75] = ja[190 + 3 * p : 193 + 3 * p]
    for p in (38, 39):
        xf[p] = zero
    for p in range(18, 24):
        yf[p] = zero
    lane = lanes_of((80, 128))
    for u in range(5):
        down, up, up_y = zero, zero, zero
        for s in range(8):
            value = turn(xf[8 * u + s], 8 * s, 1)
            place = (lane - 8 * s) & 127
            down = jnp.where((place < 5) | ((place >= 64) & (place < 68)), value, down)
            up = jnp.where(((place >= 59) & (place < 64)) | (place >= 124), value, up)
            if 8 * u + s < 18:
                value = turn(yf[8 * u + s], 8 * s + 5, 1)
                down = jnp.where(place_y(lane, s, 0), value, down)
                up_y = jnp.where(place_y(lane, s, 61), value, up_y)
        kd[u] = down
        ku[u] = up + turn(up_y, -2, 1) if u < 3 else up


def place_y(lane, s, start):
    place = (lane - 8 * s - 5) & 63
    return (place >= start) & (place < start + 3)


def rows_kernel(ib, ia, guess_low, guess_high, source_low, source_high, up, down):
    even = even_natural((8, 64))
    for out, guess, source, low, x_at, y_at in (
        (down, guess_low, source_low, 0, 0, 0),
        (up, guess_high, source_high, 56, 3, 5),
    ):
        blacks = []
        for p in range(38):
            if 3 <= p < 35:
                n = 2 * p - 6
                first, second, f_first, f_second = guess[n], guess[n + 1], source[n], source[n + 1]
                value = jnp.concatenate(
                    [jnp.where(even, second, first), jnp.where(even, f_first, f_second)], axis=1
                )
                blacks.append(jnp.where(even, f_second, f_first))
            else:
                value = ib[p, low : low + 8] if p < 3 else ia[p - 35, low : low + 8]
            out[5 * p : 5 * p + 5] = value[x_at : x_at + 5]
        for p in range(18):
            if p == 0 or p == 17:
                value = (ib if p == 0 else ia)[3, low : low + 8]
            else:
                value = jnp.concatenate(blacks[2 * p - 2 : 2 * p], axis=1)
            out[190 + 3 * p : 193 + 3 * p] = value[y_at : y_at + 3]
        out[244:248] = jnp.zeros((4, 128), F32)


def spread_kernel(xf, yf, black, g_red, g_black, c_ref, d_ref, weights):
    set_coefficients(L0, block_edges(), c_ref, d_ref)
    weights[...] = halving_weights(64)
    zero = jnp.zeros((80, 128), F32)
    own = lanes_of((80, 128)) < 64

    def first(p):
        value = gather_rows(xf, p, 80)
        black[p + 1] = jnp.where(own, value, 0.0)
        g_red[p + 1] = jnp.where(own, turn(value, 64, 1), 0.0)

    loop(0, 40, first, 4)

    def second(p):
        value = gather_rows(yf, p, 80)
        g_black[2 * p + 2] = jnp.where(own, value, 0.0)
        g_black[2 * p + 3] = jnp.where(own, turn(value, 64, 1), 0.0)

    loop(0, 18, second, 4)
    for q in (0, 1, 38, 39, 40, 41):
        g_black[q] = zero
    clear_guards(black, g_red)


def fine_kernel(
    black0, g_red0, g_black0, kb, ka, c_ref, d_ref, weights, v_black, g_red, g_black, low_quads, high_quads,
    black, red, rest, z_ref, planes, natural,
):
    edges = block_edges()
    zero = jnp.zeros((80, 128), F32)
    lane = lanes_of((80, 128))

    even = even_mask(80)

    def sides(u):
        below = jnp.where(edges.klo, 0.0, gather_rows(kb, u, 80))
        return below, jnp.where(edges.khi, 0.0, gather_rows(ka, u, 80))

    def merge(p):
        below, above = sides(p // 8)
        turned = 8 * (p % 8)
        place = (lane - turned) & 127
        edge = jnp.where(place < 5, above, jnp.where((place >= 59) & (place < 64), below, 0.0))
        black[p + 1] = black0[p + 1] + turn(edge, 64 - turned, 1)
        edge = jnp.where((place >= 64) & (place < 68), above, jnp.where(place >= 124, below, 0.0))
        g_red[p + 1] = g_red0[p + 1] + turn(edge, -turned, 1)

    def merge_black(n):
        below, above = sides(n // 8)
        below = turn(below, 2, 1)
        turned = 8 * (n % 8)
        place = (lane - turned) & 127
        edge = jnp.where((place >= 5) & (place < 8), above, jnp.where((place >= 66) & (place < 69), below, 0.0))
        g_black[2 * n + 2] = g_black0[2 * n + 2] + turn(edge, 59 - turned, 1)
        edge = jnp.where((place >= 69) & (place < 72), above, jnp.where((place >= 2) & (place < 5), below, 0.0))
        g_black[2 * n + 3] = g_black0[2 * n + 3] + turn(edge, -5 - turned, 1)

    for q in (0, 1, 38, 39, 40, 41):
        g_black[q] = zero
    for ref in (black, g_red):
        for q in (0, 39, 40, 41):
            ref[q] = zero
    for ref in (red, v_black):
        for q in (0, 1, 38, 39, 40, 41):
            ref[q] = zero
    for n in range(44):
        if n < 38:
            merge(n)
        if n % 2 == 0 and n < 36:
            merge_black(n // 2)
        if 1 <= n - 2 < 37:
            relax_at(L0, edges, c_ref, black, g_red, red, n - 2, True, even)
        if 1 <= n - 4 < 37:
            black_rest_at(L0, edges, c_ref, d_ref, red, g_black, v_black, rest, n - 4, even)
        if 3 <= n - 6 < 35:
            rest_fold_at(L0, edges, d_ref, g_red, red, v_black, rest, 3, z_ref, n - 6, even)
    halve(L0, 32, z_ref, planes, weights)

    def quad(q):
        total = planes[4 * q]
        for m in range(1, 4):
            total = total + turn(planes[4 * q + m], 32 * m, 1)
        scatter_rows(natural, q, total)
        return natural[q, 4:36]

    for q in range(4):
        low_quads[q] = quad(q)
        high_quads[q] = quad(q + 4)


def pack_quads_kernel(ib, ia, low_quads, high_quads, jb, ja, qf, ku, kd):
    for index, part in enumerate((ib, low_quads, high_quads, ia)):
        for q in range(4):
            qf[4 * index + q, 16:48] = part[q]
    for q in range(16):
        qf[q, 0:16] = jb[q]
        qf[q, 48:64] = ja[q]
    low_half = (lanes_of((64, 128)) & 31) < 16
    for u in range(8):
        first, second = qf[2 * u], qf[2 * u + 1]
        kd[u] = turn(jnp.where(low_half, first, turn(second, 16, 1)), 32, 1)
        ku[u] = turn(jnp.where(low_half, turn(first, -16, 1), second), -32, 1)


WINDOWS = (L1, L2, L3_OWN, L3)
WHOLES = (L4, L5, L6)
DOUBLINGS = ((32, False), (16, False), (8, False), (4, False), (16, True), (8, True))


def geometry_kernel(after, *refs):
    edges, whole = block_edges(), whole_edges()
    for index, lv in enumerate(WINDOWS + WHOLES):
        set_coefficients(lv, edges if lv in WINDOWS else whole, refs[2 * index], refs[2 * index + 1])
    refs = refs[2 * len(WINDOWS + WHOLES) :]
    refs[0][...] = halving_weights(0)
    for n, (size, is_whole) in enumerate(DOUBLINGS):
        at = whole if is_whole else edges
        refs[1][n] = doubling_weights(size, at.klo, at.khi)


def middle_kernel(
    qf, kb, ka, c1, d1, c2, d2, c3, d3, weights, v1, gr1, gb1, v2, gr2, gb2, message,
    red1, y1, z1, p1, red2, y2, z2, p2, gr3, gb3, red3, black3, y3, z3, p3, natural,
):
    edges = block_edges()
    lane = lanes_of((64, 128))
    even = even_mask(64)

    def unpack(u):
        below = jnp.where(edges.klo, 0.0, gather_rows(kb, u, 64))
        above = jnp.where(edges.khi, 0.0, gather_rows(ka, u, 64))
        sides = ((turn(below, 16, 1), above), (below, turn(above, -16, 1)))
        for h in range(2):
            value = gather_rows(qf, 2 * u + h, 64)
            left, right = sides[h]
            for t in range(2):
                both = []
                for m in (2 * t, 2 * t + 1):
                    place = (lane - 32 * m) & 127
                    edge = jnp.where(place < 48, right, jnp.where(place >= 112, left, 0.0))
                    both.append(turn(jnp.where(place < 32, value, edge), -32 * m, 1))
                index = 4 * u + 2 * h + t
                gr1[index] = jnp.where(even, both[0], both[1])
                gb1[index] = jnp.where(even, both[1], both[0])

    clear_guards(red1, v1)
    for n in range(36):
        if n % 4 == 0 and n < 32:
            unpack(n // 4)
        p = n - 1
        if 0 <= p < 30:
            red1[p + 1] = L1.scale * gr1[p + 1] * c1[kind(L1, edges, p, True)]
        if 0 <= n - 3 < 30:
            black_rest_at(L1, edges, c1, d1, red1, gb1, v1, y1, n - 3, even)
        if 1 <= n - 5 < 29:
            rest_fold_at(L1, edges, d1, gr1, red1, v1, y1, 1, z1, n - 5, even)
    halve(L1, 28, z1, p1, weights)
    colour_planes(p1, 14, gr2, gb2)
    clear_guards(red2, v2, gr2, gb2)
    relax_zero(L2, edges, c2, gr2, red2, 0, 14)
    relax_black_rest(L2, edges, c2, d2, red2, gb2, v2, y2, 0, 14)
    restrict(L2, edges, d2, gr2, red2, v2, y2, 1, 12, z2, p2, weights)
    colour_planes(p2, 6, gr3, gb3)
    clear_guards(red3, black3)
    relax_zero(L3_OWN, edges, c3, gr3, red3, 0, 6)
    relax_black_rest(L3_OWN, edges, c3, d3, red3, gb3, black3, y3, 0, 6)
    restrict(L3_OWN, edges, d3, gr3, red3, black3, y3, 1, 4, z3, p3, weights)
    lane = lanes_of((8, 128))
    row = rows_of((8, 128))
    third = jnp.zeros((8, 128), F32)
    for i in range(8):
        scatter_rows(natural, i, p2[i + 2])
        third = third + turn(jnp.where(lane < 8, natural[i, 4:12], 0.0), 8 * i, 1)
    folded = third + turn(turn(third, 4, 0), 64, 1)
    blocks = jnp.zeros((8, 128), F32)
    for i in range(4):
        blocks = blocks + turn(jnp.where(lane < 4, p3[i], 0.0), 16 * i, 1)
    fourth = jnp.zeros((8, 128), F32)
    for r in range(4):
        fourth = jnp.where((lane & 15) >> 2 == r, turn(turn(blocks, 4 * r, 1), -2 - r, 0), fourth)

    def store(n):
        for r in range(4):
            message[n, r] = folded[r : r + 1]
        message[n, 4] = fourth[0:1]

    loop(0, 64, store, 8)


def plane_kernel(tiles, message, near, rows, grid, blocks):
    x, y, z = (lax.axis_index(axis) for axis in ("gx", "gy", "gz"))
    shape = (8, 128)
    lane, row = lanes_of(shape), rows_of(shape)

    for n in range(64):
        rows[n : n + 1] = tiles[n, 4]
    parts = [jnp.zeros(shape, F32)] * 4
    for n in range(8):
        value = rows[pl.ds(n, 8, stride=8), :]
        here = (lane & 31) >> 2 == n
        for r in range(4):
            index = (lane >> 5) * 16 + 4 * r + (lane & 3)
            parts[r] = jnp.where(here, jnp.take_along_axis(value, index, axis=1), parts[r])
    for r in range(4):
        grid[pl.ds(r, 8, stride=4), :] = parts[r]

    lane = signed(lane)
    for dy in range(3):
        sides = []
        for dz in range(3):
            yy, zz = y + (dy - 1), z + (dz - 1)
            inside = (yy >= 0) & (yy < COUNT) & (zz >= 0) & (zz < COUNT)
            index = jnp.clip(yy, 0, COUNT - 1) * COUNT + jnp.clip(zz, 0, COUNT - 1)
            for r in range(4):
                blocks[3 * dy + dz, r : r + 1] = tiles[index, r]
            value = blocks[3 * dy + dz]
            value = jnp.where(row < 4, value, turn(turn(value, 4, 0), 64, 1))
            sides.append(jnp.where(inside, value, 0.0))
        for i in range(8):
            total = jnp.zeros(shape, F32)
            for dz in range(3):
                hit = (lane >= 8 * (dz - 1)) & (lane < 8 * dz)
                total = jnp.where(hit, turn(sides[dz], 8 * (dz - 1) - 8 * i, 1), total)
            near[i, 8 * dy : 8 * dy + 8] = total

    wide = lanes_of((24, 128))
    ends = []
    for first in (2, 0):
        total = jnp.zeros((24, 128), F32)
        for n in range(6):
            hit = (wide >= 20 * n) & (wide < 20 * n + 20)
            total = jnp.where(hit, turn(near[first + n], 20 * n + 6, 1), total)
        ends.append(total)
    for n in range(COUNT):
        message[n, 0:32] = grid[...]
        message[n, 32:56] = jnp.where(x < n, ends[0], ends[1])


def coarse_kernel(
    tiles, near, v2, gr2, gb2, v1, gr1, gb1, v0, gr0, gb0, c0, d0, c1, c2, c3, c4, d4, c5, d5, c6, halving, doubling, out, rest,
    gr4, gb4, red4, v4, y4, z4, p4, gr5, gb5, red5, v5, y5, z5, p5, gr6, gb6, red6, v6, full,
    gr3, gb3, red3, v3, b3, b2, red2, b1, red1, b0, red0, y0, e_ref, mixed, plain, natural, last, out_held, rest_held, sems,
):
    edges = block_edges()
    whole = whole_edges()
    x, y, z = (lax.axis_index(axis) for axis in ("gx", "gy", "gz"))

    lane = signed(lanes_of((24, 128)))
    even = even_natural((24, 128))
    empty = jnp.zeros((24, 128), F32)

    def put(index, low, high):
        natural[index, 0:24] = jnp.where(even, low, high)
        natural[index + 12, 0:24] = jnp.where(even, high, low)

    for n in range(4):
        put(4 + n, near[2 * n], near[2 * n + 1])
    put(0, empty, empty)
    put(11, empty, empty)
    for at, first in ((x - 1, 1), (x + 1, 8)):
        inside = (at >= 0) & (at < COUNT)
        value = jnp.where(inside, tiles[jnp.clip(at, 0, COUNT - 1), 32:56], 0.0)
        planes = [jnp.where((lane >= -6) & (lane < 14), turn(value, -20 * n - 6, 1), 0.0) for n in range(6)]
        for n in range(3):
            put(first + n, planes[2 * n], planes[2 * n + 1])
    for n in range(24):
        natural[n, 24:32] = jnp.zeros((8, 128), F32)
    for n in range(12):
        gr3[n + 1] = gather_rows(natural, n, 32)
        gb3[n + 1] = gather_rows(natural, n + 12, 32)
    clear_guards(red3, v3)
    relax_zero(L3, edges, c3, gr3, red3, 0, 12)
    relax(L3, edges, c3, red3, gb3, v3, 0, 12, False)

    lane = lanes_of((32, 128))
    even32 = even_mask(32)
    zero = jnp.zeros((8, 128), F32)

    def place(n):
        value = gather_rows(tiles, n, 32)
        for t in range(2):
            low = jnp.where(lane < 32, turn(value, -64 * t, 1), 0.0)
            high = jnp.where(lane < 32, turn(value, -64 * t - 32, 1), 0.0)
            index = 2 * n + t + 1
            gr4[index] = jnp.where(even32, low, high)
            gb4[index] = jnp.where(even32, high, low)

    loop(0, 8, place, 4)
    clear_guards(red4, v4, gr4, gb4)
    relax_zero(L4, whole, c4, gr4, red4, 0, 16)
    relax_black_rest(L4, whole, c4, d4, red4, gb4, v4, y4, 0, 16)
    restrict(L4, whole, d4, gr4, red4, v4, y4, 0, 16, z4, p4, halving)
    colour_planes(p4, 8, gr5, gb5)
    clear_guards(red5, v5, gr5, gb5)
    relax_zero(L5, whole, c5, gr5, red5, 0, 8)
    relax_black_rest(L5, whole, c5, d5, red5, gb5, v5, y5, 0, 8)
    restrict(L5, whole, d5, gr5, red5, v5, y5, 0, 8, z5, p5, halving)
    colour_planes(p5, 4, gr6, gb6)
    clear_guards(red6, v6)
    relax_zero(L6, whole, c6, gr6, red6, 0, 4)
    relax(L6, whole, c6, red6, gb6, v6, 0, 4, False)
    for _ in range(COARSE_SWEEPS - 1):
        relax(L6, whole, c6, v6, gr6, red6, 0, 4, True)
        relax(L6, whole, c6, red6, gb6, v6, 0, 4, False)

    def ascend(coarse, fine, c, w, coarse_red, coarse_black, kept, g_red, g_black, red):
        count = coarse.size
        e, rows = e_ref.at[0:count, 0:count], slice(0, count)
        n, p = mixed.at[0 : count + 2, rows], plain.at[0 : count + 2, rows]
        whole_planes(coarse, coarse_red, coarse_black, 0, coarse.pairs, e)
        prolong(e, count, 0, count, whole, w, mixed.at[1 : count + 1, rows], plain.at[1 : count + 1, rows])
        p[0] = -p[1]
        p[count + 1] = -p[count]
        correct(fine, whole, c, kept, n, p, 0, 1, kept, 0, fine.pairs)
        relax(fine, whole, c, kept, g_red, red, 0, fine.pairs, True)
        relax(fine, whole, c, red, g_black, kept, 0, fine.pairs, False)

    ascend(L6, L5, c5, doubling.at[5], red6, v6, v5, gr5, gb5, red5)
    ascend(L5, L4, c4, doubling.at[4], red5, v5, v4, gr4, gb4, red4)

    even = even_mask(32)
    for t in (0, 1, 2, 3, 36, 37, 38, 39):
        full[t] = jnp.zeros((48, 128), F32)

    def expand(t):
        r, b = red4[t + 1], v4[t + 1]
        for n, value in ((2 * t + 4, jnp.where(even, r, b)), (2 * t + 5, jnp.where(even, b, r))):
            full[n, 0:8] = zero
            scatter_rows(full, n, value, 8)
            full[n, 40:48] = zero

    loop(0, 16, expand, 4)

    def cut(t):
        rows = gather_rows(full, 4 * x + t, 16, 4 * y + 4)
        e_ref[t, 0:16] = pltpu.roll(rows, (128 - 4 * z) & 127, 1)

    loop(0, 12, cut)

    def lift(index, fine, c, count, rows, plane_zero, row_zero, size, kept, dest, low, high):
        e = e_ref.at[0:count, 0:rows]
        n, p = mixed.at[0:count, 0:rows], plain.at[0:count, 0:rows]
        prolong(e, count, plane_zero, size, edges, doubling.at[index], n, p)
        correct(fine, edges, c, kept, n, p, row_zero, plane_zero, dest, low, high)

    def smooth(lv, c, black, g_red, g_black, red, low, high, low2, high2):
        relax(lv, edges, c, black, g_red, red, low, high, True)
        relax(lv, edges, c, red, g_black, black, low2, high2, False)

    lift(3, L3, c3, 12, 16, 4, 4, 4, v3, b3, 1, 11)
    clear_guards(b3, red3)
    smooth(L3, c3, b3, gr3, gb3, red3, 2, 10, 2, 10)

    window_planes(L3, red3, b3, 2, 8, 4, natural.at[0:16, 0:32], e_ref.at[0:16, 0:16])
    lift(2, L2, c2, 16, 16, 4, 4, 8, v2, b2, 0, 14)
    clear_guards(b2, red2)
    smooth(L2, c2, b2, gr2, gb2, red2, 1, 13, 1, 13)

    whole_planes(L2, red2, b2, 1, 12, e_ref.at[0:24, 0:32])
    e = e_ref.at[0:24, 0:32]
    n, p = mixed.at[0:24, 0:32], plain.at[0:24, 0:32]
    prolong(e, 24, 4, 16, edges, doubling.at[1], n, p)
    correct1 = correct_at(L1, edges, c1, v1, n, p, 8, 4, b1)
    for index in (5, 26):
        b1[index] = jnp.zeros(b1.shape[1:], F32)
    even1 = even_mask(64)
    for n in range(5, 29):
        if n < 25:
            correct1(n)
        if 5 <= n - 2 < 25:
            relax_at(L1, edges, c1, b1, gr1, red1, n - 2, True, even1)
        if 6 <= n - 4 < 24:
            relax_at(L1, edges, c1, red1, gb1, b1, n - 4, False, even1)

    window_planes(L1, red1, b1, 5, 20, 12, natural, e_ref.at[0:40, 0:40])
    e = e_ref.at[0:40, 0:40]
    n, p = mixed.at[0:40, 0:40], plain.at[0:40, 0:40]
    prolong(e, 40, 4, 32, edges, doubling.at[0], n, p)
    correct0 = correct_at(L0, edges, c0, v0, n, p, 4, 4, b0)
    b0[1] = jnp.zeros(b0.shape[1:], F32)
    b0[38] = jnp.zeros(b0.shape[1:], F32)
    even0 = even_mask(80)
    copies = []

    def send(held, target, n):
        copy = pltpu.make_async_copy(held.at[pl.ds(8 * n, 8)], target.at[pl.ds(8 * n, 8)], sems.at[len(copies)])
        copy.start()
        copies.append(copy)

    def store(held, p, r, b):
        for n, value in ((0, jnp.where(even0, r, b)), (1, jnp.where(even0, b, r))):
            scatter_rows(last, 2 * (p & 7) + n, value)
            held[2 * p - 6 + n] = last[2 * (p & 7) + n, 8:72, 0:64]

    for n in range(1, 43):
        if n < 37:
            correct0(n)
        if 1 <= n - 2 < 37:
            relax_at(L0, edges, c0, b0, gr0, red0, n - 2, True, even0)
        p = n - 4
        if 2 <= p < 36:
            black_rest_at(L0, edges, c0, d0, red0, gb0, b0, y0, p, even0)
        if 3 <= p < 35:
            store(out_held, p, red0[p + 1], b0[p + 1])
            if p % 4 == 2:
                send(out_held, out, p // 4 - 1)
        p = n - 6
        if 3 <= p < 35:
            store(rest_held, p, red_rest(L0, edges, d0, gr0, red0, b0, p, even0), y0[p + 1])
            if p % 4 == 2:
                send(rest_held, rest, p // 4 - 1)
    for copy in copies:
        copy.wait()


def struct(*shape):
    return jax.ShapeDtypeStruct(shape, F32)


def call(kernel, outs, scratch, flops=2_000_000, out_space=pltpu.VMEM, semaphores=0):
    space = pl.BlockSpec(memory_space=pltpu.VMEM)
    extra = [pltpu.SemaphoreType.DMA((semaphores,))] if semaphores else []

    def run(*args):
        return pl.pallas_call(
            kernel,
            out_shape=outs,
            in_specs=[space] * len(args),
            out_specs=[pl.BlockSpec(memory_space=out_space)] * len(outs),
            scratch_shapes=[pltpu.VMEM(shape, F32) for shape in scratch] + extra,
            compiler_params=pltpu.CompilerParams(vmem_limit_bytes=40 * 2**20),
            cost_estimate=pl.CostEstimate(flops=flops, bytes_accessed=1_000_000, transcendentals=0),
        )(*args)

    return run


def pair(to_next, to_before, axis, ring=False):
    up = [(i, (i + 1) % COUNT) for i in range(COUNT if ring else COUNT - 1)]
    down = [(j, i) for i, j in up]
    after = lax.ppermute(to_before, axis, down)
    before = lax.ppermute(to_next, axis, up)
    return before, after


def face(guess, source, start, first):
    even = ((lax.broadcasted_iota(jnp.int32, (64, 64), 0) + lax.broadcasted_iota(jnp.int32, (64, 64), 1)) & 1) == 0
    low, high = guess[start : start + 6 : 2], guess[start + 1 : start + 6 : 2]
    f_low, f_high = source[start : start + 6 : 2], source[start + 1 : start + 6 : 2]
    red = jnp.where(even, f_low, f_high)
    black = jnp.where(even, f_high, f_low)
    mixed = jnp.concatenate([jnp.where(even, high, low), red], axis=2)
    return jnp.concatenate([mixed, jnp.concatenate([black[first : first + 1], black[first + 1 : first + 2]], axis=2)], axis=0)


def coefficient_shapes(*levels):
    shapes = []
    for lv in levels:
        shapes += [struct(4, lv.rows, 128), struct(3, lv.rows, 128)]
    return shapes


def per_device(right_side, guess):
    ib, ia = pair(face(guess, right_side, 58, 1), face(guess, right_side, 0, 0), "gx")
    x, y = call(compact_kernel, (struct(32, 64, 128), struct(16, 64, 128)), [])(guess, right_side)

    up, down = call(rows_kernel, (struct(248, 128), struct(248, 128)), [])(
        ib, ia, guess[:, 0:8], guess[:, 56:64], right_side[:, 0:8], right_side[:, 56:64]
    )
    jb, ja = pair(up, down, "gy")
    xf, yf, ku, kd = call(
        pack_kernel, (struct(40, 80, 128), struct(24, 80, 128), struct(5, 80, 128), struct(5, 80, 128)), []
    )(ib, ia, x, y, jb, ja)
    kb, ka = pair(ku, kd, "gz", True)
    fine = L0.shape()
    field = struct(*fine)
    weights = jax.ShapeDtypeStruct((256, 128), BF16)
    black, g_red, g_black, c0, d0, w0 = call(
        spread_kernel, (field, field, field, *coefficient_shapes(L0), weights), []
    )(xf, yf)
    v0, gr0, gb0, low_quads, high_quads = call(
        fine_kernel,
        (field, field, field, struct(4, 32, 128), struct(4, 32, 128)),
        [fine, fine, fine, (32, 40, 128), (32, 40, 128), (8, 40, 128)],
    )(black, g_red, g_black, kb, ka, c0, d0, w0)

    ib, ia = pair(high_quads, low_quads, "gx")
    shapes = coefficient_shapes(*WINDOWS, *WHOLES) + [weights, jax.ShapeDtypeStruct((6, 256, 256), BF16)]
    c1, d1, c2, d2, c3o, d3o, c3, _, c4, d4, c5, d5, c6, _, halving, doubling = call(
        geometry_kernel, tuple(shapes), []
    )(low_quads)

    def quad_ends(low):
        return jnp.concatenate([part[:, low : low + 16] for part in (ib, low_quads, high_quads, ia)], axis=0)

    jb, ja = pair(quad_ends(16), quad_ends(0), "gy")
    qf, ku, kd = call(pack_quads_kernel, (struct(16, 64, 128), struct(8, 64, 128), struct(8, 64, 128)), [])(
        ib, ia, low_quads, high_quads, jb, ja
    )
    kb, ka = pair(ku, kd, "gz", True)
    s1, s2, s3 = L1.shape(), L2.shape(), L3_OWN.shape()
    v1, gr1, gb1, v2, gr2, gb2, message = call(
        middle_kernel,
        tuple(struct(*s) for s in (s1, s1, s1, s2, s2, s2, (64, 5, 1, 128))),
        [s1, s1, (28, 32, 128), (28, 32, 128), s2, s2, (12, 16, 128), (12, 16, 128)]
        + [s3, s3, s3, s3, s3, (4, 8, 128), (4, 8, 128), (8, 16, 128)],
    )(qf, kb, ka, c1, d1, c2, d2, c3o, d3o, halving)

    tiles = lax.all_to_all(message, ("gy", "gz"), 0, 0)
    message, near = call(
        plane_kernel, (struct(8, 56, 128), struct(8, 24, 128)), [(64, 128), (32, 128), (9, 8, 128)]
    )(tiles)
    tiles = lax.all_to_all(message, "gx", 0, 0)
    s3, s4, s5, s6 = L3.shape(), L4.shape(), L5.shape(), L6.shape()
    return tuple(
        call(
            coarse_kernel,
            (struct(64, 64, 64), struct(64, 64, 64)),
            [s4, s4, s4, s4, s4, (16, 16, 128), (16, 16, 128)]
            + [s5, s5, s5, s5, s5, (8, 8, 128), (8, 8, 128)]
            + [s6, s6, s6, s6, (40, 48, 128)]
            + [s3, s3, s3, s3, s3, s2, s2, s1, s1, fine, fine, fine]
            + [(42, 40, 128), (42, 40, 128), (42, 40, 128), (40, 64, 128), (16, 80, 128), (64, 64, 64), (64, 64, 64)],
            out_space=pl.ANY,
            semaphores=16,
        )(tiles, near, v2, gr2, gb2, v1, gr1, gb1, v0, gr0, gb0, c0, d0, c1, c2, c3, c4, d4, c5, d5, c6, halving, doubling)
    )


def solution(mesh):
    return jax.shard_map(
        per_device,
        mesh=mesh,
        in_specs=(P("gx", "gy", "gz"), P("gx", "gy", "gz")),
        out_specs=(P("gx", "gy", "gz"), P("gx", "gy", "gz")),
        check_vma=False,
    )
```

```python
import typing

import jax
import jax.numpy as jnp
from jax import lax
from jax.experimental import pallas as pl
from jax.experimental.pallas import tpu as pltpu
from jax.sharding import PartitionSpec as P


F32 = jnp.float32
BF16 = jnp.bfloat16
COARSE_SWEEPS = 4
COUNT = 8


class Level(typing.NamedTuple):
    level: int
    pairs: int
    rows: int
    first: int
    offset: int
    size: int

    @property
    def scale(self):
        return 4.0**self.level

    @property
    def inverse(self):
        return 0.25**self.level

    @property
    def own(self):
        return self.size // 2

    def shape(self):
        return (self.pairs + 2, self.rows, 128)


L0 = Level(0, 40, 80, 3, 8, 64)
L1 = Level(1, 30, 64, 7, 16, 32)
L2 = Level(2, 14, 32, 3, 8, 16)
L3_OWN = Level(3, 6, 16, 1, 4, 8)
L3 = Level(3, 12, 32, 4, 8, 8)
L4 = Level(4, 16, 32, 0, 0, 32)
L5 = Level(5, 8, 16, 0, 0, 16)
L6 = Level(6, 4, 8, 0, 0, 8)


class Edges(typing.NamedTuple):
    ilo: typing.Any
    ihi: typing.Any
    jlo: typing.Any
    jhi: typing.Any
    klo: typing.Any
    khi: typing.Any


def block_edges():
    ends = []
    for axis in ("gx", "gy", "gz"):
        place = lax.axis_index(axis)
        ends += [place == 0, place == COUNT - 1]
    return Edges(*ends)


def whole_edges():
    yes = lax.axis_index("gx") >= 0
    return Edges(*([yes] * 6))


def lanes_of(shape):
    return lax.broadcasted_iota(jnp.int32, shape, len(shape) - 1)


def rows_of(shape):
    return lax.broadcasted_iota(jnp.int32, shape, len(shape) - 2)


def signed(lane):
    return jnp.where(lane < 96, lane, lane - 128)


def cells_of(shape):
    row = rows_of(shape)
    return (row & 7) * (shape[-2] // 8) + (row >> 3)


def even_mask(rows):
    shape = (rows, 128)
    return ((cells_of(shape) + lanes_of(shape)) & 1) == 0


def even_natural(shape):
    return ((rows_of(shape) + lanes_of(shape)) & 1) == 0


def gather_rows(ref, index, rows, start=0):
    stride = rows // 8
    if stride == 1:
        return ref[index, pl.ds(start, 8), :]
    return jnp.concatenate([ref[index, pl.ds(start + t, 8, stride=stride), :] for t in range(stride)], axis=0)


def scatter_rows(ref, index, value, start=0):
    stride = value.shape[0] // 8
    for t in range(stride):
        ref[index, pl.ds(start + t, 8, stride=stride), :] = value[8 * t : 8 * t + 8]


def row_before(value):
    last = value[value.shape[0] - 8 :]
    first = jnp.where(rows_of((8, 128)) == 0, 0.0, pltpu.roll(last, 1, 0))
    return first if value.shape[0] == 8 else jnp.concatenate([first, value[: value.shape[0] - 8]], axis=0)


def row_after(value):
    last = jnp.where(rows_of((8, 128)) == 7, 0.0, pltpu.roll(value[:8], 7, 0))
    return last if value.shape[0] == 8 else jnp.concatenate([value[8:], last], axis=0)


def fold_rows(value):
    tiles = value.shape[0] // 16
    if tiles == 0:
        raise ValueError("rows")
    return jnp.concatenate([value[16 * t : 16 * t + 8] + value[16 * t + 8 : 16 * t + 16] for t in range(tiles)], axis=0)


def double_rows(even, odd):
    parts = []
    for t in range(even.shape[0] // 8):
        parts += [even[8 * t : 8 * t + 8], odd[8 * t : 8 * t + 8]]
    return jnp.concatenate(parts, axis=0)


def turn(value, shift, axis):
    size = value.shape[axis]
    if isinstance(shift, int):
        shift %= size
        if shift == 0:
            return value
    return pltpu.roll(value, shift, axis)


def bounds(low, high, size):
    return jnp.where(low, 0, -4096), jnp.where(high, size, 4096)


def set_coefficients(lv, edges, c_ref, d_ref):
    shape = (lv.rows, 128)
    row = cells_of(shape) - lv.offset
    lane = signed(lanes_of(shape))
    row_low, row_high = bounds(edges.jlo, edges.jhi, lv.size)
    lane_low, lane_high = bounds(edges.klo, edges.khi, lv.size)
    inside = (row >= row_low) & (row < row_high) & (lane >= lane_low) & (lane < lane_high)
    diagonal = 6.0 + jnp.where(row == row_low, 1.0, 0.0) + jnp.where(row == row_high - 1, 1.0, 0.0)
    diagonal = diagonal + jnp.where(lane == lane_low, 1.0, 0.0) + jnp.where(lane == lane_high - 1, 1.0, 0.0)
    even = jnp.where(even_mask(lv.rows), 1.0, 0.0)
    for index, extra in enumerate((0.0, even, 1.0 - even)):
        d_ref[index] = diagonal + extra
        c_ref[index] = jnp.where(inside, 1.0 / (diagonal + extra), 0.0)
    c_ref[3] = jnp.zeros(shape, F32)


def kind(lv, edges, p, red):
    last = lv.first + lv.own - 1
    low, high = (1, 2) if red else (2, 1)
    if isinstance(p, int):
        if p in (lv.first, last):
            return jnp.where(edges.ilo, low, 0) if p == lv.first else jnp.where(edges.ihi, high, 0)
        return 0 if lv.first < p < last else jnp.where(edges.ilo if p < lv.first else edges.ihi, 3, 0)
    inner = jnp.where((p == lv.first) & edges.ilo, low, jnp.where((p == last) & edges.ihi, high, 0))
    return jnp.where(((p < lv.first) & edges.ilo) | ((p > last) & edges.ihi), 3, inner)


def loop(low, high, body, width=0):
    count = high - low
    width = count if width == 0 else min(width, count)

    def step(n, carry):
        for k in range(width):
            body(low + n * width + k)
        return carry

    if count // width > 1:
        lax.fori_loop(0, count // width, step, 0)
        done = count // width * width
    else:
        done = 0
    for p in range(low + done, high):
        body(p)


def group(rows):
    return max(1, 180 // (rows // 8))


def neighbour_weights():
    shape = (256, 128)
    apart = ((rows_of(shape) & 127) - lanes_of(shape)) & 127
    return jnp.where((apart == 1) | (apart == 127), 1.0, 0.0).astype(BF16)


def lane_sum(value, weights):
    rows = value.shape[0]
    part = rows if weights is None else 16
    total = turn(value[:part], 1, 1) + turn(value[:part], 127, 1)
    return total if part == rows else jnp.concatenate([total, split_dot(value[part:], weights[...])], axis=0)


def around(ref, p, even, red, weights=None):
    value = ref[p + 1]
    before, after = ref[p], ref[p + 2]
    total = value + (jnp.where(even, before, after) if red else jnp.where(even, after, before))
    total = total + (row_before(value) + row_after(value))
    return total + lane_sum(value, weights)


def relax_at(lv, edges, c_ref, other, source, dest, p, red, even, weights=None):
    total = around(other, p, even, red, weights) + (source[p + 1] if lv.level == 0 else lv.scale * source[p + 1])
    dest[p + 1] = total * c_ref[kind(lv, edges, p, red)]


def relax(lv, edges, c_ref, other, source, dest, low, high, red):
    even = even_mask(lv.rows)
    loop(low, high, lambda p: relax_at(lv, edges, c_ref, other, source, dest, p, red, even), group(lv.rows))


def relax_zero(lv, edges, c_ref, source, dest, low, high):
    def body(p):
        dest[p + 1] = lv.scale * source[p + 1] * c_ref[kind(lv, edges, p, True)]

    loop(low, high, body, group(lv.rows))


def gap(lv, d, value, total):
    return d * value - total if lv.level == 0 else lv.inverse * (d * value - total)


def black_rest_at(lv, edges, c_ref, d_ref, red, source, dest, rest, p, even, weights=None):
    total = around(red, p, even, False, weights)
    g = source[p + 1]
    at = kind(lv, edges, p, False)
    value = (total + (g if lv.level == 0 else lv.scale * g)) * c_ref[at]
    dest[p + 1] = value
    rest[p + 1] = g - gap(lv, d_ref[jnp.minimum(at, 2)], value, total)


def relax_black_rest(lv, edges, c_ref, d_ref, red, source, dest, rest, low, high):
    even = even_mask(lv.rows)
    loop(low, high, lambda p: black_rest_at(lv, edges, c_ref, d_ref, red, source, dest, rest, p, even), group(lv.rows))


def red_rest(lv, edges, d_ref, source, red, black, p, even, weights=None):
    d = d_ref[jnp.minimum(kind(lv, edges, p, True), 2)]
    return source[p + 1] - gap(lv, d, red[p + 1], around(black, p, even, True, weights))


def clear_guards(*refs):
    for ref in refs:
        ref[0] = jnp.zeros(ref.shape[1:], F32)
        ref[ref.shape[0] - 1] = jnp.zeros(ref.shape[1:], F32)


def split_dot(value, weights):
    high = value.astype(BF16)
    low = (value - high.astype(F32)).astype(BF16)
    return jnp.dot(jnp.concatenate([high, low], axis=1), weights, preferred_element_type=F32)


def halving_weights(own_lanes):
    shape = (256, 128)
    fine = signed(rows_of(shape) & 127)
    coarse = signed(lanes_of(shape))
    hit = (fine >> 1) == coarse
    if own_lanes:
        hit = hit & (fine >= 0) & (fine < own_lanes)
    return jnp.where(hit, 0.125, 0.0).astype(BF16)


def doubling_weights(size, low, high):
    shape = (256, 256)
    coarse = signed(rows_of(shape) & 127)
    lane = lanes_of(shape)
    fine = signed(lane & 127)
    parent = fine >> 1
    beside = parent + jnp.where((fine & 1) == 1, 1, -1)
    beyond = ((beside == -1) & low) | ((beside == size) & high)
    centre = jnp.where(coarse == parent, 0.25, 0.0)
    neighbour = jnp.where(coarse == beside, 0.25, 0.0)
    mixed = jnp.where(beyond, 0.0, centre + neighbour)
    return jnp.where(lane < 128, mixed, centre).astype(BF16)


def rest_fold_at(lv, edges, d_ref, g_red, red, black, rest, low, z_ref, p, even, weights=None):
    z_ref[p - low] = fold_rows(rest[p + 1] + red_rest(lv, edges, d_ref, g_red, red, black, p, even, weights))


def restrict(lv, edges, d_ref, g_red, red, black, rest, low, count, z_ref, out_ref, weights):
    even = even_mask(lv.rows)
    loop(
        low, low + count,
        lambda p: rest_fold_at(lv, edges, d_ref, g_red, red, black, rest, low, z_ref, p, even), group(lv.rows),
    )
    halve(lv, count, z_ref, out_ref, weights)


def halve(lv, count, z_ref, out_ref, weights):
    half = lv.rows // 2
    chunk = max(c for c in range(1, count + 1) if count % c == 0 and (c * half <= 320 or c == 1))

    def product(n):
        value = z_ref[pl.ds(n * chunk, chunk)].reshape(chunk * half, 128)
        out_ref[pl.ds(n * chunk, chunk)] = split_dot(value, weights[...]).reshape(chunk, half, 128)

    loop(0, count // chunk, product)


def colour_planes(planes, pairs, red, black):
    even = even_mask(planes.shape[1])

    def body(p):
        low, high = planes[2 * p], planes[2 * p + 1]
        red[p + 1] = jnp.where(even, low, high)
        black[p + 1] = jnp.where(even, high, low)

    loop(0, pairs, body, 8)


def whole_planes(lv, red, black, pair_low, pairs, e_ref):
    even = even_mask(lv.rows)

    def body(t):
        r, b = red[pair_low + t + 1], black[pair_low + t + 1]
        e_ref[2 * t] = jnp.where(even, r, b)
        e_ref[2 * t + 1] = jnp.where(even, b, r)

    loop(0, pairs, body, 8)


def window_planes(lv, red, black, pair_low, pairs, row_low, natural, e_ref):
    even = even_mask(lv.rows)
    rows = e_ref.shape[1]

    def body(t):
        r, b = red[pair_low + t + 1], black[pair_low + t + 1]
        scatter_rows(natural, 2 * t, jnp.where(even, r, b))
        scatter_rows(natural, 2 * t + 1, jnp.where(even, b, r))

    def again(t):
        e_ref[t] = gather_rows(natural, t, rows, row_low)

    loop(0, pairs, body, 4)
    loop(0, 2 * pairs, again, 8)


def prolong(e_ref, count, plane_zero, size, edges, weights, mixed, plain):
    rows = e_ref.shape[1]
    chunk = max(c for c in range(1, count + 1) if count % c == 0 and (c * rows <= 320 or c == 1))

    def body(n):
        at = pl.ds(n * chunk, chunk)
        both = split_dot(e_ref[at].reshape(chunk * rows, 128), weights[...])
        mixed[at] = both[:, :128].reshape(chunk, rows, 128)
        plain[at] = both[:, 128:].reshape(chunk, rows, 128)

    loop(0, count // chunk, body)
    if plane_zero > 0:
        pl.when(edges.ilo)(lambda: plain.__setitem__(plane_zero - 1, -plain[plane_zero]))
    last = plane_zero + size - 1
    if last + 1 < count:
        pl.when(edges.ihi)(lambda: plain.__setitem__(last + 1, -plain[last]))


def correct(lv, edges, c_ref, kept, mixed, plain, row_zero, plane_zero, dest, low, high):
    body = correct_at(lv, edges, c_ref, kept, mixed, plain, row_zero, plane_zero, dest)
    loop(low, high, body, group(lv.rows))


def correct_at(lv, edges, c_ref, kept, mixed, plain, row_zero, plane_zero, dest):
    even = even_mask(lv.rows)
    half = lv.rows // 2
    row = cells_of((half, 128)) - row_zero
    at_low = (row == 0) & edges.jlo
    at_high = (row == lv.size // 2 - 1) & edges.jhi

    def body(p):
        t = p - lv.first + plane_zero
        value, near = plain[t], mixed[t]
        before = near + jnp.where(at_low, -value, row_before(value))
        after = near + jnp.where(at_high, -value, row_after(value))
        up, down = plain[t + 1], plain[t - 1]
        step = double_rows(before, after) + jnp.where(even, double_rows(up, up), double_rows(down, down))
        c = c_ref[kind(lv, edges, p, False)]
        dest[p + 1] = jnp.where(c > 0.0, kept[p + 1] + step, 0.0)

    return body


def compact_kernel(guess, source, x_ref, y_ref):
    even = ((rows_of((64, 64)) + lanes_of((64, 64))) & 1) == 0

    def body(u):
        blacks = []
        for s in range(2):
            p = 2 * u + s
            low, high = guess[2 * p], guess[2 * p + 1]
            f_low, f_high = source[2 * p], source[2 * p + 1]
            x_ref[p] = jnp.concatenate([jnp.where(even, high, low), jnp.where(even, f_low, f_high)], axis=1)
            blacks.append(jnp.where(even, f_high, f_low))
        y_ref[u] = jnp.concatenate(blacks, axis=1)

    loop(0, 16, body, 2)


def pack_kernel(ib, ia, x, y, jb, ja, xf, yf, ku, kd):
    zero = jnp.zeros((80, 128), F32)
    for p in range(3):
        xf[p, 8:72] = ib[p]
        xf[35 + p, 8:72] = ia[p]
    loop(0, 32, lambda p: xf.__setitem__((p + 3, slice(8, 72)), x[p]), 4)
    yf[0, 8:72] = ib[3]
    yf[17, 8:72] = ia[3]
    loop(0, 16, lambda p: yf.__setitem__((p + 1, slice(8, 72)), y[p]), 4)

    tile = jnp.zeros((8, 128), F32)
    for p in range(38):
        xf[p, 0:8] = tile
        xf[p, 3:8] = jb[5 * p : 5 * p + 5]
        xf[p, 72:80] = tile
        xf[p, 72:77] = ja[5 * p : 5 * p + 5]
    for p in range(18):
        yf[p, 0:8] = tile
        yf[p, 5:8] = jb[190 + 3 * p : 193 + 3 * p]
        yf[p, 72:80] = tile
        yf[p, 72:75] = ja[190 + 3 * p : 193 + 3 * p]
    for p in (38, 39):
        xf[p] = zero
    for p in range(18, 24):
        yf[p] = zero
    lane = lanes_of((80, 128))
    for u in range(5):
        down, up, up_y = zero, zero, zero
        for s in range(8):
            value = turn(xf[8 * u + s], 8 * s, 1)
            place = (lane - 8 * s) & 127
            down = jnp.where((place < 5) | ((place >= 64) & (place < 68)), value, down)
            up = jnp.where(((place >= 59) & (place < 64)) | (place >= 124), value, up)
            if 8 * u + s < 18:
                value = turn(yf[8 * u + s], 8 * s + 5, 1)
                down = jnp.where(place_y(lane, s, 0), value, down)
                up_y = jnp.where(place_y(lane, s, 61), value, up_y)
        kd[u] = down
        ku[u] = up + turn(up_y, -2, 1) if u < 3 else up


def place_y(lane, s, start):
    place = (lane - 8 * s - 5) & 63
    return (place >= start) & (place < start + 3)


def rows_kernel(ib, ia, guess_low, guess_high, source_low, source_high, up, down):
    even = even_natural((8, 64))
    for out, guess, source, low, x_at, y_at in (
        (down, guess_low, source_low, 0, 0, 0),
        (up, guess_high, source_high, 56, 3, 5),
    ):
        blacks = []
        for p in range(38):
            if 3 <= p < 35:
                n = 2 * p - 6
                first, second, f_first, f_second = guess[n], guess[n + 1], source[n], source[n + 1]
                value = jnp.concatenate(
                    [jnp.where(even, second, first), jnp.where(even, f_first, f_second)], axis=1
                )
                blacks.append(jnp.where(even, f_second, f_first))
            else:
                value = ib[p, low : low + 8] if p < 3 else ia[p - 35, low : low + 8]
            out[5 * p : 5 * p + 5] = value[x_at : x_at + 5]
        for p in range(18):
            if p == 0 or p == 17:
                value = (ib if p == 0 else ia)[3, low : low + 8]
            else:
                value = jnp.concatenate(blacks[2 * p - 2 : 2 * p], axis=1)
            out[190 + 3 * p : 193 + 3 * p] = value[y_at : y_at + 3]
        out[244:248] = jnp.zeros((4, 128), F32)


def spread_kernel(xf, yf, black, g_red, g_black, c_ref, d_ref, weights, lanes):
    set_coefficients(L0, block_edges(), c_ref, d_ref)
    weights[...] = halving_weights(64)
    lanes[...] = neighbour_weights()
    zero = jnp.zeros((80, 128), F32)
    own = lanes_of((80, 128)) < 64

    def first(p):
        value = gather_rows(xf, p, 80)
        black[p + 1] = jnp.where(own, value, 0.0)
        g_red[p + 1] = jnp.where(own, turn(value, 64, 1), 0.0)

    loop(0, 40, first, 4)

    def second(p):
        value = gather_rows(yf, p, 80)
        g_black[2 * p + 2] = jnp.where(own, value, 0.0)
        g_black[2 * p + 3] = jnp.where(own, turn(value, 64, 1), 0.0)

    loop(0, 18, second, 4)
    for q in (0, 1, 38, 39, 40, 41):
        g_black[q] = zero
    clear_guards(black, g_red)


def fine_kernel(
    black0, g_red0, g_black0, kb, ka, c_ref, d_ref, weights, lanes, v_black, g_red, g_black, low_quads, high_quads,
    black, red, rest, z_ref, planes, natural,
):
    edges = block_edges()
    zero = jnp.zeros((80, 128), F32)
    lane = lanes_of((80, 128))

    even = even_mask(80)

    def sides(u):
        below = jnp.where(edges.klo, 0.0, gather_rows(kb, u, 80))
        return below, jnp.where(edges.khi, 0.0, gather_rows(ka, u, 80))

    def merge(p):
        below, above = sides(p // 8)
        turned = 8 * (p % 8)
        place = (lane - turned) & 127
        edge = jnp.where(place < 5, above, jnp.where((place >= 59) & (place < 64), below, 0.0))
        black[p + 1] = black0[p + 1] + turn(edge, 64 - turned, 1)
        edge = jnp.where((place >= 64) & (place < 68), above, jnp.where(place >= 124, below, 0.0))
        g_red[p + 1] = g_red0[p + 1] + turn(edge, -turned, 1)

    def merge_black(n):
        below, above = sides(n // 8)
        below = turn(below, 2, 1)
        turned = 8 * (n % 8)
        place = (lane - turned) & 127
        edge = jnp.where((place >= 5) & (place < 8), above, jnp.where((place >= 66) & (place < 69), below, 0.0))
        g_black[2 * n + 2] = g_black0[2 * n + 2] + turn(edge, 59 - turned, 1)
        edge = jnp.where((place >= 69) & (place < 72), above, jnp.where((place >= 2) & (place < 5), below, 0.0))
        g_black[2 * n + 3] = g_black0[2 * n + 3] + turn(edge, -5 - turned, 1)

    for q in (0, 1, 38, 39, 40, 41):
        g_black[q] = zero
    for ref in (black, g_red):
        for q in (0, 39, 40, 41):
            ref[q] = zero
    for ref in (red, v_black):
        for q in (0, 1, 38, 39, 40, 41):
            ref[q] = zero
    for n in range(44):
        if n < 38:
            merge(n)
        if n % 2 == 0 and n < 36:
            merge_black(n // 2)
        if 1 <= n - 2 < 37:
            relax_at(L0, edges, c_ref, black, g_red, red, n - 2, True, even, lanes)
        if 1 <= n - 4 < 37:
            black_rest_at(L0, edges, c_ref, d_ref, red, g_black, v_black, rest, n - 4, even, lanes)
        if 3 <= n - 6 < 35:
            rest_fold_at(L0, edges, d_ref, g_red, red, v_black, rest, 3, z_ref, n - 6, even, lanes)
    halve(L0, 32, z_ref, planes, weights)

    def quad(q):
        total = planes[4 * q]
        for m in range(1, 4):
            total = total + turn(planes[4 * q + m], 32 * m, 1)
        scatter_rows(natural, q, total)
        return natural[q, 4:36]

    for q in range(4):
        low_quads[q] = quad(q)
        high_quads[q] = quad(q + 4)


def quad_rows(ib, ia, low_quads, high_quads, jb, ja, q):
    own = (ib, low_quads, high_quads, ia)[q // 4][q % 4]
    return jnp.concatenate([jb[q], own, ja[q]], axis=0)


def pack_quads_kernel(ib, ia, low_quads, high_quads, jb, ja, ku, kd):
    low_half = (lanes_of((64, 128)) & 31) < 16
    for u in range(8):
        first, second = (quad_rows(ib, ia, low_quads, high_quads, jb, ja, 2 * u + k) for k in range(2))
        kd[u] = turn(jnp.where(low_half, first, turn(second, 16, 1)), 32, 1)
        ku[u] = turn(jnp.where(low_half, turn(first, -16, 1), second), -32, 1)


def join_kernel(ib, ia, low_quads, high_quads, jb, ja, qf):
    for q in range(16):
        qf[q] = quad_rows(ib, ia, low_quads, high_quads, jb, ja, q)


WINDOWS = (L1, L2, L3_OWN, L3)
WHOLES = (L4, L5, L6)
DOUBLINGS = ((32, False), (16, False), (8, False), (4, False), (16, True), (8, True))


def geometry_kernel(after, *refs):
    edges, whole = block_edges(), whole_edges()
    for index, lv in enumerate(WINDOWS + WHOLES):
        set_coefficients(lv, edges if lv in WINDOWS else whole, refs[2 * index], refs[2 * index + 1])
    refs = refs[2 * len(WINDOWS + WHOLES) :]
    refs[0][...] = halving_weights(0)
    for n, (size, is_whole) in enumerate(DOUBLINGS):
        at = whole if is_whole else edges
        refs[1][n] = doubling_weights(size, at.klo, at.khi)


def middle_kernel(
    qf, kb, ka, c1, d1, c2, d2, c3, d3, weights, lanes, v1, gr1, gb1, v2, gr2, gb2, message,
    red1, y1, z1, p1, red2, y2, z2, p2, gr3, gb3, red3, black3, y3, z3, p3, natural,
):
    edges = block_edges()
    lane = lanes_of((64, 128))
    even = even_mask(64)

    def unpack(u):
        below = jnp.where(edges.klo, 0.0, gather_rows(kb, u, 64))
        above = jnp.where(edges.khi, 0.0, gather_rows(ka, u, 64))
        sides = ((turn(below, 16, 1), above), (below, turn(above, -16, 1)))
        for h in range(2):
            value = gather_rows(qf, 2 * u + h, 64)
            left, right = sides[h]
            for t in range(2):
                both = []
                for m in (2 * t, 2 * t + 1):
                    place = (lane - 32 * m) & 127
                    edge = jnp.where(place < 48, right, jnp.where(place >= 112, left, 0.0))
                    both.append(turn(jnp.where(place < 32, value, edge), -32 * m, 1))
                index = 4 * u + 2 * h + t
                gr1[index] = jnp.where(even, both[0], both[1])
                gb1[index] = jnp.where(even, both[1], both[0])

    clear_guards(red1, v1)
    for n in range(36):
        if n % 4 == 0 and n < 32:
            unpack(n // 4)
        p = n - 1
        if 0 <= p < 30:
            red1[p + 1] = L1.scale * gr1[p + 1] * c1[kind(L1, edges, p, True)]
        if 0 <= n - 3 < 30:
            black_rest_at(L1, edges, c1, d1, red1, gb1, v1, y1, n - 3, even, lanes)
        if 1 <= n - 5 < 29:
            rest_fold_at(L1, edges, d1, gr1, red1, v1, y1, 1, z1, n - 5, even, lanes)
    halve(L1, 28, z1, p1, weights)
    colour_planes(p1, 14, gr2, gb2)
    clear_guards(red2, v2, gr2, gb2)
    relax_zero(L2, edges, c2, gr2, red2, 0, 14)
    relax_black_rest(L2, edges, c2, d2, red2, gb2, v2, y2, 0, 14)
    restrict(L2, edges, d2, gr2, red2, v2, y2, 1, 12, z2, p2, weights)
    colour_planes(p2, 6, gr3, gb3)
    clear_guards(red3, black3)
    relax_zero(L3_OWN, edges, c3, gr3, red3, 0, 6)
    relax_black_rest(L3_OWN, edges, c3, d3, red3, gb3, black3, y3, 0, 6)
    restrict(L3_OWN, edges, d3, gr3, red3, black3, y3, 1, 4, z3, p3, weights)
    lane = lanes_of((8, 128))
    row = rows_of((8, 128))
    third = jnp.zeros((8, 128), F32)
    for i in range(8):
        scatter_rows(natural, i, p2[i + 2])
        third = third + turn(jnp.where(lane < 8, natural[i, 4:12], 0.0), 8 * i, 1)
    folded = third + turn(turn(third, 4, 0), 64, 1)
    blocks = jnp.zeros((8, 128), F32)
    for i in range(4):
        blocks = blocks + turn(jnp.where(lane < 4, p3[i], 0.0), 16 * i, 1)
    fourth = jnp.zeros((8, 128), F32)
    for r in range(4):
        fourth = jnp.where((lane & 15) >> 2 == r, turn(turn(blocks, 4 * r, 1), -2 - r, 0), fourth)

    def store(n):
        for r in range(4):
            message[n, r] = folded[r : r + 1]
        message[n, 4] = fourth[0:1]

    loop(0, 64, store, 8)


def plane_kernel(tiles, message, near, rows, grid, blocks):
    x, y, z = (lax.axis_index(axis) for axis in ("gx", "gy", "gz"))
    shape = (8, 128)
    lane, row = lanes_of(shape), rows_of(shape)

    for n in range(64):
        rows[n : n + 1] = tiles[n, 4]
    parts = [jnp.zeros(shape, F32)] * 4
    for n in range(8):
        value = rows[pl.ds(n, 8, stride=8), :]
        here = (lane & 31) >> 2 == n
        for r in range(4):
            index = (lane >> 5) * 16 + 4 * r + (lane & 3)
            parts[r] = jnp.where(here, jnp.take_along_axis(value, index, axis=1), parts[r])
    for r in range(4):
        grid[pl.ds(r, 8, stride=4), :] = parts[r]

    lane = signed(lane)
    for dy in range(3):
        sides = []
        for dz in range(3):
            yy, zz = y + (dy - 1), z + (dz - 1)
            inside = (yy >= 0) & (yy < COUNT) & (zz >= 0) & (zz < COUNT)
            index = jnp.clip(yy, 0, COUNT - 1) * COUNT + jnp.clip(zz, 0, COUNT - 1)
            for r in range(4):
                blocks[3 * dy + dz, r : r + 1] = tiles[index, r]
            value = blocks[3 * dy + dz]
            value = jnp.where(row < 4, value, turn(turn(value, 4, 0), 64, 1))
            sides.append(jnp.where(inside, value, 0.0))
        for i in range(8):
            total = jnp.zeros(shape, F32)
            for dz in range(3):
                hit = (lane >= 8 * (dz - 1)) & (lane < 8 * dz)
                total = jnp.where(hit, turn(sides[dz], 8 * (dz - 1) - 8 * i, 1), total)
            near[i, 8 * dy : 8 * dy + 8] = total

    wide = lanes_of((24, 128))
    ends = []
    for first in (2, 0):
        total = jnp.zeros((24, 128), F32)
        for n in range(6):
            hit = (wide >= 20 * n) & (wide < 20 * n + 20)
            total = jnp.where(hit, turn(near[first + n], 20 * n + 6, 1), total)
        ends.append(total)
    for n in range(COUNT):
        message[n, 0:32] = grid[...]
        message[n, 32:56] = jnp.where(x < n, ends[0], ends[1])


def coarse_kernel(
    tiles, near, v2, gr2, gb2, v1, gr1, gb1, v0, gr0, gb0, c0, d0, c1, c2, c3, c4, d4, c5, d5, c6, halving, doubling, lanes, out, rest,
    gr4, gb4, red4, v4, y4, z4, p4, gr5, gb5, red5, v5, y5, z5, p5, gr6, gb6, red6, v6, full,
    gr3, gb3, red3, v3, b3, b2, red2, b1, red1, b0, red0, y0, e_ref, mixed, plain, fine_mixed, fine_plain, natural, last, out_held, rest_held, sems,
):
    edges = block_edges()
    whole = whole_edges()
    x, y, z = (lax.axis_index(axis) for axis in ("gx", "gy", "gz"))

    lane = signed(lanes_of((24, 128)))
    even = even_natural((24, 128))
    empty = jnp.zeros((24, 128), F32)

    def put(index, low, high):
        natural[index, 0:24] = jnp.where(even, low, high)
        natural[index + 12, 0:24] = jnp.where(even, high, low)

    for n in range(4):
        put(4 + n, near[2 * n], near[2 * n + 1])
    put(0, empty, empty)
    put(11, empty, empty)
    for at, first in ((x - 1, 1), (x + 1, 8)):
        inside = (at >= 0) & (at < COUNT)
        value = jnp.where(inside, tiles[jnp.clip(at, 0, COUNT - 1), 32:56], 0.0)
        planes = [jnp.where((lane >= -6) & (lane < 14), turn(value, -20 * n - 6, 1), 0.0) for n in range(6)]
        for n in range(3):
            put(first + n, planes[2 * n], planes[2 * n + 1])
    for n in range(24):
        natural[n, 24:32] = jnp.zeros((8, 128), F32)
    for n in range(12):
        gr3[n + 1] = gather_rows(natural, n, 32)
        gb3[n + 1] = gather_rows(natural, n + 12, 32)
    clear_guards(red3, v3)
    relax_zero(L3, edges, c3, gr3, red3, 0, 12)
    relax(L3, edges, c3, red3, gb3, v3, 0, 12, False)

    lane = lanes_of((32, 128))
    even32 = even_mask(32)
    zero = jnp.zeros((8, 128), F32)

    def place(n):
        value = gather_rows(tiles, n, 32)
        for t in range(2):
            low = jnp.where(lane < 32, turn(value, -64 * t, 1), 0.0)
            high = jnp.where(lane < 32, turn(value, -64 * t - 32, 1), 0.0)
            index = 2 * n + t + 1
            gr4[index] = jnp.where(even32, low, high)
            gb4[index] = jnp.where(even32, high, low)

    loop(0, 8, place, 4)
    clear_guards(red4, v4, gr4, gb4)
    relax_zero(L4, whole, c4, gr4, red4, 0, 16)
    relax_black_rest(L4, whole, c4, d4, red4, gb4, v4, y4, 0, 16)
    restrict(L4, whole, d4, gr4, red4, v4, y4, 0, 16, z4, p4, halving)
    colour_planes(p4, 8, gr5, gb5)
    clear_guards(red5, v5, gr5, gb5)
    relax_zero(L5, whole, c5, gr5, red5, 0, 8)
    relax_black_rest(L5, whole, c5, d5, red5, gb5, v5, y5, 0, 8)
    restrict(L5, whole, d5, gr5, red5, v5, y5, 0, 8, z5, p5, halving)
    colour_planes(p5, 4, gr6, gb6)
    clear_guards(red6, v6)
    relax_zero(L6, whole, c6, gr6, red6, 0, 4)
    relax(L6, whole, c6, red6, gb6, v6, 0, 4, False)
    for _ in range(COARSE_SWEEPS - 1):
        relax(L6, whole, c6, v6, gr6, red6, 0, 4, True)
        relax(L6, whole, c6, red6, gb6, v6, 0, 4, False)

    def ascend(coarse, fine, c, w, coarse_red, coarse_black, kept, g_red, g_black, red):
        count = coarse.size
        e, rows = e_ref.at[0:count, 0:count], slice(0, count)
        n, p = mixed.at[0 : count + 2, rows], plain.at[0 : count + 2, rows]
        whole_planes(coarse, coarse_red, coarse_black, 0, coarse.pairs, e)
        prolong(e, count, 0, count, whole, w, mixed.at[1 : count + 1, rows], plain.at[1 : count + 1, rows])
        p[0] = -p[1]
        p[count + 1] = -p[count]
        correct(fine, whole, c, kept, n, p, 0, 1, kept, 0, fine.pairs)
        relax(fine, whole, c, kept, g_red, red, 0, fine.pairs, True)
        relax(fine, whole, c, red, g_black, kept, 0, fine.pairs, False)

    ascend(L6, L5, c5, doubling.at[5], red6, v6, v5, gr5, gb5, red5)
    ascend(L5, L4, c4, doubling.at[4], red5, v5, v4, gr4, gb4, red4)

    even = even_mask(32)
    for t in (0, 1, 2, 3, 36, 37, 38, 39):
        full[t] = jnp.zeros((48, 128), F32)

    def expand(t):
        r, b = red4[t + 1], v4[t + 1]
        for n, value in ((2 * t + 4, jnp.where(even, r, b)), (2 * t + 5, jnp.where(even, b, r))):
            full[n, 0:8] = zero
            scatter_rows(full, n, value, 8)
            full[n, 40:48] = zero

    loop(0, 16, expand, 4)

    def cut(t):
        rows = gather_rows(full, 4 * x + t, 16, 4 * y + 4)
        e_ref[t, 0:16] = pltpu.roll(rows, (128 - 4 * z) & 127, 1)

    loop(0, 12, cut)

    def lift(index, fine, c, count, rows, plane_zero, row_zero, size, kept, dest, low, high):
        e = e_ref.at[0:count, 0:rows]
        n, p = mixed.at[0:count, 0:rows], plain.at[0:count, 0:rows]
        prolong(e, count, plane_zero, size, edges, doubling.at[index], n, p)
        correct(fine, edges, c, kept, n, p, row_zero, plane_zero, dest, low, high)

    def smooth(lv, c, black, g_red, g_black, red, low, high, low2, high2):
        relax(lv, edges, c, black, g_red, red, low, high, True)
        relax(lv, edges, c, red, g_black, black, low2, high2, False)

    lift(3, L3, c3, 12, 16, 4, 4, 4, v3, b3, 1, 11)
    clear_guards(b3, red3)
    smooth(L3, c3, b3, gr3, gb3, red3, 2, 10, 2, 10)

    window_planes(L3, red3, b3, 2, 8, 4, natural.at[0:16, 0:32], e_ref.at[0:16, 0:16])
    lift(2, L2, c2, 16, 16, 4, 4, 8, v2, b2, 0, 14)
    clear_guards(b2, red2)
    smooth(L2, c2, b2, gr2, gb2, red2, 1, 13, 1, 13)

    whole_planes(L2, red2, b2, 1, 12, e_ref.at[0:24, 0:32])
    e = e_ref.at[0:24, 0:32]
    n, p = mixed.at[0:24, 0:32], plain.at[0:24, 0:32]
    prolong(e, 24, 4, 16, edges, doubling.at[1], n, p)
    correct1 = correct_at(L1, edges, c1, v1, n, p, 8, 4, b1)
    for index in (5, 26):
        b1[index] = jnp.zeros(b1.shape[1:], F32)
    even1 = even_mask(64)
    even0 = even_mask(80)
    mixed0, plain0 = fine_mixed, fine_plain
    correct0 = correct_at(L0, edges, c0, v0, mixed0, plain0, 4, 4, b0)
    b0[1] = jnp.zeros(b0.shape[1:], F32)
    b0[38] = jnp.zeros(b0.shape[1:], F32)
    copies = []

    def send(held, target, n):
        copy = pltpu.make_async_copy(held.at[pl.ds(8 * n, 8)], target.at[pl.ds(8 * n, 8)], sems.at[len(copies)])
        copy.start()
        copies.append(copy)

    def store(held, p, r, b):
        for n, value in ((0, jnp.where(even0, r, b)), (1, jnp.where(even0, b, r))):
            scatter_rows(last, 2 * (p & 7) + n, value)
            held[2 * p - 6 + n] = last[2 * (p & 7) + n, 8:72, 0:64]

    def coarse_step(n):
        if n < 25:
            correct1(n)
        if 5 <= n - 2 < 25:
            relax_at(L1, edges, c1, b1, gr1, red1, n - 2, True, even1, lanes)
        if 6 <= n - 4 < 24:
            relax_at(L1, edges, c1, red1, gb1, b1, n - 4, False, even1)

    def lift_planes(c):
        planes = []
        for t in range(4 * c, 4 * c + 4):
            r, b = red1[t + 6], b1[t + 6]
            scatter_rows(natural, 2 * t, jnp.where(even1, r, b))
            scatter_rows(natural, 2 * t + 1, jnp.where(even1, b, r))
            planes += [gather_rows(natural, 2 * t + k, 40, 12) for k in range(2)]
        both = split_dot(jnp.concatenate(planes, axis=0), doubling[0])
        for k in range(8):
            mixed0[8 * c + k] = both[40 * k : 40 * k + 40, :128]
            plain0[8 * c + k] = both[40 * k : 40 * k + 40, 128:]
        if c == 0:
            plain0[3] = jnp.where(edges.ilo, -plain0[4], plain0[3])
        if c == 4:
            plain0[36] = jnp.where(edges.ihi, -plain0[35], plain0[36])

    def fine_step(n):
        if n < 37:
            correct0(n)
        if 1 <= n - 2 < 37:
            relax_at(L0, edges, c0, b0, gr0, red0, n - 2, True, even0, lanes)
        p = n - 4
        if 2 <= p < 36:
            black_rest_at(L0, edges, c0, d0, red0, gb0, b0, y0, p, even0)
        if 3 <= p < 35:
            store(out_held, p, red0[p + 1], b0[p + 1])
            if p % 4 == 2:
                send(out_held, out, p // 4 - 1)
        p = n - 6
        if 3 <= p < 35:
            store(rest_held, p, red_rest(L0, edges, d0, gr0, red0, b0, p, even0), y0[p + 1])
            if p % 4 == 2:
                send(rest_held, rest, p // 4 - 1)

    done, ready = 0, 0
    for n in range(5, 29):
        coarse_step(n)
        for _ in range(2):
            if done < ready:
                done += 1
                fine_step(done)
        if n >= 12 and n % 4 == 0:
            lift_planes(n // 4 - 3)
            ready = 2 * n - 19
    for n in range(done + 1, 43):
        fine_step(n)
    for copy in copies:
        copy.wait()


def struct(*shape):
    return jax.ShapeDtypeStruct(shape, F32)


def call(kernel, outs, scratch, flops=2_000_000, out_space=pltpu.VMEM, semaphores=0):
    space = pl.BlockSpec(memory_space=pltpu.VMEM)
    extra = [pltpu.SemaphoreType.DMA((semaphores,))] if semaphores else []

    def run(*args):
        return pl.pallas_call(
            kernel,
            out_shape=outs,
            in_specs=[space] * len(args),
            out_specs=[pl.BlockSpec(memory_space=out_space)] * len(outs),
            scratch_shapes=[pltpu.VMEM(shape, F32) for shape in scratch] + extra,
            compiler_params=pltpu.CompilerParams(vmem_limit_bytes=40 * 2**20),
            cost_estimate=pl.CostEstimate(flops=flops, bytes_accessed=1_000_000, transcendentals=0),
        )(*args)

    return run


def pair(to_next, to_before, axis, ring=False):
    up = [(i, (i + 1) % COUNT) for i in range(COUNT if ring else COUNT - 1)]
    down = [(j, i) for i, j in up]
    after = lax.ppermute(to_before, axis, down)
    before = lax.ppermute(to_next, axis, up)
    return before, after


def face(guess, source, start, first):
    even = ((lax.broadcasted_iota(jnp.int32, (64, 64), 0) + lax.broadcasted_iota(jnp.int32, (64, 64), 1)) & 1) == 0
    low, high = guess[start : start + 6 : 2], guess[start + 1 : start + 6 : 2]
    f_low, f_high = source[start : start + 6 : 2], source[start + 1 : start + 6 : 2]
    red = jnp.where(even, f_low, f_high)
    black = jnp.where(even, f_high, f_low)
    mixed = jnp.concatenate([jnp.where(even, high, low), red], axis=2)
    return jnp.concatenate([mixed, jnp.concatenate([black[first : first + 1], black[first + 1 : first + 2]], axis=2)], axis=0)


def coefficient_shapes(*levels):
    shapes = []
    for lv in levels:
        shapes += [struct(4, lv.rows, 128), struct(3, lv.rows, 128)]
    return shapes


def per_device(right_side, guess):
    ib, ia = pair(face(guess, right_side, 58, 1), face(guess, right_side, 0, 0), "gx")
    x, y = call(compact_kernel, (struct(32, 64, 128), struct(16, 64, 128)), [])(guess, right_side)

    up, down = call(rows_kernel, (struct(248, 128), struct(248, 128)), [])(
        ib, ia, guess[:, 0:8], guess[:, 56:64], right_side[:, 0:8], right_side[:, 56:64]
    )
    jb, ja = pair(up, down, "gy")
    xf, yf, ku, kd = call(
        pack_kernel, (struct(40, 80, 128), struct(24, 80, 128), struct(5, 80, 128), struct(5, 80, 128)), []
    )(ib, ia, x, y, jb, ja)
    kb, ka = pair(ku, kd, "gz", True)
    fine = L0.shape()
    field = struct(*fine)
    weights = jax.ShapeDtypeStruct((256, 128), BF16)
    black, g_red, g_black, c0, d0, w0, lanes = call(
        spread_kernel, (field, field, field, *coefficient_shapes(L0), weights, weights), []
    )(xf, yf)
    v0, gr0, gb0, low_quads, high_quads = call(
        fine_kernel,
        (field, field, field, struct(4, 32, 128), struct(4, 32, 128)),
        [fine, fine, fine, (32, 40, 128), (32, 40, 128), (8, 40, 128)],
    )(black, g_red, g_black, kb, ka, c0, d0, w0, lanes)

    ib, ia = pair(high_quads, low_quads, "gx")
    shapes = coefficient_shapes(*WINDOWS, *WHOLES) + [weights, jax.ShapeDtypeStruct((6, 256, 256), BF16)]
    c1, d1, c2, d2, c3o, d3o, c3, _, c4, d4, c5, d5, c6, _, halving, doubling = call(
        geometry_kernel, tuple(shapes), []
    )(low_quads)

    def quad_ends(low):
        return jnp.concatenate([part[:, low : low + 16] for part in (ib, low_quads, high_quads, ia)], axis=0)

    jb, ja = pair(quad_ends(16), quad_ends(0), "gy")
    parts = (ib, ia, low_quads, high_quads, jb, ja)
    ku, kd = call(pack_quads_kernel, (struct(8, 64, 128), struct(8, 64, 128)), [])(*parts)
    kb, ka = pair(ku, kd, "gz", True)
    (qf,) = call(join_kernel, (struct(16, 64, 128),), [])(*parts)
    s1, s2, s3 = L1.shape(), L2.shape(), L3_OWN.shape()
    v1, gr1, gb1, v2, gr2, gb2, message = call(
        middle_kernel,
        tuple(struct(*s) for s in (s1, s1, s1, s2, s2, s2, (64, 5, 1, 128))),
        [s1, s1, (28, 32, 128), (28, 32, 128), s2, s2, (12, 16, 128), (12, 16, 128)]
        + [s3, s3, s3, s3, s3, (4, 8, 128), (4, 8, 128), (8, 16, 128)],
    )(qf, kb, ka, c1, d1, c2, d2, c3o, d3o, halving, lanes)

    tiles = lax.all_to_all(message, ("gy", "gz"), 0, 0)
    message, near = call(
        plane_kernel, (struct(8, 56, 128), struct(8, 24, 128)), [(64, 128), (32, 128), (9, 8, 128)]
    )(tiles)
    tiles = lax.all_to_all(message, "gx", 0, 0)
    s3, s4, s5, s6 = L3.shape(), L4.shape(), L5.shape(), L6.shape()
    return tuple(
        call(
            coarse_kernel,
            (struct(64, 64, 64), struct(64, 64, 64)),
            [s4, s4, s4, s4, s4, (16, 16, 128), (16, 16, 128)]
            + [s5, s5, s5, s5, s5, (8, 8, 128), (8, 8, 128)]
            + [s6, s6, s6, s6, (40, 48, 128)]
            + [s3, s3, s3, s3, s3, s2, s2, s1, s1, fine, fine, fine]
            + [(42, 40, 128), (42, 40, 128), (42, 40, 128), (40, 40, 128), (40, 40, 128), (40, 64, 128), (16, 80, 128), (64, 64, 64), (64, 64, 64)],
            out_space=pl.ANY,
            semaphores=16,
        )(tiles, near, v2, gr2, gb2, v1, gr1, gb1, v0, gr0, gb0, c0, d0, c1, c2, c3, c4, d4, c5, d5, c6, halving, doubling, lanes)
    )


def solution(mesh):
    return jax.shard_map(
        per_device,
        mesh=mesh,
        in_specs=(P("gx", "gy", "gz"), P("gx", "gy", "gz")),
        out_specs=(P("gx", "gy", "gz"), P("gx", "gy", "gz")),
        check_vma=False,
    )
```

```python
import typing

import jax
import jax.numpy as jnp
from jax import lax
from jax.experimental import pallas as pl
from jax.experimental.pallas import tpu as pltpu
from jax.sharding import PartitionSpec as P


F32 = jnp.float32
BF16 = jnp.bfloat16
COARSE_SWEEPS = 4
COUNT = 8


class Level(typing.NamedTuple):
    level: int
    pairs: int
    rows: int
    first: int
    offset: int
    size: int

    @property
    def scale(self):
        return 4.0**self.level

    @property
    def inverse(self):
        return 0.25**self.level

    @property
    def own(self):
        return self.size // 2

    def shape(self):
        return (self.pairs + 2, self.rows, 128)


L0 = Level(0, 40, 80, 3, 8, 64)
L1 = Level(1, 30, 64, 7, 16, 32)
L2 = Level(2, 14, 32, 3, 8, 16)
L3_OWN = Level(3, 6, 16, 1, 4, 8)
L3 = Level(3, 12, 32, 4, 8, 8)
L4 = Level(4, 16, 32, 0, 0, 32)
L5 = Level(5, 8, 16, 0, 0, 16)
L6 = Level(6, 4, 8, 0, 0, 8)


class Edges(typing.NamedTuple):
    ilo: typing.Any
    ihi: typing.Any
    jlo: typing.Any
    jhi: typing.Any
    klo: typing.Any
    khi: typing.Any


def block_edges():
    ends = []
    for axis in ("gx", "gy", "gz"):
        place = lax.axis_index(axis)
        ends += [place == 0, place == COUNT - 1]
    return Edges(*ends)


def whole_edges():
    yes = lax.axis_index("gx") >= 0
    return Edges(*([yes] * 6))


def lanes_of(shape):
    return lax.broadcasted_iota(jnp.int32, shape, len(shape) - 1)


def rows_of(shape):
    return lax.broadcasted_iota(jnp.int32, shape, len(shape) - 2)


def signed(lane):
    return jnp.where(lane < 96, lane, lane - 128)


def cells_of(shape):
    row = rows_of(shape)
    return (row & 7) * (shape[-2] // 8) + (row >> 3)


def even_mask(rows):
    shape = (rows, 128)
    return ((cells_of(shape) + lanes_of(shape)) & 1) == 0


def even_natural(shape):
    return ((rows_of(shape) + lanes_of(shape)) & 1) == 0


def gather_rows(ref, index, rows, start=0):
    stride = rows // 8
    if stride == 1:
        return ref[index, pl.ds(start, 8), :]
    return jnp.concatenate([ref[index, pl.ds(start + t, 8, stride=stride), :] for t in range(stride)], axis=0)


def scatter_rows(ref, index, value, start=0):
    stride = value.shape[0] // 8
    for t in range(stride):
        ref[index, pl.ds(start + t, 8, stride=stride), :] = value[8 * t : 8 * t + 8]


def row_before(value):
    last = value[value.shape[0] - 8 :]
    first = jnp.where(rows_of((8, 128)) == 0, 0.0, pltpu.roll(last, 1, 0))
    return first if value.shape[0] == 8 else jnp.concatenate([first, value[: value.shape[0] - 8]], axis=0)


def row_after(value):
    last = jnp.where(rows_of((8, 128)) == 7, 0.0, pltpu.roll(value[:8], 7, 0))
    return last if value.shape[0] == 8 else jnp.concatenate([value[8:], last], axis=0)


def fold_rows(value):
    tiles = value.shape[0] // 16
    if tiles == 0:
        raise ValueError("rows")
    return jnp.concatenate([value[16 * t : 16 * t + 8] + value[16 * t + 8 : 16 * t + 16] for t in range(tiles)], axis=0)


def double_rows(even, odd):
    parts = []
    for t in range(even.shape[0] // 8):
        parts += [even[8 * t : 8 * t + 8], odd[8 * t : 8 * t + 8]]
    return jnp.concatenate(parts, axis=0)


def turn(value, shift, axis):
    size = value.shape[axis]
    if isinstance(shift, int):
        shift %= size
        if shift == 0:
            return value
    return pltpu.roll(value, shift, axis)


def bounds(low, high, size):
    return jnp.where(low, 0, -4096), jnp.where(high, size, 4096)


def set_coefficients(lv, edges, c_ref, d_ref):
    shape = (lv.rows, 128)
    row = cells_of(shape) - lv.offset
    lane = signed(lanes_of(shape))
    row_low, row_high = bounds(edges.jlo, edges.jhi, lv.size)
    lane_low, lane_high = bounds(edges.klo, edges.khi, lv.size)
    inside = (row >= row_low) & (row < row_high) & (lane >= lane_low) & (lane < lane_high)
    diagonal = 6.0 + jnp.where(row == row_low, 1.0, 0.0) + jnp.where(row == row_high - 1, 1.0, 0.0)
    diagonal = diagonal + jnp.where(lane == lane_low, 1.0, 0.0) + jnp.where(lane == lane_high - 1, 1.0, 0.0)
    even = jnp.where(even_mask(lv.rows), 1.0, 0.0)
    for index, extra in enumerate((0.0, even, 1.0 - even)):
        d_ref[index] = diagonal + extra
        c_ref[index] = jnp.where(inside, 1.0 / (diagonal + extra), 0.0)
    c_ref[3] = jnp.zeros(shape, F32)


def kind(lv, edges, p, red):
    last = lv.first + lv.own - 1
    low, high = (1, 2) if red else (2, 1)
    if isinstance(p, int):
        if p in (lv.first, last):
            return jnp.where(edges.ilo, low, 0) if p == lv.first else jnp.where(edges.ihi, high, 0)
        return 0 if lv.first < p < last else jnp.where(edges.ilo if p < lv.first else edges.ihi, 3, 0)
    inner = jnp.where((p == lv.first) & edges.ilo, low, jnp.where((p == last) & edges.ihi, high, 0))
    return jnp.where(((p < lv.first) & edges.ilo) | ((p > last) & edges.ihi), 3, inner)


def loop(low, high, body, width=0):
    count = high - low
    width = count if width == 0 else min(width, count)

    def step(n, carry):
        for k in range(width):
            body(low + n * width + k)
        return carry

    if count // width > 1:
        lax.fori_loop(0, count // width, step, 0)
        done = count // width * width
    else:
        done = 0
    for p in range(low + done, high):
        body(p)


def group(rows):
    return max(1, 180 // (rows // 8))


def neighbour_weights():
    shape = (256, 128)
    apart = ((rows_of(shape) & 127) - lanes_of(shape)) & 127
    return jnp.where((apart == 1) | (apart == 127), 1.0, 0.0).astype(BF16)


def lane_sum(value, weights):
    rows = value.shape[0]
    part = rows if weights is None else 16
    total = turn(value[:part], 1, 1) + turn(value[:part], 127, 1)
    return total if part == rows else jnp.concatenate([total, split_dot(value[part:], weights[...])], axis=0)


def around(ref, p, even, red, weights=None):
    value = ref[p + 1]
    before, after = ref[p], ref[p + 2]
    total = value + (jnp.where(even, before, after) if red else jnp.where(even, after, before))
    total = total + (row_before(value) + row_after(value))
    return total + lane_sum(value, weights)


def relax_at(lv, edges, c_ref, other, source, dest, p, red, even, weights=None):
    total = around(other, p, even, red, weights) + (source[p + 1] if lv.level == 0 else lv.scale * source[p + 1])
    dest[p + 1] = total * c_ref[kind(lv, edges, p, red)]


def relax(lv, edges, c_ref, other, source, dest, low, high, red):
    even = even_mask(lv.rows)
    loop(low, high, lambda p: relax_at(lv, edges, c_ref, other, source, dest, p, red, even), group(lv.rows))


def relax_zero(lv, edges, c_ref, source, dest, low, high):
    def body(p):
        dest[p + 1] = lv.scale * source[p + 1] * c_ref[kind(lv, edges, p, True)]

    loop(low, high, body, group(lv.rows))


def gap(lv, d, value, total):
    return d * value - total if lv.level == 0 else lv.inverse * (d * value - total)


def black_rest_at(lv, edges, c_ref, d_ref, red, source, dest, rest, p, even, weights=None):
    total = around(red, p, even, False, weights)
    g = source[p + 1]
    at = kind(lv, edges, p, False)
    value = (total + (g if lv.level == 0 else lv.scale * g)) * c_ref[at]
    dest[p + 1] = value
    rest[p + 1] = g - gap(lv, d_ref[jnp.minimum(at, 2)], value, total)


def relax_black_rest(lv, edges, c_ref, d_ref, red, source, dest, rest, low, high):
    even = even_mask(lv.rows)
    loop(low, high, lambda p: black_rest_at(lv, edges, c_ref, d_ref, red, source, dest, rest, p, even), group(lv.rows))


def red_rest(lv, edges, d_ref, source, red, black, p, even, weights=None):
    d = d_ref[jnp.minimum(kind(lv, edges, p, True), 2)]
    return source[p + 1] - gap(lv, d, red[p + 1], around(black, p, even, True, weights))


def clear_guards(*refs):
    for ref in refs:
        ref[0] = jnp.zeros(ref.shape[1:], F32)
        ref[ref.shape[0] - 1] = jnp.zeros(ref.shape[1:], F32)


def split_dot(value, weights):
    high = value.astype(BF16)
    low = (value - high.astype(F32)).astype(BF16)
    return jnp.dot(jnp.concatenate([high, low], axis=1), weights, preferred_element_type=F32)


def halving_weights(own_lanes):
    shape = (256, 128)
    fine = signed(rows_of(shape) & 127)
    coarse = signed(lanes_of(shape))
    hit = (fine >> 1) == coarse
    if own_lanes:
        hit = hit & (fine >= 0) & (fine < own_lanes)
    return jnp.where(hit, 0.125, 0.0).astype(BF16)


def doubling_weights(size, low, high):
    shape = (256, 256)
    coarse = signed(rows_of(shape) & 127)
    lane = lanes_of(shape)
    fine = signed(lane & 127)
    parent = fine >> 1
    beside = parent + jnp.where((fine & 1) == 1, 1, -1)
    beyond = ((beside == -1) & low) | ((beside == size) & high)
    centre = jnp.where(coarse == parent, 0.25, 0.0)
    neighbour = jnp.where(coarse == beside, 0.25, 0.0)
    mixed = jnp.where(beyond, 0.0, centre + neighbour)
    return jnp.where(lane < 128, mixed, centre).astype(BF16)


def rest_fold_at(lv, edges, d_ref, g_red, red, black, rest, low, z_ref, p, even, weights=None):
    z_ref[p - low] = fold_rows(rest[p + 1] + red_rest(lv, edges, d_ref, g_red, red, black, p, even, weights))


def restrict(lv, edges, d_ref, g_red, red, black, rest, low, count, z_ref, out_ref, weights):
    even = even_mask(lv.rows)
    loop(
        low, low + count,
        lambda p: rest_fold_at(lv, edges, d_ref, g_red, red, black, rest, low, z_ref, p, even), group(lv.rows),
    )
    halve(lv, count, z_ref, out_ref, weights)


def halve(lv, count, z_ref, out_ref, weights):
    half = lv.rows // 2
    chunk = max(c for c in range(1, count + 1) if count % c == 0 and (c * half <= 320 or c == 1))

    def product(n):
        value = z_ref[pl.ds(n * chunk, chunk)].reshape(chunk * half, 128)
        out_ref[pl.ds(n * chunk, chunk)] = split_dot(value, weights[...]).reshape(chunk, half, 128)

    loop(0, count // chunk, product)


def colour_planes(planes, pairs, red, black):
    even = even_mask(planes.shape[1])

    def body(p):
        low, high = planes[2 * p], planes[2 * p + 1]
        red[p + 1] = jnp.where(even, low, high)
        black[p + 1] = jnp.where(even, high, low)

    loop(0, pairs, body, 8)


def whole_planes(lv, red, black, pair_low, pairs, e_ref):
    even = even_mask(lv.rows)

    def body(t):
        r, b = red[pair_low + t + 1], black[pair_low + t + 1]
        e_ref[2 * t] = jnp.where(even, r, b)
        e_ref[2 * t + 1] = jnp.where(even, b, r)

    loop(0, pairs, body, 8)


def window_planes(lv, red, black, pair_low, pairs, row_low, natural, e_ref):
    even = even_mask(lv.rows)
    rows = e_ref.shape[1]

    def body(t):
        r, b = red[pair_low + t + 1], black[pair_low + t + 1]
        scatter_rows(natural, 2 * t, jnp.where(even, r, b))
        scatter_rows(natural, 2 * t + 1, jnp.where(even, b, r))

    def again(t):
        e_ref[t] = gather_rows(natural, t, rows, row_low)

    loop(0, pairs, body, 4)
    loop(0, 2 * pairs, again, 8)


def prolong(e_ref, count, plane_zero, size, edges, weights, mixed, plain):
    rows = e_ref.shape[1]
    chunk = max(c for c in range(1, count + 1) if count % c == 0 and (c * rows <= 320 or c == 1))

    def body(n):
        at = pl.ds(n * chunk, chunk)
        both = split_dot(e_ref[at].reshape(chunk * rows, 128), weights[...])
        mixed[at] = both[:, :128].reshape(chunk, rows, 128)
        plain[at] = both[:, 128:].reshape(chunk, rows, 128)

    loop(0, count // chunk, body)
    if plane_zero > 0:
        pl.when(edges.ilo)(lambda: plain.__setitem__(plane_zero - 1, -plain[plane_zero]))
    last = plane_zero + size - 1
    if last + 1 < count:
        pl.when(edges.ihi)(lambda: plain.__setitem__(last + 1, -plain[last]))


def correct(lv, edges, c_ref, kept, mixed, plain, row_zero, plane_zero, dest, low, high):
    body = correct_at(lv, edges, c_ref, kept, mixed, plain, row_zero, plane_zero, dest)
    loop(low, high, body, group(lv.rows))


def correct_at(lv, edges, c_ref, kept, mixed, plain, row_zero, plane_zero, dest):
    even = even_mask(lv.rows)
    half = lv.rows // 2
    row = cells_of((half, 128)) - row_zero
    at_low = (row == 0) & edges.jlo
    at_high = (row == lv.size // 2 - 1) & edges.jhi

    def body(p):
        t = p - lv.first + plane_zero
        value, near = plain[t], mixed[t]
        before = near + jnp.where(at_low, -value, row_before(value))
        after = near + jnp.where(at_high, -value, row_after(value))
        up, down = plain[t + 1], plain[t - 1]
        step = double_rows(before, after) + jnp.where(even, double_rows(up, up), double_rows(down, down))
        c = c_ref[kind(lv, edges, p, False)]
        dest[p + 1] = jnp.where(c > 0.0, kept[p + 1] + step, 0.0)

    return body


def compact_kernel(guess, source, x_ref, y_ref):
    even = ((rows_of((64, 64)) + lanes_of((64, 64))) & 1) == 0

    def body(u):
        blacks = []
        for s in range(2):
            p = 2 * u + s
            low, high = guess[2 * p], guess[2 * p + 1]
            f_low, f_high = source[2 * p], source[2 * p + 1]
            x_ref[p] = jnp.concatenate([jnp.where(even, high, low), jnp.where(even, f_low, f_high)], axis=1)
            blacks.append(jnp.where(even, f_high, f_low))
        y_ref[u] = jnp.concatenate(blacks, axis=1)

    loop(0, 16, body, 2)


def pack_kernel(ib, ia, x, y, jb, ja, xf, yf, ku, kd):
    zero = jnp.zeros((80, 128), F32)
    for p in range(3):
        xf[p, 8:72] = ib[p]
        xf[35 + p, 8:72] = ia[p]
    loop(0, 32, lambda p: xf.__setitem__((p + 3, slice(8, 72)), x[p]), 4)
    yf[0, 8:72] = ib[3]
    yf[17, 8:72] = ia[3]
    loop(0, 16, lambda p: yf.__setitem__((p + 1, slice(8, 72)), y[p]), 4)

    tile = jnp.zeros((8, 128), F32)
    for p in range(38):
        xf[p, 0:8] = tile
        xf[p, 3:8] = jb[5 * p : 5 * p + 5]
        xf[p, 72:80] = tile
        xf[p, 72:77] = ja[5 * p : 5 * p + 5]
    for p in range(18):
        yf[p, 0:8] = tile
        yf[p, 5:8] = jb[190 + 3 * p : 193 + 3 * p]
        yf[p, 72:80] = tile
        yf[p, 72:75] = ja[190 + 3 * p : 193 + 3 * p]
    for p in (38, 39):
        xf[p] = zero
    for p in range(18, 24):
        yf[p] = zero
    lane = lanes_of((80, 128))
    for u in range(5):
        down, up, up_y = zero, zero, zero
        for s in range(8):
            value = turn(xf[8 * u + s], 8 * s, 1)
            place = (lane - 8 * s) & 127
            down = jnp.where((place < 5) | ((place >= 64) & (place < 68)), value, down)
            up = jnp.where(((place >= 59) & (place < 64)) | (place >= 124), value, up)
            if 8 * u + s < 18:
                value = turn(yf[8 * u + s], 8 * s + 5, 1)
                down = jnp.where(place_y(lane, s, 0), value, down)
                up_y = jnp.where(place_y(lane, s, 61), value, up_y)
        kd[u] = down
        ku[u] = up + turn(up_y, -2, 1) if u < 3 else up


def place_y(lane, s, start):
    place = (lane - 8 * s - 5) & 63
    return (place >= start) & (place < start + 3)


def rows_kernel(ib, ia, guess_low, guess_high, source_low, source_high, up, down):
    even = even_natural((8, 64))
    for out, guess, source, low, x_at, y_at in (
        (down, guess_low, source_low, 0, 0, 0),
        (up, guess_high, source_high, 56, 3, 5),
    ):
        blacks = []
        for p in range(38):
            if 3 <= p < 35:
                n = 2 * p - 6
                first, second, f_first, f_second = guess[n], guess[n + 1], source[n], source[n + 1]
                value = jnp.concatenate(
                    [jnp.where(even, second, first), jnp.where(even, f_first, f_second)], axis=1
                )
                blacks.append(jnp.where(even, f_second, f_first))
            else:
                value = ib[p, low : low + 8] if p < 3 else ia[p - 35, low : low + 8]
            out[5 * p : 5 * p + 5] = value[x_at : x_at + 5]
        for p in range(18):
            if p == 0 or p == 17:
                value = (ib if p == 0 else ia)[3, low : low + 8]
            else:
                value = jnp.concatenate(blacks[2 * p - 2 : 2 * p], axis=1)
            out[190 + 3 * p : 193 + 3 * p] = value[y_at : y_at + 3]
        out[244:248] = jnp.zeros((4, 128), F32)


def spread_kernel(xf, yf, black, g_red, g_black, c_ref, d_ref, weights, lanes):
    set_coefficients(L0, block_edges(), c_ref, d_ref)
    weights[...] = halving_weights(64)
    lanes[...] = neighbour_weights()
    zero = jnp.zeros((80, 128), F32)
    own = lanes_of((80, 128)) < 64

    def first(p):
        value = gather_rows(xf, p, 80)
        black[p + 1] = jnp.where(own, value, 0.0)
        g_red[p + 1] = jnp.where(own, turn(value, 64, 1), 0.0)

    loop(0, 40, first, 4)

    def second(p):
        value = gather_rows(yf, p, 80)
        g_black[2 * p + 2] = jnp.where(own, value, 0.0)
        g_black[2 * p + 3] = jnp.where(own, turn(value, 64, 1), 0.0)

    loop(0, 18, second, 4)
    for q in (0, 1, 38, 39, 40, 41):
        g_black[q] = zero
    clear_guards(black, g_red)


def fine_kernel(
    black0, g_red0, g_black0, kb, ka, c_ref, d_ref, weights, lanes, v_black, g_red, g_black, low_quads, high_quads,
    black, red, rest, z_ref, planes, natural, later,
):
    edges = block_edges()
    zero = jnp.zeros((80, 128), F32)
    lane = lanes_of((80, 128))

    even = even_mask(80)

    def sides(u):
        below = jnp.where(edges.klo, 0.0, gather_rows(kb, u, 80))
        return below, jnp.where(edges.khi, 0.0, gather_rows(ka, u, 80))

    def merge(p):
        below, above = sides(p // 8)
        turned = 8 * (p % 8)
        place = (lane - turned) & 127
        edge = jnp.where(place < 5, above, jnp.where((place >= 59) & (place < 64), below, 0.0))
        black[p + 1] = black0[p + 1] + turn(edge, 64 - turned, 1)
        edge = jnp.where((place >= 64) & (place < 68), above, jnp.where(place >= 124, below, 0.0))
        g_red[p + 1] = g_red0[p + 1] + turn(edge, -turned, 1)

    def merge_black(n):
        above = jnp.where(edges.khi, 0.0, gather_rows(ka, n // 8, 80))
        below = later[n // 8]
        turned = 8 * (n % 8)
        place = (lane - turned) & 127
        edge = jnp.where((place >= 5) & (place < 8), above, jnp.where((place >= 66) & (place < 69), below, 0.0))
        g_black[2 * n + 2] = g_black0[2 * n + 2] + turn(edge, 59 - turned, 1)
        edge = jnp.where((place >= 69) & (place < 72), above, jnp.where((place >= 2) & (place < 5), below, 0.0))
        g_black[2 * n + 3] = g_black0[2 * n + 3] + turn(edge, -5 - turned, 1)

    for u in range(3):
        later[u] = turn(sides(u)[0], 2, 1)
    for q in (0, 1, 38, 39, 40, 41):
        g_black[q] = zero
    for ref in (black, g_red):
        for q in (0, 39, 40, 41):
            ref[q] = zero
    for ref in (red, v_black):
        for q in (0, 1, 38, 39, 40, 41):
            ref[q] = zero
    for n in range(44):
        if n < 38:
            merge(n)
        if n % 2 == 0 and n < 36:
            merge_black(n // 2)
        if 1 <= n - 2 < 37:
            relax_at(L0, edges, c_ref, black, g_red, red, n - 2, True, even, lanes)
        if 1 <= n - 4 < 37:
            black_rest_at(L0, edges, c_ref, d_ref, red, g_black, v_black, rest, n - 4, even, lanes)
        if 3 <= n - 6 < 35:
            rest_fold_at(L0, edges, d_ref, g_red, red, v_black, rest, 3, z_ref, n - 6, even, lanes)
    halve(L0, 32, z_ref, planes, weights)

    def quad(q):
        total = planes[4 * q]
        for m in range(1, 4):
            total = total + turn(planes[4 * q + m], 32 * m, 1)
        scatter_rows(natural, q, total)
        return natural[q, 4:36]

    for q in range(4):
        low_quads[q] = quad(q)
        high_quads[q] = quad(q + 4)


def quad_rows(ib, ia, low_quads, high_quads, jb, ja, q):
    own = (ib, low_quads, high_quads, ia)[q // 4][q % 4]
    return jnp.concatenate([jb[q], own, ja[q]], axis=0)


def pack_quads_kernel(ib, ia, low_quads, high_quads, jb, ja, ku, kd):
    low_half = (lanes_of((64, 128)) & 31) < 16
    for u in range(8):
        first, second = (quad_rows(ib, ia, low_quads, high_quads, jb, ja, 2 * u + k) for k in range(2))
        kd[u] = jnp.where(low_half, turn(first, 32, 1), turn(second, 48, 1))
        ku[u] = jnp.where(low_half, turn(first, -48, 1), turn(second, -32, 1))


def join_kernel(ib, ia, low_quads, high_quads, jb, ja, qf):
    for q in range(16):
        qf[q] = quad_rows(ib, ia, low_quads, high_quads, jb, ja, q)


WINDOWS = (L1, L2, L3_OWN, L3)
WHOLES = (L4, L5, L6)
DOUBLINGS = ((32, False), (16, False), (8, False), (4, False), (16, True), (8, True))


def geometry_kernel(after, *refs):
    edges, whole = block_edges(), whole_edges()
    for index, lv in enumerate(WINDOWS + WHOLES):
        set_coefficients(lv, edges if lv in WINDOWS else whole, refs[2 * index], refs[2 * index + 1])
    refs = refs[2 * len(WINDOWS + WHOLES) :]
    refs[0][...] = halving_weights(0)
    for n, (size, is_whole) in enumerate(DOUBLINGS):
        at = whole if is_whole else edges
        refs[1][n] = doubling_weights(size, at.klo, at.khi)


def middle_kernel(
    qf, kb, ka, c1, d1, c2, d2, c3, d3, weights, lanes, v1, gr1, gb1, v2, gr2, gb2, message,
    red1, y1, z1, p1, red2, y2, z2, p2, gr3, gb3, red3, black3, y3, z3, p3, natural,
):
    edges = block_edges()
    lane = lanes_of((64, 128))
    even = even_mask(64)

    def unpack(u):
        below = jnp.where(edges.klo, 0.0, gather_rows(kb, u, 64))
        above = jnp.where(edges.khi, 0.0, gather_rows(ka, u, 64))
        sides = ((turn(below, 16, 1), above), (below, turn(above, -16, 1)))
        for h in range(2):
            value = gather_rows(qf, 2 * u + h, 64)
            left, right = sides[h]
            for t in range(2):
                both = []
                for m in (2 * t, 2 * t + 1):
                    place = (lane - 32 * m) & 127
                    edge = jnp.where(place < 48, right, jnp.where(place >= 112, left, 0.0))
                    both.append(turn(jnp.where(place < 32, value, edge), -32 * m, 1))
                index = 4 * u + 2 * h + t
                gr1[index] = jnp.where(even, both[0], both[1])
                gb1[index] = jnp.where(even, both[1], both[0])

    clear_guards(red1, v1)
    for n in range(36):
        if n % 4 == 0 and n < 32:
            unpack(n // 4)
        p = n - 1
        if 0 <= p < 30:
            red1[p + 1] = L1.scale * gr1[p + 1] * c1[kind(L1, edges, p, True)]
        if 0 <= n - 3 < 30:
            black_rest_at(L1, edges, c1, d1, red1, gb1, v1, y1, n - 3, even, lanes)
        if 1 <= n - 5 < 29:
            rest_fold_at(L1, edges, d1, gr1, red1, v1, y1, 1, z1, n - 5, even, lanes)
    halve(L1, 28, z1, p1, weights)
    colour_planes(p1, 14, gr2, gb2)
    clear_guards(red2, v2, gr2, gb2)
    relax_zero(L2, edges, c2, gr2, red2, 0, 14)
    relax_black_rest(L2, edges, c2, d2, red2, gb2, v2, y2, 0, 14)
    restrict(L2, edges, d2, gr2, red2, v2, y2, 1, 12, z2, p2, weights)
    colour_planes(p2, 6, gr3, gb3)
    clear_guards(red3, black3)
    relax_zero(L3_OWN, edges, c3, gr3, red3, 0, 6)
    relax_black_rest(L3_OWN, edges, c3, d3, red3, gb3, black3, y3, 0, 6)
    restrict(L3_OWN, edges, d3, gr3, red3, black3, y3, 1, 4, z3, p3, weights)
    lane = lanes_of((8, 128))
    row = rows_of((8, 128))
    third = jnp.zeros((8, 128), F32)
    for i in range(8):
        scatter_rows(natural, i, p2[i + 2])
        third = third + turn(jnp.where(lane < 8, natural[i, 4:12], 0.0), 8 * i, 1)
    folded = third + turn(turn(third, 4, 0), 64, 1)
    blocks = jnp.zeros((8, 128), F32)
    for i in range(4):
        blocks = blocks + turn(jnp.where(lane < 4, p3[i], 0.0), 16 * i, 1)
    fourth = jnp.zeros((8, 128), F32)
    for r in range(4):
        fourth = jnp.where((lane & 15) >> 2 == r, turn(turn(blocks, 4 * r, 1), -2 - r, 0), fourth)

    def store(n):
        for r in range(4):
            message[n, r] = folded[r : r + 1]
        message[n, 4] = fourth[0:1]

    loop(0, 64, store, 8)


def plane_kernel(tiles, message, near, rows, grid, blocks):
    x, y, z = (lax.axis_index(axis) for axis in ("gx", "gy", "gz"))
    shape = (8, 128)
    lane, row = lanes_of(shape), rows_of(shape)

    for n in range(64):
        rows[n : n + 1] = tiles[n, 4]
    parts = [jnp.zeros(shape, F32)] * 4
    for n in range(8):
        value = rows[pl.ds(n, 8, stride=8), :]
        here = (lane & 31) >> 2 == n
        for r in range(4):
            index = (lane >> 5) * 16 + 4 * r + (lane & 3)
            parts[r] = jnp.where(here, jnp.take_along_axis(value, index, axis=1), parts[r])
    for r in range(4):
        grid[pl.ds(r, 8, stride=4), :] = parts[r]

    lane = signed(lane)
    for dy in range(3):
        sides = []
        for dz in range(3):
            yy, zz = y + (dy - 1), z + (dz - 1)
            inside = (yy >= 0) & (yy < COUNT) & (zz >= 0) & (zz < COUNT)
            index = jnp.clip(yy, 0, COUNT - 1) * COUNT + jnp.clip(zz, 0, COUNT - 1)
            for r in range(4):
                blocks[3 * dy + dz, r : r + 1] = tiles[index, r]
            value = blocks[3 * dy + dz]
            value = jnp.where(row < 4, value, turn(turn(value, 4, 0), 64, 1))
            sides.append(jnp.where(inside, value, 0.0))
        for i in range(8):
            total = jnp.zeros(shape, F32)
            for dz in range(3):
                hit = (lane >= 8 * (dz - 1)) & (lane < 8 * dz)
                total = jnp.where(hit, turn(sides[dz], 8 * (dz - 1) - 8 * i, 1), total)
            near[i, 8 * dy : 8 * dy + 8] = total

    wide = lanes_of((24, 128))
    ends = []
    for first in (2, 0):
        total = jnp.zeros((24, 128), F32)
        for n in range(6):
            hit = (wide >= 20 * n) & (wide < 20 * n + 20)
            total = jnp.where(hit, turn(near[first + n], 20 * n + 6, 1), total)
        ends.append(total)
    for n in range(COUNT):
        message[n, 0:32] = grid[...]
        message[n, 32:56] = jnp.where(x < n, ends[0], ends[1])


def coarse_kernel(
    tiles, near, v2, gr2, gb2, v1, gr1, gb1, v0, gr0, gb0, c0, d0, c1, c2, c3, c4, d4, c5, d5, c6, halving, doubling, lanes, out, rest,
    gr4, gb4, red4, v4, y4, z4, p4, gr5, gb5, red5, v5, y5, z5, p5, gr6, gb6, red6, v6, full,
    gr3, gb3, red3, v3, b3, b2, red2, b1, red1, b0, red0, y0, e_ref, mixed, plain, fine_mixed, fine_plain, natural, last, out_held, rest_held, sems,
):
    edges = block_edges()
    whole = whole_edges()
    x, y, z = (lax.axis_index(axis) for axis in ("gx", "gy", "gz"))

    lane = signed(lanes_of((24, 128)))
    even = even_natural((24, 128))
    empty = jnp.zeros((24, 128), F32)

    def put(index, low, high):
        natural[index, 0:24] = jnp.where(even, low, high)
        natural[index + 12, 0:24] = jnp.where(even, high, low)

    for n in range(4):
        put(4 + n, near[2 * n], near[2 * n + 1])
    put(0, empty, empty)
    put(11, empty, empty)
    for at, first in ((x - 1, 1), (x + 1, 8)):
        inside = (at >= 0) & (at < COUNT)
        value = jnp.where(inside, tiles[jnp.clip(at, 0, COUNT - 1), 32:56], 0.0)
        planes = [jnp.where((lane >= -6) & (lane < 14), turn(value, -20 * n - 6, 1), 0.0) for n in range(6)]
        for n in range(3):
            put(first + n, planes[2 * n], planes[2 * n + 1])
    for n in range(24):
        natural[n, 24:32] = jnp.zeros((8, 128), F32)
    for n in range(12):
        gr3[n + 1] = gather_rows(natural, n, 32)
        gb3[n + 1] = gather_rows(natural, n + 12, 32)
    clear_guards(red3, v3)
    relax_zero(L3, edges, c3, gr3, red3, 0, 12)
    relax(L3, edges, c3, red3, gb3, v3, 0, 12, False)

    lane = lanes_of((32, 128))
    even32 = even_mask(32)
    zero = jnp.zeros((8, 128), F32)

    def place(n):
        value = gather_rows(tiles, n, 32)
        for t in range(2):
            low = jnp.where(lane < 32, turn(value, -64 * t, 1), 0.0)
            high = jnp.where(lane < 32, turn(value, -64 * t - 32, 1), 0.0)
            index = 2 * n + t + 1
            gr4[index] = jnp.where(even32, low, high)
            gb4[index] = jnp.where(even32, high, low)

    loop(0, 8, place, 4)
    clear_guards(red4, v4, gr4, gb4)
    relax_zero(L4, whole, c4, gr4, red4, 0, 16)
    relax_black_rest(L4, whole, c4, d4, red4, gb4, v4, y4, 0, 16)
    restrict(L4, whole, d4, gr4, red4, v4, y4, 0, 16, z4, p4, halving)
    colour_planes(p4, 8, gr5, gb5)
    clear_guards(red5, v5, gr5, gb5)
    relax_zero(L5, whole, c5, gr5, red5, 0, 8)
    relax_black_rest(L5, whole, c5, d5, red5, gb5, v5, y5, 0, 8)
    restrict(L5, whole, d5, gr5, red5, v5, y5, 0, 8, z5, p5, halving)
    colour_planes(p5, 4, gr6, gb6)
    clear_guards(red6, v6)
    relax_zero(L6, whole, c6, gr6, red6, 0, 4)
    relax(L6, whole, c6, red6, gb6, v6, 0, 4, False)
    for _ in range(COARSE_SWEEPS - 1):
        relax(L6, whole, c6, v6, gr6, red6, 0, 4, True)
        relax(L6, whole, c6, red6, gb6, v6, 0, 4, False)

    def ascend(coarse, fine, c, w, coarse_red, coarse_black, kept, g_red, g_black, red):
        count = coarse.size
        e, rows = e_ref.at[0:count, 0:count], slice(0, count)
        n, p = mixed.at[0 : count + 2, rows], plain.at[0 : count + 2, rows]
        whole_planes(coarse, coarse_red, coarse_black, 0, coarse.pairs, e)
        prolong(e, count, 0, count, whole, w, mixed.at[1 : count + 1, rows], plain.at[1 : count + 1, rows])
        p[0] = -p[1]
        p[count + 1] = -p[count]
        correct(fine, whole, c, kept, n, p, 0, 1, kept, 0, fine.pairs)
        relax(fine, whole, c, kept, g_red, red, 0, fine.pairs, True)
        relax(fine, whole, c, red, g_black, kept, 0, fine.pairs, False)

    ascend(L6, L5, c5, doubling.at[5], red6, v6, v5, gr5, gb5, red5)
    ascend(L5, L4, c4, doubling.at[4], red5, v5, v4, gr4, gb4, red4)

    even = even_mask(32)
    for t in (0, 1, 2, 3, 36, 37, 38, 39):
        full[t] = jnp.zeros((48, 128), F32)

    def expand(t):
        r, b = red4[t + 1], v4[t + 1]
        for n, value in ((2 * t + 4, jnp.where(even, r, b)), (2 * t + 5, jnp.where(even, b, r))):
            full[n, 0:8] = zero
            scatter_rows(full, n, value, 8)
            full[n, 40:48] = zero

    loop(0, 16, expand, 4)

    def cut(t):
        rows = gather_rows(full, 4 * x + t, 16, 4 * y + 4)
        e_ref[t, 0:16] = pltpu.roll(rows, (128 - 4 * z) & 127, 1)

    loop(0, 12, cut)

    def lift(index, fine, c, count, rows, plane_zero, row_zero, size, kept, dest, low, high):
        e = e_ref.at[0:count, 0:rows]
        n, p = mixed.at[0:count, 0:rows], plain.at[0:count, 0:rows]
        prolong(e, count, plane_zero, size, edges, doubling.at[index], n, p)
        correct(fine, edges, c, kept, n, p, row_zero, plane_zero, dest, low, high)

    def smooth(lv, c, black, g_red, g_black, red, low, high, low2, high2):
        relax(lv, edges, c, black, g_red, red, low, high, True)
        relax(lv, edges, c, red, g_black, black, low2, high2, False)

    lift(3, L3, c3, 12, 16, 4, 4, 4, v3, b3, 1, 11)
    clear_guards(b3, red3)
    smooth(L3, c3, b3, gr3, gb3, red3, 2, 10, 2, 10)

    window_planes(L3, red3, b3, 2, 8, 4, natural.at[0:16, 0:32], e_ref.at[0:16, 0:16])
    lift(2, L2, c2, 16, 16, 4, 4, 8, v2, b2, 0, 14)
    clear_guards(b2, red2)
    smooth(L2, c2, b2, gr2, gb2, red2, 1, 13, 1, 13)

    whole_planes(L2, red2, b2, 1, 12, e_ref.at[0:24, 0:32])
    e = e_ref.at[0:24, 0:32]
    n, p = mixed.at[0:24, 0:32], plain.at[0:24, 0:32]
    prolong(e, 24, 4, 16, edges, doubling.at[1], n, p)
    correct1 = correct_at(L1, edges, c1, v1, n, p, 8, 4, b1)
    for index in (5, 26):
        b1[index] = jnp.zeros(b1.shape[1:], F32)
    even1 = even_mask(64)
    even0 = even_mask(80)
    mixed0, plain0 = fine_mixed, fine_plain
    correct0 = correct_at(L0, edges, c0, v0, mixed0, plain0, 4, 4, b0)
    b0[1] = jnp.zeros(b0.shape[1:], F32)
    b0[38] = jnp.zeros(b0.shape[1:], F32)
    copies = []

    def send(held, target, n):
        copy = pltpu.make_async_copy(held.at[pl.ds(8 * n, 8)], target.at[pl.ds(8 * n, 8)], sems.at[len(copies)])
        copy.start()
        copies.append(copy)

    def store(held, p, r, b):
        for n, value in ((0, jnp.where(even0, r, b)), (1, jnp.where(even0, b, r))):
            scatter_rows(last, 2 * (p & 7) + n, value)
            held[2 * p - 6 + n] = last[2 * (p & 7) + n, 8:72, 0:64]

    def coarse_step(n):
        if n < 25:
            correct1(n)
        if 5 <= n - 2 < 25:
            relax_at(L1, edges, c1, b1, gr1, red1, n - 2, True, even1, lanes)
        if 6 <= n - 4 < 24:
            relax_at(L1, edges, c1, red1, gb1, b1, n - 4, False, even1)

    def lift_planes(c):
        planes = []
        for t in range(4 * c, 4 * c + 4):
            r, b = red1[t + 6], b1[t + 6]
            scatter_rows(natural, 2 * t, jnp.where(even1, r, b))
            scatter_rows(natural, 2 * t + 1, jnp.where(even1, b, r))
            planes += [gather_rows(natural, 2 * t + k, 40, 12) for k in range(2)]
        both = split_dot(jnp.concatenate(planes, axis=0), doubling[0])
        for k in range(8):
            mixed0[8 * c + k] = both[40 * k : 40 * k + 40, :128]
            plain0[8 * c + k] = both[40 * k : 40 * k + 40, 128:]
        if c == 0:
            plain0[3] = jnp.where(edges.ilo, -plain0[4], plain0[3])
        if c == 4:
            plain0[36] = jnp.where(edges.ihi, -plain0[35], plain0[36])

    def fine_step(n):
        if n < 37:
            correct0(n)
        if 1 <= n - 2 < 37:
            relax_at(L0, edges, c0, b0, gr0, red0, n - 2, True, even0, lanes)
        p = n - 4
        if 2 <= p < 36:
            black_rest_at(L0, edges, c0, d0, red0, gb0, b0, y0, p, even0)
        if 3 <= p < 35:
            store(out_held, p, red0[p + 1], b0[p + 1])
            if p % 4 == 2:
                send(out_held, out, p // 4 - 1)
        p = n - 6
        if 3 <= p < 35:
            store(rest_held, p, red_rest(L0, edges, d0, gr0, red0, b0, p, even0), y0[p + 1])
            if p % 4 == 2:
                send(rest_held, rest, p // 4 - 1)

    done, ready = 0, 0
    for n in range(5, 29):
        coarse_step(n)
        for _ in range(2):
            if done < ready:
                done += 1
                fine_step(done)
        if n >= 12 and n % 4 == 0:
            lift_planes(n // 4 - 3)
            ready = 2 * n - 19
    for n in range(done + 1, 43):
        fine_step(n)
    for copy in copies:
        copy.wait()


def struct(*shape):
    return jax.ShapeDtypeStruct(shape, F32)


def call(kernel, outs, scratch, flops=2_000_000, out_space=pltpu.VMEM, semaphores=0):
    space = pl.BlockSpec(memory_space=pltpu.VMEM)
    extra = [pltpu.SemaphoreType.DMA((semaphores,))] if semaphores else []

    def run(*args):
        return pl.pallas_call(
            kernel,
            out_shape=outs,
            in_specs=[space] * len(args),
            out_specs=[pl.BlockSpec(memory_space=out_space)] * len(outs),
            scratch_shapes=[pltpu.VMEM(shape, F32) for shape in scratch] + extra,
            compiler_params=pltpu.CompilerParams(vmem_limit_bytes=40 * 2**20),
            cost_estimate=pl.CostEstimate(flops=flops, bytes_accessed=1_000_000, transcendentals=0),
        )(*args)

    return run


def pair(to_next, to_before, axis, ring=False):
    up = [(i, (i + 1) % COUNT) for i in range(COUNT if ring else COUNT - 1)]
    down = [(j, i) for i, j in up]
    after = lax.ppermute(to_before, axis, down)
    before = lax.ppermute(to_next, axis, up)
    return before, after


def face(guess, source, start, first):
    even = ((lax.broadcasted_iota(jnp.int32, (64, 64), 0) + lax.broadcasted_iota(jnp.int32, (64, 64), 1)) & 1) == 0
    low, high = guess[start : start + 6 : 2], guess[start + 1 : start + 6 : 2]
    f_low, f_high = source[start : start + 6 : 2], source[start + 1 : start + 6 : 2]
    red = jnp.where(even, f_low, f_high)
    black = jnp.where(even, f_high, f_low)
    mixed = jnp.concatenate([jnp.where(even, high, low), red], axis=2)
    return jnp.concatenate([mixed, jnp.concatenate([black[first : first + 1], black[first + 1 : first + 2]], axis=2)], axis=0)


def coefficient_shapes(*levels):
    shapes = []
    for lv in levels:
        shapes += [struct(4, lv.rows, 128), struct(3, lv.rows, 128)]
    return shapes


def per_device(right_side, guess):
    ib, ia = pair(face(guess, right_side, 58, 1), face(guess, right_side, 0, 0), "gx")
    x, y = call(compact_kernel, (struct(32, 64, 128), struct(16, 64, 128)), [])(guess, right_side)

    up, down = call(rows_kernel, (struct(248, 128), struct(248, 128)), [])(
        ib, ia, guess[:, 0:8], guess[:, 56:64], right_side[:, 0:8], right_side[:, 56:64]
    )
    jb, ja = pair(up, down, "gy")
    xf, yf, ku, kd = call(
        pack_kernel, (struct(40, 80, 128), struct(24, 80, 128), struct(5, 80, 128), struct(5, 80, 128)), []
    )(ib, ia, x, y, jb, ja)
    kb, ka = pair(ku, kd, "gz", True)
    fine = L0.shape()
    field = struct(*fine)
    weights = jax.ShapeDtypeStruct((256, 128), BF16)
    black, g_red, g_black, c0, d0, w0, lanes = call(
        spread_kernel, (field, field, field, *coefficient_shapes(L0), weights, weights), []
    )(xf, yf)
    v0, gr0, gb0, low_quads, high_quads = call(
        fine_kernel,
        (field, field, field, struct(4, 32, 128), struct(4, 32, 128)),
        [fine, fine, fine, (32, 40, 128), (32, 40, 128), (8, 40, 128), (3, 80, 128)],
    )(black, g_red, g_black, kb, ka, c0, d0, w0, lanes)

    ib, ia = pair(high_quads, low_quads, "gx")
    shapes = coefficient_shapes(*WINDOWS, *WHOLES) + [weights, jax.ShapeDtypeStruct((6, 256, 256), BF16)]
    c1, d1, c2, d2, c3o, d3o, c3, _, c4, d4, c5, d5, c6, _, halving, doubling = call(
        geometry_kernel, tuple(shapes), []
    )(low_quads)

    def quad_ends(low):
        return jnp.concatenate([part[:, low : low + 16] for part in (ib, low_quads, high_quads, ia)], axis=0)

    jb, ja = pair(quad_ends(16), quad_ends(0), "gy")
    parts = (ib, ia, low_quads, high_quads, jb, ja)
    ku, kd = call(pack_quads_kernel, (struct(8, 64, 128), struct(8, 64, 128)), [])(*parts)
    kb, ka = pair(ku, kd, "gz", True)
    (qf,) = call(join_kernel, (struct(16, 64, 128),), [])(*parts)
    s1, s2, s3 = L1.shape(), L2.shape(), L3_OWN.shape()
    v1, gr1, gb1, v2, gr2, gb2, message = call(
        middle_kernel,
        tuple(struct(*s) for s in (s1, s1, s1, s2, s2, s2, (64, 5, 1, 128))),
        [s1, s1, (28, 32, 128), (28, 32, 128), s2, s2, (12, 16, 128), (12, 16, 128)]
        + [s3, s3, s3, s3, s3, (4, 8, 128), (4, 8, 128), (8, 16, 128)],
    )(qf, kb, ka, c1, d1, c2, d2, c3o, d3o, halving, lanes)

    tiles = lax.all_to_all(message, ("gy", "gz"), 0, 0)
    message, near = call(
        plane_kernel, (struct(8, 56, 128), struct(8, 24, 128)), [(64, 128), (32, 128), (9, 8, 128)]
    )(tiles)
    tiles = lax.all_to_all(message, "gx", 0, 0)
    s3, s4, s5, s6 = L3.shape(), L4.shape(), L5.shape(), L6.shape()
    return tuple(
        call(
            coarse_kernel,
            (struct(64, 64, 64), struct(64, 64, 64)),
            [s4, s4, s4, s4, s4, (16, 16, 128), (16, 16, 128)]
            + [s5, s5, s5, s5, s5, (8, 8, 128), (8, 8, 128)]
            + [s6, s6, s6, s6, (40, 48, 128)]
            + [s3, s3, s3, s3, s3, s2, s2, s1, s1, fine, fine, fine]
            + [(42, 40, 128), (42, 40, 128), (42, 40, 128), (40, 40, 128), (40, 40, 128), (40, 64, 128), (16, 80, 128), (64, 64, 64), (64, 64, 64)],
            out_space=pl.ANY,
            semaphores=16,
        )(tiles, near, v2, gr2, gb2, v1, gr1, gb1, v0, gr0, gb0, c0, d0, c1, c2, c3, c4, d4, c5, d5, c6, halving, doubling, lanes)
    )


def solution(mesh):
    return jax.shard_map(
        per_device,
        mesh=mesh,
        in_specs=(P("gx", "gy", "gz"), P("gx", "gy", "gz")),
        out_specs=(P("gx", "gy", "gz"), P("gx", "gy", "gz")),
        check_vma=False,
    )
```

```python
import typing

import jax
import jax.numpy as jnp
from jax import lax
from jax.experimental import pallas as pl
from jax.experimental.pallas import tpu as pltpu
from jax.sharding import PartitionSpec as P


F32 = jnp.float32
BF16 = jnp.bfloat16
COARSE_SWEEPS = 4
COUNT = 8


class Level(typing.NamedTuple):
    level: int
    pairs: int
    rows: int
    first: int
    offset: int
    size: int

    @property
    def scale(self):
        return 4.0**self.level

    @property
    def inverse(self):
        return 0.25**self.level

    @property
    def own(self):
        return self.size // 2

    def shape(self):
        return (self.pairs + 2, self.rows, 128)


L0 = Level(0, 40, 80, 3, 8, 64)
L1 = Level(1, 30, 64, 7, 16, 32)
L2 = Level(2, 14, 32, 3, 8, 16)
L3_OWN = Level(3, 6, 16, 1, 4, 8)
L3 = Level(3, 12, 32, 4, 8, 8)
L4 = Level(4, 16, 32, 0, 0, 32)
L5 = Level(5, 8, 16, 0, 0, 16)
L6 = Level(6, 4, 8, 0, 0, 8)


class Edges(typing.NamedTuple):
    ilo: typing.Any
    ihi: typing.Any
    jlo: typing.Any
    jhi: typing.Any
    klo: typing.Any
    khi: typing.Any


def block_edges():
    ends = []
    for axis in ("gx", "gy", "gz"):
        place = lax.axis_index(axis)
        ends += [place == 0, place == COUNT - 1]
    return Edges(*ends)


def whole_edges():
    yes = lax.axis_index("gx") >= 0
    return Edges(*([yes] * 6))


def lanes_of(shape):
    return lax.broadcasted_iota(jnp.int32, shape, len(shape) - 1)


def rows_of(shape):
    return lax.broadcasted_iota(jnp.int32, shape, len(shape) - 2)


def signed(lane):
    return jnp.where(lane < 96, lane, lane - 128)


def cells_of(shape):
    row = rows_of(shape)
    return (row & 7) * (shape[-2] // 8) + (row >> 3)


def even_mask(rows):
    shape = (rows, 128)
    return ((cells_of(shape) + lanes_of(shape)) & 1) == 0


def even_natural(shape):
    return ((rows_of(shape) + lanes_of(shape)) & 1) == 0


def gather_rows(ref, index, rows, start=0):
    stride = rows // 8
    if stride == 1:
        return ref[index, pl.ds(start, 8), :]
    return jnp.concatenate([ref[index, pl.ds(start + t, 8, stride=stride), :] for t in range(stride)], axis=0)


def scatter_rows(ref, index, value, start=0):
    stride = value.shape[0] // 8
    for t in range(stride):
        ref[index, pl.ds(start + t, 8, stride=stride), :] = value[8 * t : 8 * t + 8]


def row_before(value):
    last = value[value.shape[0] - 8 :]
    first = jnp.where(rows_of((8, 128)) == 0, 0.0, pltpu.roll(last, 1, 0))
    return first if value.shape[0] == 8 else jnp.concatenate([first, value[: value.shape[0] - 8]], axis=0)


def row_after(value):
    last = jnp.where(rows_of((8, 128)) == 7, 0.0, pltpu.roll(value[:8], 7, 0))
    return last if value.shape[0] == 8 else jnp.concatenate([value[8:], last], axis=0)


def fold_rows(value):
    tiles = value.shape[0] // 16
    if tiles == 0:
        raise ValueError("rows")
    return jnp.concatenate([value[16 * t : 16 * t + 8] + value[16 * t + 8 : 16 * t + 16] for t in range(tiles)], axis=0)


def double_rows(even, odd):
    parts = []
    for t in range(even.shape[0] // 8):
        parts += [even[8 * t : 8 * t + 8], odd[8 * t : 8 * t + 8]]
    return jnp.concatenate(parts, axis=0)


def turn(value, shift, axis):
    size = value.shape[axis]
    if isinstance(shift, int):
        shift %= size
        if shift == 0:
            return value
    return pltpu.roll(value, shift, axis)


def bounds(low, high, size):
    return jnp.where(low, 0, -4096), jnp.where(high, size, 4096)


def set_coefficients(lv, edges, c_ref, d_ref):
    shape = (lv.rows, 128)
    row = cells_of(shape) - lv.offset
    lane = signed(lanes_of(shape))
    row_low, row_high = bounds(edges.jlo, edges.jhi, lv.size)
    lane_low, lane_high = bounds(edges.klo, edges.khi, lv.size)
    inside = (row >= row_low) & (row < row_high) & (lane >= lane_low) & (lane < lane_high)
    diagonal = 6.0 + jnp.where(row == row_low, 1.0, 0.0) + jnp.where(row == row_high - 1, 1.0, 0.0)
    diagonal = diagonal + jnp.where(lane == lane_low, 1.0, 0.0) + jnp.where(lane == lane_high - 1, 1.0, 0.0)
    even = jnp.where(even_mask(lv.rows), 1.0, 0.0)
    for index, extra in enumerate((0.0, even, 1.0 - even)):
        d_ref[index] = diagonal + extra
        c_ref[index] = jnp.where(inside, 1.0 / (diagonal + extra), 0.0)
    c_ref[3] = jnp.zeros(shape, F32)


def kind(lv, edges, p, red):
    last = lv.first + lv.own - 1
    low, high = (1, 2) if red else (2, 1)
    if isinstance(p, int):
        if p in (lv.first, last):
            return jnp.where(edges.ilo, low, 0) if p == lv.first else jnp.where(edges.ihi, high, 0)
        return 0 if lv.first < p < last else jnp.where(edges.ilo if p < lv.first else edges.ihi, 3, 0)
    inner = jnp.where((p == lv.first) & edges.ilo, low, jnp.where((p == last) & edges.ihi, high, 0))
    return jnp.where(((p < lv.first) & edges.ilo) | ((p > last) & edges.ihi), 3, inner)


def loop(low, high, body, width=0):
    count = high - low
    width = count if width == 0 else min(width, count)

    def step(n, carry):
        for k in range(width):
            body(low + n * width + k)
        return carry

    if count // width > 1:
        lax.fori_loop(0, count // width, step, 0)
        done = count // width * width
    else:
        done = 0
    for p in range(low + done, high):
        body(p)


def group(rows):
    return max(1, 180 // (rows // 8))


def neighbour_weights():
    shape = (256, 128)
    apart = ((rows_of(shape) & 127) - lanes_of(shape)) & 127
    return jnp.where((apart == 1) | (apart == 127), 1.0, 0.0).astype(BF16)


def lane_sum(value, weights):
    rows = value.shape[0]
    part = rows if weights is None else 16
    total = turn(value[:part], 1, 1) + turn(value[:part], 127, 1)
    return total if part == rows else jnp.concatenate([total, split_dot(value[part:], weights[...])], axis=0)


def around(ref, p, even, red, weights=None):
    value = ref[p + 1]
    before, after = ref[p], ref[p + 2]
    total = value + (jnp.where(even, before, after) if red else jnp.where(even, after, before))
    total = total + (row_before(value) + row_after(value))
    return total + lane_sum(value, weights)


def relax_at(lv, edges, c_ref, other, source, dest, p, red, even, weights=None):
    total = around(other, p, even, red, weights) + (source[p + 1] if lv.level == 0 else lv.scale * source[p + 1])
    dest[p + 1] = total * c_ref[kind(lv, edges, p, red)]


def relax(lv, edges, c_ref, other, source, dest, low, high, red):
    even = even_mask(lv.rows)
    loop(low, high, lambda p: relax_at(lv, edges, c_ref, other, source, dest, p, red, even), group(lv.rows))


def relax_zero(lv, edges, c_ref, source, dest, low, high):
    def body(p):
        dest[p + 1] = lv.scale * source[p + 1] * c_ref[kind(lv, edges, p, True)]

    loop(low, high, body, group(lv.rows))


def gap(lv, d, value, total):
    return d * value - total if lv.level == 0 else lv.inverse * (d * value - total)


def black_rest_at(lv, edges, c_ref, d_ref, red, source, dest, rest, p, even, weights=None):
    total = around(red, p, even, False, weights)
    g = source[p + 1]
    at = kind(lv, edges, p, False)
    value = (total + (g if lv.level == 0 else lv.scale * g)) * c_ref[at]
    dest[p + 1] = value
    rest[p + 1] = g - gap(lv, d_ref[jnp.minimum(at, 2)], value, total)


def relax_black_rest(lv, edges, c_ref, d_ref, red, source, dest, rest, low, high):
    even = even_mask(lv.rows)
    loop(low, high, lambda p: black_rest_at(lv, edges, c_ref, d_ref, red, source, dest, rest, p, even), group(lv.rows))


def red_rest(lv, edges, d_ref, source, red, black, p, even, weights=None):
    d = d_ref[jnp.minimum(kind(lv, edges, p, True), 2)]
    return source[p + 1] - gap(lv, d, red[p + 1], around(black, p, even, True, weights))


def clear_guards(*refs):
    for ref in refs:
        ref[0] = jnp.zeros(ref.shape[1:], F32)
        ref[ref.shape[0] - 1] = jnp.zeros(ref.shape[1:], F32)


def split_dot(value, weights):
    high = value.astype(BF16)
    low = (value - high.astype(F32)).astype(BF16)
    return jnp.dot(jnp.concatenate([high, low], axis=1), weights, preferred_element_type=F32)


def halving_weights(own_lanes):
    shape = (256, 128)
    fine = signed(rows_of(shape) & 127)
    coarse = signed(lanes_of(shape))
    hit = (fine >> 1) == coarse
    if own_lanes:
        hit = hit & (fine >= 0) & (fine < own_lanes)
    return jnp.where(hit, 0.125, 0.0).astype(BF16)


def doubling_weights(size, low, high):
    shape = (256, 256)
    coarse = signed(rows_of(shape) & 127)
    lane = lanes_of(shape)
    fine = signed(lane & 127)
    parent = fine >> 1
    beside = parent + jnp.where((fine & 1) == 1, 1, -1)
    beyond = ((beside == -1) & low) | ((beside == size) & high)
    centre = jnp.where(coarse == parent, 0.25, 0.0)
    neighbour = jnp.where(coarse == beside, 0.25, 0.0)
    mixed = jnp.where(beyond, 0.0, centre + neighbour)
    return jnp.where(lane < 128, mixed, centre).astype(BF16)


def rest_fold_at(lv, edges, d_ref, g_red, red, black, rest, low, z_ref, p, even, weights=None):
    z_ref[p - low] = fold_rows(rest[p + 1] + red_rest(lv, edges, d_ref, g_red, red, black, p, even, weights))


def restrict(lv, edges, d_ref, g_red, red, black, rest, low, count, z_ref, out_ref, weights):
    even = even_mask(lv.rows)
    loop(
        low, low + count,
        lambda p: rest_fold_at(lv, edges, d_ref, g_red, red, black, rest, low, z_ref, p, even), group(lv.rows),
    )
    halve(lv, count, z_ref, out_ref, weights)


def halve(lv, count, z_ref, out_ref, weights):
    half = lv.rows // 2
    chunk = max(c for c in range(1, count + 1) if count % c == 0 and (c * half <= 320 or c == 1))

    def product(n):
        value = z_ref[pl.ds(n * chunk, chunk)].reshape(chunk * half, 128)
        out_ref[pl.ds(n * chunk, chunk)] = split_dot(value, weights[...]).reshape(chunk, half, 128)

    loop(0, count // chunk, product)


def colour_planes(planes, pairs, red, black):
    even = even_mask(planes.shape[1])

    def body(p):
        low, high = planes[2 * p], planes[2 * p + 1]
        red[p + 1] = jnp.where(even, low, high)
        black[p + 1] = jnp.where(even, high, low)

    loop(0, pairs, body, 8)


def whole_planes(lv, red, black, pair_low, pairs, e_ref):
    even = even_mask(lv.rows)

    def body(t):
        r, b = red[pair_low + t + 1], black[pair_low + t + 1]
        e_ref[2 * t] = jnp.where(even, r, b)
        e_ref[2 * t + 1] = jnp.where(even, b, r)

    loop(0, pairs, body, 8)


def window_planes(lv, red, black, pair_low, pairs, row_low, natural, e_ref):
    even = even_mask(lv.rows)
    rows = e_ref.shape[1]

    def body(t):
        r, b = red[pair_low + t + 1], black[pair_low + t + 1]
        scatter_rows(natural, 2 * t, jnp.where(even, r, b))
        scatter_rows(natural, 2 * t + 1, jnp.where(even, b, r))

    def again(t):
        e_ref[t] = gather_rows(natural, t, rows, row_low)

    loop(0, pairs, body, 4)
    loop(0, 2 * pairs, again, 8)


def prolong(e_ref, count, plane_zero, size, edges, weights, mixed, plain):
    rows = e_ref.shape[1]
    chunk = max(c for c in range(1, count + 1) if count % c == 0 and (c * rows <= 320 or c == 1))

    def body(n):
        at = pl.ds(n * chunk, chunk)
        both = split_dot(e_ref[at].reshape(chunk * rows, 128), weights[...])
        mixed[at] = both[:, :128].reshape(chunk, rows, 128)
        plain[at] = both[:, 128:].reshape(chunk, rows, 128)

    loop(0, count // chunk, body)
    if plane_zero > 0:
        pl.when(edges.ilo)(lambda: plain.__setitem__(plane_zero - 1, -plain[plane_zero]))
    last = plane_zero + size - 1
    if last + 1 < count:
        pl.when(edges.ihi)(lambda: plain.__setitem__(last + 1, -plain[last]))


def correct(lv, edges, c_ref, kept, mixed, plain, row_zero, plane_zero, dest, low, high):
    body = correct_at(lv, edges, c_ref, kept, mixed, plain, row_zero, plane_zero, dest)
    loop(low, high, body, group(lv.rows))


def correct_at(lv, edges, c_ref, kept, mixed, plain, row_zero, plane_zero, dest):
    even = even_mask(lv.rows)
    half = lv.rows // 2
    row = cells_of((half, 128)) - row_zero
    at_low = (row == 0) & edges.jlo
    at_high = (row == lv.size // 2 - 1) & edges.jhi

    def body(p):
        t = p - lv.first + plane_zero
        value, near = plain[t], mixed[t]
        before = near + jnp.where(at_low, -value, row_before(value))
        after = near + jnp.where(at_high, -value, row_after(value))
        up, down = plain[t + 1], plain[t - 1]
        step = double_rows(before, after) + jnp.where(even, double_rows(up, up), double_rows(down, down))
        c = c_ref[kind(lv, edges, p, False)]
        dest[p + 1] = jnp.where(c > 0.0, kept[p + 1] + step, 0.0)

    return body


def compact_kernel(guess, source, x_ref, y_ref):
    even = ((rows_of((64, 64)) + lanes_of((64, 64))) & 1) == 0

    def body(u):
        blacks = []
        for s in range(2):
            p = 2 * u + s
            low, high = guess[2 * p], guess[2 * p + 1]
            f_low, f_high = source[2 * p], source[2 * p + 1]
            x_ref[p] = jnp.concatenate([jnp.where(even, high, low), jnp.where(even, f_low, f_high)], axis=1)
            blacks.append(jnp.where(even, f_high, f_low))
        y_ref[u] = jnp.concatenate(blacks, axis=1)

    loop(0, 16, body, 2)


def pack_kernel(ib, ia, x, y, jb, ja, xf, yf, ku, kd):
    zero = jnp.zeros((80, 128), F32)
    for p in range(3):
        xf[p, 8:72] = ib[p]
        xf[35 + p, 8:72] = ia[p]
    loop(0, 32, lambda p: xf.__setitem__((p + 3, slice(8, 72)), x[p]), 4)
    yf[0, 8:72] = ib[3]
    yf[17, 8:72] = ia[3]
    loop(0, 16, lambda p: yf.__setitem__((p + 1, slice(8, 72)), y[p]), 4)

    tile = jnp.zeros((8, 128), F32)
    for p in range(38):
        xf[p, 0:8] = tile
        xf[p, 3:8] = jb[5 * p : 5 * p + 5]
        xf[p, 72:80] = tile
        xf[p, 72:77] = ja[5 * p : 5 * p + 5]
    for p in range(18):
        yf[p, 0:8] = tile
        yf[p, 5:8] = jb[190 + 3 * p : 193 + 3 * p]
        yf[p, 72:80] = tile
        yf[p, 72:75] = ja[190 + 3 * p : 193 + 3 * p]
    for p in (38, 39):
        xf[p] = zero
    for p in range(18, 24):
        yf[p] = zero
    lane = lanes_of((80, 128))
    for u in range(5):
        down, up, up_y = zero, zero, zero
        for s in range(8):
            value = turn(xf[8 * u + s], 8 * s, 1)
            place = (lane - 8 * s) & 127
            down = jnp.where((place < 5) | ((place >= 64) & (place < 68)), value, down)
            up = jnp.where(((place >= 59) & (place < 64)) | (place >= 124), value, up)
            if 8 * u + s < 18:
                value = turn(yf[8 * u + s], 8 * s + 5, 1)
                down = jnp.where(place_y(lane, s, 0), value, down)
                up_y = jnp.where(place_y(lane, s, 61), value, up_y)
        kd[u] = down
        ku[u] = up + turn(up_y, -2, 1) if u < 3 else up


def place_y(lane, s, start):
    place = (lane - 8 * s - 5) & 63
    return (place >= start) & (place < start + 3)


def rows_kernel(ib, ia, guess_low, guess_high, source_low, source_high, up, down):
    even = even_natural((8, 64))
    for out, guess, source, low, x_at, y_at in (
        (down, guess_low, source_low, 0, 0, 0),
        (up, guess_high, source_high, 56, 3, 5),
    ):
        blacks = []
        for p in range(38):
            if 3 <= p < 35:
                n = 2 * p - 6
                first, second, f_first, f_second = guess[n], guess[n + 1], source[n], source[n + 1]
                value = jnp.concatenate(
                    [jnp.where(even, second, first), jnp.where(even, f_first, f_second)], axis=1
                )
                blacks.append(jnp.where(even, f_second, f_first))
            else:
                value = ib[p, low : low + 8] if p < 3 else ia[p - 35, low : low + 8]
            out[5 * p : 5 * p + 5] = value[x_at : x_at + 5]
        for p in range(18):
            if p == 0 or p == 17:
                value = (ib if p == 0 else ia)[3, low : low + 8]
            else:
                value = jnp.concatenate(blacks[2 * p - 2 : 2 * p], axis=1)
            out[190 + 3 * p : 193 + 3 * p] = value[y_at : y_at + 3]
        out[244:248] = jnp.zeros((4, 128), F32)


def spread_kernel(xf, yf, black, g_red, g_black, c_ref, d_ref, weights, lanes):
    set_coefficients(L0, block_edges(), c_ref, d_ref)
    weights[...] = halving_weights(64)
    lanes[...] = neighbour_weights()
    zero = jnp.zeros((80, 128), F32)
    own = lanes_of((80, 128)) < 64

    def first(p):
        value = gather_rows(xf, p, 80)
        black[p + 1] = jnp.where(own, value, 0.0)
        g_red[p + 1] = jnp.where(own, turn(value, 64, 1), 0.0)

    loop(0, 40, first, 4)

    def second(p):
        value = gather_rows(yf, p, 80)
        g_black[2 * p + 2] = jnp.where(own, value, 0.0)
        g_black[2 * p + 3] = jnp.where(own, turn(value, 64, 1), 0.0)

    loop(0, 18, second, 4)
    for q in (0, 1, 38, 39, 40, 41):
        g_black[q] = zero
    clear_guards(black, g_red)


def fine_kernel(
    black0, g_red0, g_black0, kb, ka, c_ref, d_ref, weights, lanes, v_black, g_red, g_black, low_quads, high_quads,
    black, red, rest, z_ref, planes, natural, later, held,
):
    edges = block_edges()
    zero = jnp.zeros((80, 128), F32)
    lane = lanes_of((80, 128))

    even = even_mask(80)

    def sides(u):
        below = jnp.where(edges.klo, 0.0, gather_rows(kb, u, 80))
        return below, jnp.where(edges.khi, 0.0, gather_rows(ka, u, 80))

    def merge(p):
        below, above = held[2 * (p // 8)], held[2 * (p // 8) + 1]
        turned = 8 * (p % 8)
        place = (lane - turned) & 127
        edge = jnp.where(place < 5, above, jnp.where((place >= 59) & (place < 64), below, 0.0))
        black[p + 1] = black0[p + 1] + turn(edge, 64 - turned, 1)
        edge = jnp.where((place >= 64) & (place < 68), above, jnp.where(place >= 124, below, 0.0))
        g_red[p + 1] = g_red0[p + 1] + turn(edge, -turned, 1)

    def merge_black(n):
        below, above = later[n // 8], held[2 * (n // 8) + 1]
        turned = 8 * (n % 8)
        place = (lane - turned) & 127
        edge = jnp.where((place >= 5) & (place < 8), above, jnp.where((place >= 66) & (place < 69), below, 0.0))
        g_black[2 * n + 2] = g_black0[2 * n + 2] + turn(edge, 59 - turned, 1)
        edge = jnp.where((place >= 69) & (place < 72), above, jnp.where((place >= 2) & (place < 5), below, 0.0))
        g_black[2 * n + 3] = g_black0[2 * n + 3] + turn(edge, -5 - turned, 1)

    for u in range(5):
        held[2 * u], held[2 * u + 1] = sides(u)
        if u < 3:
            later[u] = turn(held[2 * u], 2, 1)
    for q in (0, 1, 38, 39, 40, 41):
        g_black[q] = zero
    for ref in (black, g_red):
        for q in (0, 39, 40, 41):
            ref[q] = zero
    for ref in (red, v_black):
        for q in (0, 1, 38, 39, 40, 41):
            ref[q] = zero
    for n in range(44):
        if n < 38:
            merge(n)
        if n % 2 == 0 and n < 36:
            merge_black(n // 2)
        if 1 <= n - 2 < 37:
            relax_at(L0, edges, c_ref, black, g_red, red, n - 2, True, even, lanes)
        if 1 <= n - 4 < 37:
            black_rest_at(L0, edges, c_ref, d_ref, red, g_black, v_black, rest, n - 4, even, lanes)
        if 3 <= n - 6 < 35:
            rest_fold_at(L0, edges, d_ref, g_red, red, v_black, rest, 3, z_ref, n - 6, even, lanes)
    halve(L0, 32, z_ref, planes, weights)

    def quad(q):
        total = planes[4 * q]
        for m in range(1, 4):
            total = total + turn(planes[4 * q + m], 32 * m, 1)
        scatter_rows(natural, q, total)
        return natural[q, 4:36]

    for q in range(4):
        low_quads[q] = quad(q)
        high_quads[q] = quad(q + 4)


def quad_rows(ib, ia, low_quads, high_quads, jb, ja, q):
    own = (ib, low_quads, high_quads, ia)[q // 4][q % 4]
    return jnp.concatenate([jb[q], own, ja[q]], axis=0)


def pack_quads_kernel(ib, ia, low_quads, high_quads, jb, ja, ku, kd):
    low_half = (lanes_of((64, 128)) & 31) < 16
    for u in range(8):
        first, second = (quad_rows(ib, ia, low_quads, high_quads, jb, ja, 2 * u + k) for k in range(2))
        kd[u] = jnp.where(low_half, turn(first, 32, 1), turn(second, 48, 1))
        ku[u] = jnp.where(low_half, turn(first, -48, 1), turn(second, -32, 1))


def join_kernel(ib, ia, low_quads, high_quads, jb, ja, qf):
    for q in range(16):
        qf[q] = quad_rows(ib, ia, low_quads, high_quads, jb, ja, q)


WINDOWS = (L1, L2, L3_OWN, L3)
WHOLES = (L4, L5, L6)
DOUBLINGS = ((32, False), (16, False), (8, False), (4, False), (16, True), (8, True))


def geometry_kernel(after, *refs):
    edges, whole = block_edges(), whole_edges()
    for index, lv in enumerate(WINDOWS + WHOLES):
        set_coefficients(lv, edges if lv in WINDOWS else whole, refs[2 * index], refs[2 * index + 1])
    refs = refs[2 * len(WINDOWS + WHOLES) :]
    refs[0][...] = halving_weights(0)
    for n, (size, is_whole) in enumerate(DOUBLINGS):
        at = whole if is_whole else edges
        refs[1][n] = doubling_weights(size, at.klo, at.khi)


def middle_kernel(
    qf, kb, ka, c1, d1, c2, d2, c3, d3, weights, lanes, v1, gr1, gb1, v2, gr2, gb2, message,
    red1, y1, z1, p1, red2, y2, z2, p2, gr3, gb3, red3, black3, y3, z3, p3, natural,
):
    edges = block_edges()
    lane = lanes_of((64, 128))
    even = even_mask(64)

    def unpack(u):
        below = jnp.where(edges.klo, 0.0, gather_rows(kb, u, 64))
        above = jnp.where(edges.khi, 0.0, gather_rows(ka, u, 64))
        sides = ((turn(below, 16, 1), above), (below, turn(above, -16, 1)))
        for h in range(2):
            value = gather_rows(qf, 2 * u + h, 64)
            left, right = sides[h]
            for t in range(2):
                both = []
                for m in (2 * t, 2 * t + 1):
                    place = (lane - 32 * m) & 127
                    edge = jnp.where(place < 48, right, jnp.where(place >= 112, left, 0.0))
                    both.append(turn(jnp.where(place < 32, value, edge), -32 * m, 1))
                index = 4 * u + 2 * h + t
                gr1[index] = jnp.where(even, both[0], both[1])
                gb1[index] = jnp.where(even, both[1], both[0])

    clear_guards(red1, v1)
    for n in range(36):
        if n % 4 == 0 and n < 32:
            unpack(n // 4)
        p = n - 1
        if 0 <= p < 30:
            red1[p + 1] = L1.scale * gr1[p + 1] * c1[kind(L1, edges, p, True)]
        if 0 <= n - 3 < 30:
            black_rest_at(L1, edges, c1, d1, red1, gb1, v1, y1, n - 3, even, lanes)
        if 1 <= n - 5 < 29:
            rest_fold_at(L1, edges, d1, gr1, red1, v1, y1, 1, z1, n - 5, even, lanes)
    halve(L1, 28, z1, p1, weights)
    colour_planes(p1, 14, gr2, gb2)
    clear_guards(red2, v2, gr2, gb2)
    relax_zero(L2, edges, c2, gr2, red2, 0, 14)
    relax_black_rest(L2, edges, c2, d2, red2, gb2, v2, y2, 0, 14)
    restrict(L2, edges, d2, gr2, red2, v2, y2, 1, 12, z2, p2, weights)
    colour_planes(p2, 6, gr3, gb3)
    clear_guards(red3, black3)
    relax_zero(L3_OWN, edges, c3, gr3, red3, 0, 6)
    relax_black_rest(L3_OWN, edges, c3, d3, red3, gb3, black3, y3, 0, 6)
    restrict(L3_OWN, edges, d3, gr3, red3, black3, y3, 1, 4, z3, p3, weights)
    lane = lanes_of((8, 128))
    row = rows_of((8, 128))
    third = jnp.zeros((8, 128), F32)
    for i in range(8):
        scatter_rows(natural, i, p2[i + 2])
        third = third + turn(jnp.where(lane < 8, natural[i, 4:12], 0.0), 8 * i, 1)
    folded = third + turn(turn(third, 4, 0), 64, 1)
    blocks = jnp.zeros((8, 128), F32)
    for i in range(4):
        blocks = blocks + turn(jnp.where(lane < 4, p3[i], 0.0), 16 * i, 1)
    fourth = jnp.zeros((8, 128), F32)
    for r in range(4):
        fourth = jnp.where((lane & 15) >> 2 == r, turn(turn(blocks, 4 * r, 1), -2 - r, 0), fourth)

    def store(n):
        for r in range(4):
            message[n, r] = folded[r : r + 1]
        message[n, 4] = fourth[0:1]

    loop(0, 64, store, 8)


def plane_kernel(tiles, message, near, rows, grid, blocks):
    x, y, z = (lax.axis_index(axis) for axis in ("gx", "gy", "gz"))
    shape = (8, 128)
    lane, row = lanes_of(shape), rows_of(shape)

    for n in range(64):
        rows[n : n + 1] = tiles[n, 4]
    parts = [jnp.zeros(shape, F32)] * 4
    for n in range(8):
        value = rows[pl.ds(n, 8, stride=8), :]
        here = (lane & 31) >> 2 == n
        for r in range(4):
            index = (lane >> 5) * 16 + 4 * r + (lane & 3)
            parts[r] = jnp.where(here, jnp.take_along_axis(value, index, axis=1), parts[r])
    for r in range(4):
        grid[pl.ds(r, 8, stride=4), :] = parts[r]

    lane = signed(lane)
    for dy in range(3):
        sides = []
        for dz in range(3):
            yy, zz = y + (dy - 1), z + (dz - 1)
            inside = (yy >= 0) & (yy < COUNT) & (zz >= 0) & (zz < COUNT)
            index = jnp.clip(yy, 0, COUNT - 1) * COUNT + jnp.clip(zz, 0, COUNT - 1)
            for r in range(4):
                blocks[3 * dy + dz, r : r + 1] = tiles[index, r]
            value = blocks[3 * dy + dz]
            value = jnp.where(row < 4, value, turn(turn(value, 4, 0), 64, 1))
            sides.append(jnp.where(inside, value, 0.0))
        for i in range(8):
            total = jnp.zeros(shape, F32)
            for dz in range(3):
                hit = (lane >= 8 * (dz - 1)) & (lane < 8 * dz)
                total = jnp.where(hit, turn(sides[dz], 8 * (dz - 1) - 8 * i, 1), total)
            near[i, 8 * dy : 8 * dy + 8] = total

    wide = lanes_of((24, 128))
    ends = []
    for first in (2, 0):
        total = jnp.zeros((24, 128), F32)
        for n in range(6):
            hit = (wide >= 20 * n) & (wide < 20 * n + 20)
            total = jnp.where(hit, turn(near[first + n], 20 * n + 6, 1), total)
        ends.append(total)
    for n in range(COUNT):
        message[n, 0:32] = grid[...]
        message[n, 32:56] = jnp.where(x < n, ends[0], ends[1])


def coarse_kernel(
    tiles, near, v2, gr2, gb2, v1, gr1, gb1, v0, gr0, gb0, c0, d0, c1, c2, c3, c4, d4, c5, d5, c6, halving, doubling, lanes, out, rest,
    gr4, gb4, red4, v4, y4, z4, p4, gr5, gb5, red5, v5, y5, z5, p5, gr6, gb6, red6, v6, full,
    gr3, gb3, red3, v3, b3, b2, red2, b1, red1, b0, red0, y0, e_ref, mixed, plain, fine_mixed, fine_plain, natural, last, out_held, rest_held, sems,
):
    edges = block_edges()
    whole = whole_edges()
    x, y, z = (lax.axis_index(axis) for axis in ("gx", "gy", "gz"))

    lane = signed(lanes_of((24, 128)))
    even = even_natural((24, 128))
    empty = jnp.zeros((24, 128), F32)

    def put(index, low, high):
        natural[index, 0:24] = jnp.where(even, low, high)
        natural[index + 12, 0:24] = jnp.where(even, high, low)

    for n in range(4):
        put(4 + n, near[2 * n], near[2 * n + 1])
    put(0, empty, empty)
    put(11, empty, empty)
    for at, first in ((x - 1, 1), (x + 1, 8)):
        inside = (at >= 0) & (at < COUNT)
        value = jnp.where(inside, tiles[jnp.clip(at, 0, COUNT - 1), 32:56], 0.0)
        planes = [jnp.where((lane >= -6) & (lane < 14), turn(value, -20 * n - 6, 1), 0.0) for n in range(6)]
        for n in range(3):
            put(first + n, planes[2 * n], planes[2 * n + 1])
    for n in range(24):
        natural[n, 24:32] = jnp.zeros((8, 128), F32)
    for n in range(12):
        gr3[n + 1] = gather_rows(natural, n, 32)
        gb3[n + 1] = gather_rows(natural, n + 12, 32)
    clear_guards(red3, v3)
    relax_zero(L3, edges, c3, gr3, red3, 0, 12)
    relax(L3, edges, c3, red3, gb3, v3, 0, 12, False)

    lane = lanes_of((32, 128))
    even32 = even_mask(32)
    zero = jnp.zeros((8, 128), F32)

    def place(n):
        value = gather_rows(tiles, n, 32)
        for t in range(2):
            low = jnp.where(lane < 32, turn(value, -64 * t, 1), 0.0)
            high = jnp.where(lane < 32, turn(value, -64 * t - 32, 1), 0.0)
            index = 2 * n + t + 1
            gr4[index] = jnp.where(even32, low, high)
            gb4[index] = jnp.where(even32, high, low)

    loop(0, 8, place, 4)
    clear_guards(red4, v4, gr4, gb4)
    relax_zero(L4, whole, c4, gr4, red4, 0, 16)
    relax_black_rest(L4, whole, c4, d4, red4, gb4, v4, y4, 0, 16)
    restrict(L4, whole, d4, gr4, red4, v4, y4, 0, 16, z4, p4, halving)
    colour_planes(p4, 8, gr5, gb5)
    clear_guards(red5, v5, gr5, gb5)
    relax_zero(L5, whole, c5, gr5, red5, 0, 8)
    relax_black_rest(L5, whole, c5, d5, red5, gb5, v5, y5, 0, 8)
    restrict(L5, whole, d5, gr5, red5, v5, y5, 0, 8, z5, p5, halving)
    colour_planes(p5, 4, gr6, gb6)
    clear_guards(red6, v6)
    relax_zero(L6, whole, c6, gr6, red6, 0, 4)
    relax(L6, whole, c6, red6, gb6, v6, 0, 4, False)
    for _ in range(COARSE_SWEEPS - 1):
        relax(L6, whole, c6, v6, gr6, red6, 0, 4, True)
        relax(L6, whole, c6, red6, gb6, v6, 0, 4, False)

    def ascend(coarse, fine, c, w, coarse_red, coarse_black, kept, g_red, g_black, red):
        count = coarse.size
        e, rows = e_ref.at[0:count, 0:count], slice(0, count)
        n, p = mixed.at[0 : count + 2, rows], plain.at[0 : count + 2, rows]
        whole_planes(coarse, coarse_red, coarse_black, 0, coarse.pairs, e)
        prolong(e, count, 0, count, whole, w, mixed.at[1 : count + 1, rows], plain.at[1 : count + 1, rows])
        p[0] = -p[1]
        p[count + 1] = -p[count]
        correct(fine, whole, c, kept, n, p, 0, 1, kept, 0, fine.pairs)
        relax(fine, whole, c, kept, g_red, red, 0, fine.pairs, True)
        relax(fine, whole, c, red, g_black, kept, 0, fine.pairs, False)

    ascend(L6, L5, c5, doubling.at[5], red6, v6, v5, gr5, gb5, red5)
    ascend(L5, L4, c4, doubling.at[4], red5, v5, v4, gr4, gb4, red4)

    even = even_mask(32)
    for t in (0, 1, 2, 3, 36, 37, 38, 39):
        full[t] = jnp.zeros((48, 128), F32)

    def expand(t):
        r, b = red4[t + 1], v4[t + 1]
        for n, value in ((2 * t + 4, jnp.where(even, r, b)), (2 * t + 5, jnp.where(even, b, r))):
            full[n, 0:8] = zero
            scatter_rows(full, n, value, 8)
            full[n, 40:48] = zero

    loop(0, 16, expand, 4)

    def cut(t):
        rows = gather_rows(full, 4 * x + t, 16, 4 * y + 4)
        e_ref[t, 0:16] = pltpu.roll(rows, (128 - 4 * z) & 127, 1)

    loop(0, 12, cut)

    def lift(index, fine, c, count, rows, plane_zero, row_zero, size, kept, dest, low, high):
        e = e_ref.at[0:count, 0:rows]
        n, p = mixed.at[0:count, 0:rows], plain.at[0:count, 0:rows]
        prolong(e, count, plane_zero, size, edges, doubling.at[index], n, p)
        correct(fine, edges, c, kept, n, p, row_zero, plane_zero, dest, low, high)

    def smooth(lv, c, black, g_red, g_black, red, low, high, low2, high2):
        relax(lv, edges, c, black, g_red, red, low, high, True)
        relax(lv, edges, c, red, g_black, black, low2, high2, False)

    lift(3, L3, c3, 12, 16, 4, 4, 4, v3, b3, 1, 11)
    clear_guards(b3, red3)
    smooth(L3, c3, b3, gr3, gb3, red3, 2, 10, 2, 10)

    window_planes(L3, red3, b3, 2, 8, 4, natural.at[0:16, 0:32], e_ref.at[0:16, 0:16])
    lift(2, L2, c2, 16, 16, 4, 4, 8, v2, b2, 0, 14)
    clear_guards(b2, red2)
    smooth(L2, c2, b2, gr2, gb2, red2, 1, 13, 1, 13)

    whole_planes(L2, red2, b2, 1, 12, e_ref.at[0:24, 0:32])
    e = e_ref.at[0:24, 0:32]
    n, p = mixed.at[0:24, 0:32], plain.at[0:24, 0:32]
    prolong(e, 24, 4, 16, edges, doubling.at[1], n, p)
    correct1 = correct_at(L1, edges, c1, v1, n, p, 8, 4, b1)
    for index in (5, 26):
        b1[index] = jnp.zeros(b1.shape[1:], F32)
    even1 = even_mask(64)
    even0 = even_mask(80)
    mixed0, plain0 = fine_mixed, fine_plain
    correct0 = correct_at(L0, edges, c0, v0, mixed0, plain0, 4, 4, b0)
    b0[1] = jnp.zeros(b0.shape[1:], F32)
    b0[38] = jnp.zeros(b0.shape[1:], F32)
    copies = []

    def send(held, target, n):
        copy = pltpu.make_async_copy(held.at[pl.ds(8 * n, 8)], target.at[pl.ds(8 * n, 8)], sems.at[len(copies)])
        copy.start()
        copies.append(copy)

    def store(held, p, r, b):
        for n, value in ((0, jnp.where(even0, r, b)), (1, jnp.where(even0, b, r))):
            scatter_rows(last, 2 * (p & 7) + n, value)
            held[2 * p - 6 + n] = last[2 * (p & 7) + n, 8:72, 0:64]

    def coarse_step(n):
        if n < 25:
            correct1(n)
        if 5 <= n - 2 < 25:
            relax_at(L1, edges, c1, b1, gr1, red1, n - 2, True, even1, lanes)
        if 6 <= n - 4 < 24:
            relax_at(L1, edges, c1, red1, gb1, b1, n - 4, False, even1)

    def lift_planes(c):
        planes = []
        for t in range(4 * c, 4 * c + 4):
            r, b = red1[t + 6], b1[t + 6]
            scatter_rows(natural, 2 * t, jnp.where(even1, r, b))
            scatter_rows(natural, 2 * t + 1, jnp.where(even1, b, r))
            planes += [gather_rows(natural, 2 * t + k, 40, 12) for k in range(2)]
        both = split_dot(jnp.concatenate(planes, axis=0), doubling[0])
        for k in range(8):
            mixed0[8 * c + k] = both[40 * k : 40 * k + 40, :128]
            plain0[8 * c + k] = both[40 * k : 40 * k + 40, 128:]
        if c == 0:
            plain0[3] = jnp.where(edges.ilo, -plain0[4], plain0[3])
        if c == 4:
            plain0[36] = jnp.where(edges.ihi, -plain0[35], plain0[36])

    def fine_step(n):
        if n < 37:
            correct0(n)
        if 1 <= n - 2 < 37:
            relax_at(L0, edges, c0, b0, gr0, red0, n - 2, True, even0, lanes)
        p = n - 4
        if 2 <= p < 36:
            black_rest_at(L0, edges, c0, d0, red0, gb0, b0, y0, p, even0)
        if 3 <= p < 35:
            store(out_held, p, red0[p + 1], b0[p + 1])
            if p % 4 == 2:
                send(out_held, out, p // 4 - 1)
        p = n - 6
        if 3 <= p < 35:
            store(rest_held, p, red_rest(L0, edges, d0, gr0, red0, b0, p, even0, lanes), y0[p + 1])
            if p % 4 == 2:
                send(rest_held, rest, p // 4 - 1)

    done, ready = 0, 0
    for n in range(5, 29):
        coarse_step(n)
        for _ in range(2):
            if done < ready:
                done += 1
                fine_step(done)
        if n >= 12 and n % 4 == 0:
            lift_planes(n // 4 - 3)
            ready = 2 * n - 19
    for n in range(done + 1, 43):
        fine_step(n)
    for copy in copies:
        copy.wait()


def struct(*shape):
    return jax.ShapeDtypeStruct(shape, F32)


def call(kernel, outs, scratch, flops=2_000_000, out_space=pltpu.VMEM, semaphores=0):
    space = pl.BlockSpec(memory_space=pltpu.VMEM)
    extra = [pltpu.SemaphoreType.DMA((semaphores,))] if semaphores else []

    def run(*args):
        return pl.pallas_call(
            kernel,
            out_shape=outs,
            in_specs=[space] * len(args),
            out_specs=[pl.BlockSpec(memory_space=out_space)] * len(outs),
            scratch_shapes=[pltpu.VMEM(shape, F32) for shape in scratch] + extra,
            compiler_params=pltpu.CompilerParams(vmem_limit_bytes=40 * 2**20),
            cost_estimate=pl.CostEstimate(flops=flops, bytes_accessed=1_000_000, transcendentals=0),
        )(*args)

    return run


def pair(to_next, to_before, axis, ring=False):
    up = [(i, (i + 1) % COUNT) for i in range(COUNT if ring else COUNT - 1)]
    down = [(j, i) for i, j in up]
    after = lax.ppermute(to_before, axis, down)
    before = lax.ppermute(to_next, axis, up)
    return before, after


def face(guess, source, start, first):
    even = ((lax.broadcasted_iota(jnp.int32, (64, 64), 0) + lax.broadcasted_iota(jnp.int32, (64, 64), 1)) & 1) == 0
    low, high = guess[start : start + 6 : 2], guess[start + 1 : start + 6 : 2]
    f_low, f_high = source[start : start + 6 : 2], source[start + 1 : start + 6 : 2]
    red = jnp.where(even, f_low, f_high)
    black = jnp.where(even, f_high, f_low)
    mixed = jnp.concatenate([jnp.where(even, high, low), red], axis=2)
    return jnp.concatenate([mixed, jnp.concatenate([black[first : first + 1], black[first + 1 : first + 2]], axis=2)], axis=0)


def coefficient_shapes(*levels):
    shapes = []
    for lv in levels:
        shapes += [struct(4, lv.rows, 128), struct(3, lv.rows, 128)]
    return shapes


def per_device(right_side, guess):
    ib, ia = pair(face(guess, right_side, 58, 1), face(guess, right_side, 0, 0), "gx")
    x, y = call(compact_kernel, (struct(32, 64, 128), struct(16, 64, 128)), [])(guess, right_side)

    up, down = call(rows_kernel, (struct(248, 128), struct(248, 128)), [])(
        ib, ia, guess[:, 0:8], guess[:, 56:64], right_side[:, 0:8], right_side[:, 56:64]
    )
    jb, ja = pair(up, down, "gy")
    xf, yf, ku, kd = call(
        pack_kernel, (struct(40, 80, 128), struct(24, 80, 128), struct(5, 80, 128), struct(5, 80, 128)), []
    )(ib, ia, x, y, jb, ja)
    kb, ka = pair(ku, kd, "gz", True)
    fine = L0.shape()
    field = struct(*fine)
    weights = jax.ShapeDtypeStruct((256, 128), BF16)
    black, g_red, g_black, c0, d0, w0, lanes = call(
        spread_kernel, (field, field, field, *coefficient_shapes(L0), weights, weights), []
    )(xf, yf)
    v0, gr0, gb0, low_quads, high_quads = call(
        fine_kernel,
        (field, field, field, struct(4, 32, 128), struct(4, 32, 128)),
        [fine, fine, fine, (32, 40, 128), (32, 40, 128), (8, 40, 128), (3, 80, 128), (10, 80, 128)],
    )(black, g_red, g_black, kb, ka, c0, d0, w0, lanes)

    ib, ia = pair(high_quads, low_quads, "gx")
    shapes = coefficient_shapes(*WINDOWS, *WHOLES) + [weights, jax.ShapeDtypeStruct((6, 256, 256), BF16)]
    c1, d1, c2, d2, c3o, d3o, c3, _, c4, d4, c5, d5, c6, _, halving, doubling = call(
        geometry_kernel, tuple(shapes), []
    )(low_quads)

    def quad_ends(low):
        return jnp.concatenate([part[:, low : low + 16] for part in (ib, low_quads, high_quads, ia)], axis=0)

    jb, ja = pair(quad_ends(16), quad_ends(0), "gy")
    parts = (ib, ia, low_quads, high_quads, jb, ja)
    ku, kd = call(pack_quads_kernel, (struct(8, 64, 128), struct(8, 64, 128)), [])(*parts)
    kb, ka = pair(ku, kd, "gz", True)
    (qf,) = call(join_kernel, (struct(16, 64, 128),), [])(*parts)
    s1, s2, s3 = L1.shape(), L2.shape(), L3_OWN.shape()
    v1, gr1, gb1, v2, gr2, gb2, message = call(
        middle_kernel,
        tuple(struct(*s) for s in (s1, s1, s1, s2, s2, s2, (64, 5, 1, 128))),
        [s1, s1, (28, 32, 128), (28, 32, 128), s2, s2, (12, 16, 128), (12, 16, 128)]
        + [s3, s3, s3, s3, s3, (4, 8, 128), (4, 8, 128), (8, 16, 128)],
    )(qf, kb, ka, c1, d1, c2, d2, c3o, d3o, halving, lanes)

    tiles = lax.all_to_all(message, ("gy", "gz"), 0, 0)
    message, near = call(
        plane_kernel, (struct(8, 56, 128), struct(8, 24, 128)), [(64, 128), (32, 128), (9, 8, 128)]
    )(tiles)
    tiles = lax.all_to_all(message, "gx", 0, 0)
    s3, s4, s5, s6 = L3.shape(), L4.shape(), L5.shape(), L6.shape()
    return tuple(
        call(
            coarse_kernel,
            (struct(64, 64, 64), struct(64, 64, 64)),
            [s4, s4, s4, s4, s4, (16, 16, 128), (16, 16, 128)]
            + [s5, s5, s5, s5, s5, (8, 8, 128), (8, 8, 128)]
            + [s6, s6, s6, s6, (40, 48, 128)]
            + [s3, s3, s3, s3, s3, s2, s2, s1, s1, fine, fine, fine]
            + [(42, 40, 128), (42, 40, 128), (42, 40, 128), (40, 40, 128), (40, 40, 128), (40, 64, 128), (16, 80, 128), (64, 64, 64), (64, 64, 64)],
            out_space=pl.ANY,
            semaphores=16,
        )(tiles, near, v2, gr2, gb2, v1, gr1, gb1, v0, gr0, gb0, c0, d0, c1, c2, c3, c4, d4, c5, d5, c6, halving, doubling, lanes)
    )


def solution(mesh):
    return jax.shard_map(
        per_device,
        mesh=mesh,
        in_specs=(P("gx", "gy", "gz"), P("gx", "gy", "gz")),
        out_specs=(P("gx", "gy", "gz"), P("gx", "gy", "gz")),
        check_vma=False,
    )
```
